32 devices in a mesh: expert: 8 (over z, y), gate: 4 (over x, core).
Axes of the slice: x: 2, y: 2, z: 4, core: 2. Of those that a mesh axis runs over, the one named last changes fastest.
Arguments:
- samples: bfloat16 [6144, 4096], P('expert', 'gate'), may hold values from -4 to 4
- gate_weight: bfloat16 [4096, 32], P('gate'), may hold values from -1 to 1
- expert_ids: int32 [6144, 2], P('expert'), may hold values from 0 to 31, all different within a row; in each aligned block of 768 rows (0 to 767, 768 to 1535, ...) at most 96 rows name the same one
- pad_mask: int32 [6144], P('expert'), may hold values 0 or 1
- up_weight: bfloat16 [32, 4096, 1024], P(('expert', 'gate')), may hold values from -0.09375 to 0.09375
- down_weight: bfloat16 [32, 1024, 1024], P(('expert', 'gate')), may hold values from -0.1875 to 0.1875
Outputs:
- combined: bfloat16 [6144, 1024], P('expert', 'gate')
The draws below stay inside these ranges and needn't reach their ends.
Inputs may be any that keep to these rules, and one draw needn't show every extreme that they name: `expert_ids`: each sample names two different experts; among the 768 samples of one index of expert no expert is named more than 96 times, a bound that some block reaches.
All inputs are finite; a program needn't handle non-finite values. No bound on the sum of `pad_mask` on one device may be relied on, other than what follows from the above.
Results may differ from the reference program's by a relative error of at most 0.0057.
Values may be sent and summed in bfloat16 or wider, within the bound.
A program may use at most 128 MiB of HBM per device.

```python
import math
import jax
import jax.numpy as jnp
import numpy as np
from jax import lax

D = 4096
H = 1024
OUT = 1024
ROWS_DEV = 768
EXPERTS = 32
CAP = 96
BATCH = 6144
N_EXPERT = 8


def draw_samples(key, part):
    inner = jax.random.fold_in(key, 3)
    drawn = jnp.clip(jax.random.normal(inner, (BATCH, D), jnp.float32), -4.0, 4.0)
    return drawn.astype(jnp.bfloat16)


def draw_gate_weight(key, part):
    inner = jax.random.fold_in(key, 5)
    spread_key = jax.random.fold_in(key, 6)
    scales = jnp.exp(jax.random.uniform(spread_key, (1, EXPERTS), jnp.float32, jnp.log(0.15), jnp.log(1.5)))
    drawn = jnp.clip(jax.random.normal(inner, (D, EXPERTS), jnp.float32), -4.0, 4.0)
    drawn = drawn * scales / jnp.sqrt(jnp.float32(D))
    return drawn.astype(jnp.bfloat16)


def place_ends(entries, rng, low, high):
    place = [jax.random.randint(jax.random.fold_in(rng, axis), (), 0, length) for axis, length in enumerate(entries.shape)]
    longest = entries.shape.index(max(entries.shape))
    neighbour = place[:longest] + [(place[longest] + 1) % entries.shape[longest]] + place[longest + 1:]
    return entries.at[tuple(place)].set(low).at[tuple(neighbour)].set(high)


def levels(key, extent, cuts, low, largest):
    def one(dim, blocks):
        draws = jax.random.uniform(jax.random.fold_in(jax.random.fold_in(key, 6), dim), (blocks,), jnp.float32, low / len(cuts), largest / len(cuts))
        return jnp.repeat(jnp.exp(draws), extent[dim] // blocks).reshape((-1,) + (1,) * (len(extent) - dim - 1))

    loudness = one(*cuts[0])
    for cut in cuts[1:]:
        loudness = loudness * one(*cut)
    return loudness


def routed_block(rng, own, number, rows, number_of, top, reach, skew):
    order = jax.random.permutation(rng, number_of)
    packed, usual = portions_of(number_of, rows * top, reach, skew, True), portions_of(number_of, rows * top, reach, skew, False)
    places = jnp.arange(number_of)

    def named(sizes, offset_by):
        used = int((sizes > 0).sum())
        fixed = max(1, used // 4)
        moved = fixed + (places - fixed + offset_by * (used - fixed)) % max(1, number_of - fixed)
        return jnp.zeros((number_of,), jnp.int32).at[order[jnp.where(places < fixed, places, moved)]].set(jnp.asarray(sizes, jnp.int32))

    sizes = jnp.where(number % 4 == 0, named(packed, number // 4), named(usual, number - number // 4 - 1))
    mixed = jax.random.permutation(jax.random.fold_in(own, 3), number_of)
    source_of, taker = mixed[0:number_of // 2 * 2:2], mixed[1:number_of // 2 * 2:2]
    room = jnp.minimum(sizes[source_of] - 1, reach - sizes[taker]) // 2
    room = jnp.where((source_of == order[0]) | (taker == order[0]) | (sizes[taker] == 0), 0, jnp.maximum(room, 0))
    moved = jax.random.randint(jax.random.fold_in(own, 4), (number_of // 2,), 0, 1 << 20) % (room + 1)
    sizes = sizes.at[source_of].add(-moved).at[taker].add(moved)
    labels = jnp.searchsorted(jnp.cumsum(sizes), jnp.arange(rows * top), side="right").astype(jnp.int32)
    listing = labels.reshape(top, rows).T
    listing = listing[jax.random.permutation(jax.random.fold_in(own, 1), rows)]
    offset_by = jax.random.randint(jax.random.fold_in(own, 2), (rows, 1), 0, top)
    return jnp.take_along_axis(listing, (jnp.arange(top)[None, :] + offset_by) % top, axis=1)


def portions_of(number_of, total, limit, slope, full):
    weights = [(1 << 20) // math.isqrt(standing ** slope) + 1 for standing in range(1, number_of + 1)]
    largest = limit if full else min(limit, max(-(-total // number_of), total * weights[0] // sum(weights)))
    least = 1 if total - largest >= number_of - 1 else 0
    counts, rest = [largest] + [least] * (number_of - 1), total - largest - least * (number_of - 1)
    while rest > 0:
        movable = [i for i in range(1, number_of) if counts[i] < largest] or [i for i in range(1, number_of) if counts[i] < limit]
        whole, budget = sum([weights[i] for i in movable]), rest
        for i in movable:
            addition = min(limit - counts[i], max(1, budget * weights[i] // whole), rest)
            counts[i] = counts[i] + addition
            rest = rest - addition
    return np.array(counts)


def noise(stream_key, extent, spread, most, cuts=(), kind=jnp.bfloat16):
    gain = levels(stream_key, extent, cuts, -0.22, 0.18) if cuts else 1.0
    drawn = jax.random.normal(stream_key, extent, jnp.float32) * spread * gain
    return jnp.minimum(jnp.maximum(drawn, -most), most).astype(kind)


def setup_inputs(seed: int = 0) -> dict:
    key_of = jax.random.split(jax.random.key(seed), 7)
    samples = draw_samples(jax.random.fold_in(key_of[6], 71), 0)
    gate_weight = draw_gate_weight(jax.random.fold_in(key_of[6], 71), 0)
    expert_ids_keys = jax.random.split(jax.random.fold_in(key_of[2], 1), BATCH // ROWS_DEV)
    expert_ids_turns = jax.random.permutation(jax.random.fold_in(key_of[2], 3), BATCH // ROWS_DEV)
    expert_ids = jax.vmap(lambda own, number: routed_block(jax.random.fold_in(key_of[2], 2), own, number, ROWS_DEV, EXPERTS, 2, CAP, 1))(expert_ids_keys, expert_ids_turns).reshape((BATCH, 2))
    pad_mask = place_ends((jax.random.randint(key_of[3], (BATCH,), 0, 8) < 7).astype(jnp.int32), jax.random.fold_in(key_of[3], 1), 0, 1)
    up_weight = noise(key_of[4], (EXPERTS, D, H), D ** -0.5, 0.09375, ((0, 32),))
    down_weight = noise(key_of[5], (EXPERTS, H, OUT), H ** -0.5, 0.1875, ((0, 32),))
    return {"samples": samples, "gate_weight": gate_weight, "expert_ids": expert_ids, "pad_mask": pad_mask, "up_weight": up_weight, "down_weight": down_weight}


def reference(samples, gate_weight, expert_ids, pad_mask, up_weight, down_weight):
    logits = jnp.dot(samples, gate_weight, preferred_element_type=jnp.float32)
    row_top = jnp.max(logits, axis=1, keepdims=True)
    row_total = jnp.sum(jnp.exp(logits - row_top), axis=1, keepdims=True)
    chosen = jnp.take_along_axis(logits, expert_ids, axis=1)
    factor = EXPERTS * jnp.exp(chosen - row_top) / row_total * pad_mask.astype(jnp.float32)[:, None]
    grouped = expert_ids.reshape(N_EXPERT, ROWS_DEV * 2)
    onehot = (grouped[:, :, None] == jnp.arange(EXPERTS, dtype=jnp.int32)[None, None, :]).astype(jnp.int32)
    slot_rank = jnp.sum(onehot * (jnp.cumsum(onehot, axis=1) - 1), axis=2)
    source_index = jnp.arange(N_EXPERT, dtype=jnp.int32)[:, None]
    position = (grouped * (N_EXPERT * CAP) + source_index * CAP + slot_rank).reshape(-1).astype(jnp.int32)
    row_index = jnp.repeat(jnp.arange(BATCH, dtype=jnp.int32), 2)
    owners = jnp.full((EXPERTS * N_EXPERT * CAP,), BATCH, jnp.int32).at[position].set(row_index)
    padded = jnp.concatenate([samples, jnp.zeros((1, D), samples.dtype)], axis=0)

    def expert_pass(operands):
        owner_block, first, second = operands
        slot_block = padded[owner_block]
        hidden = jnp.dot(slot_block, first, preferred_element_type=jnp.float32)
        active = jnp.maximum(hidden, 0.0).astype(jnp.bfloat16)
        return jnp.dot(active, second, preferred_element_type=jnp.float32).astype(jnp.bfloat16)

    results = lax.map(expert_pass, (owners.reshape(EXPERTS, N_EXPERT * CAP), up_weight, down_weight))
    flat_out = results.reshape(EXPERTS * N_EXPERT * CAP, OUT)
    picked = flat_out[position].astype(jnp.float32).reshape(BATCH, 2, OUT)
    return jnp.sum(factor[:, :, None] * picked, axis=1).astype(jnp.bfloat16)
```

```python
import functools

import jax
import jax.numpy as jnp
from jax import lax
from jax.experimental import pallas as pl
from jax.experimental.pallas import tpu as pltpu
from jax.sharding import PartitionSpec as P


MESH = pl.DeviceIdType.MESH
CHUNKS = 4
SIDES = 2


def routing(expert_ids, expert_count):
    row_count = expert_ids.shape[0]
    lanes = jnp.arange(expert_count, dtype=jnp.int32)[None, :]
    first = expert_ids[:, 0:1] == lanes
    second = expert_ids[:, 1:2] == lanes
    member = first | second
    rows = jnp.arange(row_count, dtype=jnp.int32)
    lower = (rows[:, None] > rows[None, :]).astype(jnp.bfloat16)
    before = jnp.dot(lower, member.astype(jnp.bfloat16), preferred_element_type=jnp.float32)
    before = before.astype(jnp.int32)
    return first, second, member, before


def factors(logits, first, second, pad_mask, expert_count):
    top = jnp.max(logits, axis=1, keepdims=True)
    terms = jnp.exp(logits - top)
    scale = pad_mask.astype(jnp.float32)[:, None] / jnp.sum(terms, axis=1, keepdims=True)
    factor0 = expert_count * jnp.sum(jnp.where(first, terms, 0.0), axis=1, keepdims=True) * scale
    factor1 = expert_count * jnp.sum(jnp.where(second, terms, 0.0), axis=1, keepdims=True) * scale
    return factor0, factor1


def copied(source, target, sem):
    return pltpu.make_async_copy(source, target, sem)


def sent(source, target, send_sem, recv_sem, device):
    return pltpu.make_async_remote_copy(
        src_ref=source,
        dst_ref=target,
        send_sem=send_sem,
        recv_sem=recv_sem,
        device_id=device,
        device_id_type=MESH,
    )


def table(values, index):
    out = values[0]
    for k in range(1, len(values)):
        out = jnp.where(index == k, values[k], out)
    return out


ORDER = ((0, 0), (0, 1), (0, 2), (2, 0), (2, 1), (3, 0), (3, 1), (3, 2), (3, 3), (2, 2), (2, 3), (0, 3))


def exchange_kernel(
    gates,
    capacity,
    samples,
    ids,
    gate_weight,
    up,
    down,
    out,
    blocks,
    named,
    places,
    lower,
    onehot,
    dbuf,
    inc,
    upv,
    downv,
    hidden,
    obuf,
    logits,
    factor,
    edge_factor,
    ret,
    edge_ret,
    select,
    mixed,
    part,
    taken,
    own_sem,
    w_sem,
    raw_s,
    raw_r,
    id_s,
    id_r,
    ds,
    pr,
    rs,
    rr,
    er,
    gs,
    gr,
    fs,
    fr,
    ts,
    tr,
):
    chunks = CHUNKS
    local = SIDES * gates
    planes = blocks.shape[0]
    total = planes * local
    rows = blocks.shape[2]
    width = blocks.shape[3]
    slots = local * capacity
    e = lax.axis_index("expert")
    g = lax.axis_index("gate")
    z = e // SIDES
    y = lax.rem(e, SIDES)
    mine = y * gates + g
    me = e * gates + g
    low = z < planes // 2
    toward = jnp.where(low, 1, -1)
    near = jnp.where(low, 0, planes - 1)
    far = planes - 1 - near
    edge = z == near
    middle = jnp.logical_not(edge)
    mid = near + toward
    inner = z + toward

    def plane_of(rel):
        return table((mid, near, mid + toward, far), rel)

    own = [
        copied(samples.at[:, pl.ds(c * width, width)], blocks.at[z, c], own_sem.at[c])
        for c in range(chunks)
    ]
    for copy in own:
        copy.start()
    weights = (copied(up.at[0], upv, w_sem.at[0]), copied(down.at[0], downv, w_sem.at[1]))
    for copy in weights:
        copy.start()

    barrier = pltpu.get_barrier_semaphore()

    def greet(d, carry):
        t = lax.rem(me + d, total)
        pl.semaphore_signal(
            barrier, inc=1, device_id=(t // gates, lax.rem(t, gates)), device_id_type=MESH
        )
        return carry

    lax.fori_loop(1, total, greet, 0)

    earlier = lax.broadcasted_iota(jnp.int32, (rows, rows), 0)
    later = lax.broadcasted_iota(jnp.int32, (rows, rows), 1)
    lower[...] = jnp.where(earlier < later, 1.0, 0.0).astype(jnp.bfloat16)
    named[z] = ids[...]

    def end_index(rel):
        return jnp.where(rel == 0, planes, planes - 1 + rel)

    def prepare(j, rel):
        lanes = lax.broadcasted_iota(jnp.int32, (total, rows), 0)
        member = (named[j, 0:1, :] == lanes) | (named[j, 1:2, :] == lanes)
        flags = jnp.where(member, 1.0, 0.0).astype(jnp.bfloat16)
        before = jnp.dot(flags, lower[...], preferred_element_type=jnp.float32)
        places[j] = jnp.where(member, before, -1.0)
        ranks = lax.broadcasted_iota(jnp.int32, (capacity, rows), 0).astype(jnp.float32)

        def build(index, plane):
            def one(i, carry):
                line = places[j, pl.ds(plane * local + i, 1), :]
                onehot[index, pl.ds(pl.multiple_of(i * capacity, capacity), capacity), :] = (
                    jnp.where(line == ranks, 1.0, 0.0).astype(jnp.bfloat16)
                )
                return carry

            lax.fori_loop(0, local, one, 0)

        @pl.when(middle & (rel != 1))
        def _():
            build(end_index(rel), near)

        build(rel, z)

    own_rel = jnp.where(edge, 1, 0)
    prepare(z, own_rel)
    for copy in own:
        copy.wait()
    pl.semaphore_wait(barrier, total - 1)

    def ids_to(step, sem):
        return sent(named.at[z], named.at[z], sem, id_r.at[z], ((z + step) * SIDES + y, g))

    ids_to(toward, id_s.at[0]).start()

    @pl.when(edge)
    def _():
        ids_to(2 * toward, id_s.at[1]).start()

    def shift(j, c):
        return sent(
            blocks.at[j, c], blocks.at[j, c], raw_s.at[j, c], raw_r.at[j, c], (inner * SIDES + y, g)
        )

    for c in range(2):
        shift(z, c).start()

    @pl.when(edge)
    def _():
        for c in range(2, chunks):
            shift(z, c).start()

    gate_routes = []
    for d in range(1, gates):
        t = lax.rem(g + d, gates)
        gate_routes.append(sent(logits.at[g], logits.at[g], gs.at[d - 1], gr.at[d - 1], (e, t)))

    def listed(s):
        rel = table([rel for rel, c in ORDER], s)
        return rel, table([c for rel, c in ORDER], s)

    def dispatch(s, q):
        rel, c = listed(jnp.minimum(s, len(ORDER) - 1))
        second = q == 2
        rel = jnp.where(edge | (second & (s < 5)), 1, jnp.where(second, 0, rel))
        c = jnp.where(edge, s, jnp.where(second, jnp.where(s < 5, s - 1, chunks - 1), c))
        valid = jnp.where(
            edge,
            (q == 1) & (s < chunks),
            jnp.where(
                q == 0,
                s < len(ORDER),
                jnp.where(q == 1, s < len(ORDER) - 1, (s >= 1) & (s <= 5)),
            ),
        )
        fresh = middle & (((q == 0) & (rel >= 2)) | ((q == 2) & (rel == 1)))

        @pl.when(valid)
        def _():
            j = plane_of(rel)

            @pl.when(fresh)
            def _():
                copied(blocks.at[j, c], blocks.at[j, c], raw_r.at[j, c]).wait()

                @pl.when(rel == 1)
                def _():
                    shift(j, c).start()

                    @pl.when(c == chunks - 1)
                    def _():
                        for k in range(2, chunks):
                            shift(z, k).start()

                @pl.when(c == 0)
                def _():
                    copied(named.at[j], named.at[j], id_r.at[j]).wait()
                    prepare(j, rel)

            to_end = q == 0
            index = jnp.where(to_end, end_index(rel), rel)
            plane = jnp.where(to_end, near, z)
            half = slots // 2
            for h in range(2):
                picked = jnp.dot(
                    onehot[index, h * half : (h + 1) * half, :],
                    blocks[j, c],
                    preferred_element_type=jnp.float32,
                ).astype(jnp.bfloat16)
                dbuf[index, c, h * half : (h + 1) * half, :] = picked

            def give(d, carry):
                i = lax.rem(mine + d, local)
                piece = dbuf.at[index, c, pl.ds(i * capacity, capacity)]
                place = inc.at[j, c, g, pl.ds(y * capacity, capacity)]
                here = jnp.logical_not(to_end) & (d == 0)

                @pl.when(here)
                def _():
                    copied(piece, place, pr.at[j, c]).start()

                @pl.when(jnp.logical_not(here))
                def _():
                    sent(
                        piece,
                        place,
                        ds,
                        pr.at[j, c],
                        (plane * SIDES + i // gates, lax.rem(i, gates)),
                    ).start()

                return carry

            lax.fori_loop(0, local, give, 0)

    def give_back(j):
        ends = (j == 0) | (j == planes - 1)
        joined = ends & (j != z)
        plane = jnp.where(joined, jnp.where(j == 0, 1, planes - 2), j)

        def hand(i, carry):
            side, k = i // gates, lax.rem(i, gates)
            block = obuf.at[j, k, pl.ds(side * capacity, capacity)]
            here = (plane == z) & (i == mine)
            spot = pl.ds(mine * capacity, capacity)

            def hand_to(buffer, sem):
                @pl.when(here)
                def _():
                    copied(block, buffer.at[z, spot], sem.at[z]).start()

                @pl.when(jnp.logical_not(here))
                def _():
                    sent(
                        block, buffer.at[z, spot], rs, sem.at[z], (plane * SIDES + side, k)
                    ).start()

            @pl.when(joined)
            def _():
                hand_to(edge_ret, er)

            @pl.when(jnp.logical_not(joined))
            def _():
                hand_to(ret, rr)

            return carry

        lax.fori_loop(0, local, hand, 0)

    def expert(s, q):
        t = s - 1
        order = jnp.where(edge, jnp.maximum(t - chunks, 0), jnp.minimum(t, len(ORDER) - 1))
        rel, c = listed(order)
        second = q == 1
        first_own = edge & (t < chunks)
        rel = jnp.where(
            first_own, 1, jnp.where(second, jnp.where(t < 5, 1, 0), rel)
        )
        c = jnp.where(
            first_own, t, jnp.where(second, jnp.where(t < 5, t - 1, chunks - 1), c)
        )
        valid = jnp.where(
            edge,
            (q == 0) & (t >= 0) & (t < len(ORDER) + chunks),
            jnp.where(q == 0, (t >= 0) & (t < len(ORDER) - 1), (t >= 1) & (t <= 5)),
        )

        @pl.when(valid)
        def _():
            j = plane_of(rel)
            copied(inc.at[j, c], inc.at[j, c], pr.at[j, c]).wait()
            share = width * chunks
            tile = 256
            for n in range(hidden.shape[2] // tile):
                cols = slice(n * tile, (n + 1) * tile)
                acc = jnp.zeros((SIDES * capacity, tile), jnp.float32)
                for k in range(gates):
                    start = pl.multiple_of(k * share + c * width, width)
                    acc += jnp.dot(
                        inc[j, c, k],
                        upv[pl.ds(start, width), cols],
                        preferred_element_type=jnp.float32,
                    )

                @pl.when(c == 0)
                def _():
                    hidden[j, :, cols] = acc

                @pl.when(c != 0)
                def _():
                    hidden[j, :, cols] += acc

            @pl.when(c == chunks - 1)
            def _():
                active = jnp.maximum(hidden[j], 0.0).astype(jnp.bfloat16)
                out_width = downv.shape[1] // gates
                for k in range(gates):
                    obuf[j, k] = jnp.dot(
                        active,
                        downv[:, k * out_width : (k + 1) * out_width],
                        preferred_element_type=jnp.float32,
                    ).astype(jnp.bfloat16)
                give_back(j)

    edge_route = sent(factor, edge_factor, fs, fr, (inner * SIDES + y, g))

    def step(s, carry):
        def dispatch_one(q, carry):
            dispatch(s, q)
            return carry

        lax.fori_loop(0, 3, dispatch_one, 0)

        @pl.when(s == 0)
        def _():
            partial = 0.0
            for c in range(chunks):
                partial += lax.dot_general(
                    gate_weight[:, c * width : (c + 1) * width],
                    blocks[z, c],
                    (((1,), (1,)), ((), ())),
                    preferred_element_type=jnp.float32,
                )
            logits[g] = partial
            for copy in gate_routes:
                copy.start()
            for copy in weights:
                copy.wait()

        @pl.when(s == 2)
        def _():
            for copy in gate_routes:
                copy.wait_recv()
            summed = logits[0]
            for k in range(1, gates):
                summed += logits[k]
            top = jnp.max(summed, axis=0, keepdims=True)
            terms = jnp.exp(summed - top)
            mask = ids[2:3, :].astype(jnp.float32)
            scale = mask / jnp.sum(terms, axis=0, keepdims=True)
            factor[...] = total * terms * scale

            @pl.when(edge)
            def _():
                edge_route.start()

        def expert_one(q, carry):
            expert(s, q)
            return carry

        lax.fori_loop(0, 2, expert_one, 0)
        return carry

    lax.fori_loop(0, len(ORDER) + chunks + 1, step, 0)

    def join(j, p, weight, returned, sem, index, first):
        ranks = lax.broadcasted_iota(jnp.int32, (capacity, rows), 0).astype(jnp.float32)

        def one(i, carry):
            line = places[j, pl.ds(p * local + i, 1), :]
            scale = weight[pl.ds(p * local + i, 1), :]
            select[pl.ds(pl.multiple_of(i * capacity, capacity), capacity), :] = jnp.where(
                line == ranks, scale, 0.0
            ).astype(jnp.bfloat16)
            return carry

        lax.fori_loop(0, local, one, 0)
        copied(returned.at[p], returned.at[p], sem.at[p]).wait()
        found = lax.dot_general(
            select[...],
            returned[p],
            (((0,), (0,)), ((), ())),
            preferred_element_type=jnp.float32,
        )

        @pl.when(first)
        def _():
            mixed[index] = found

        @pl.when(jnp.logical_not(first))
        def _():
            mixed[index] += found

    part_route = sent(part, taken, ts, tr, (near * SIDES + y, g))

    @pl.when(middle)
    def _():
        copied(edge_factor, edge_factor, fr).wait()

        def for_edge(k, carry):
            p = table((mid, mid + toward, far), k)
            join(near, p, edge_factor, edge_ret, er, 0, k == 0)
            return carry

        lax.fori_loop(0, planes - 1, for_edge, 0)
        part[...] = mixed[0].astype(jnp.bfloat16)
        part_route.start()

    def for_own(k, carry):
        p = jnp.where(edge, z, table((mid, mid + toward, far, near), k))
        join(z, p, factor, ret, rr, 1, k == 0)
        return carry

    lax.fori_loop(0, jnp.where(edge, 1, planes), for_own, 0)

    @pl.when(edge)
    def _():
        copied(taken, taken, tr).wait()
        out[...] = (mixed[1] + taken[...].astype(jnp.float32)).astype(jnp.bfloat16)

    @pl.when(middle)
    def _():
        out[...] = mixed[1].astype(jnp.bfloat16)
        part_route.wait_send()

    for copy in gate_routes:
        copy.wait_send()
    ids_to(toward, id_s.at[0]).wait_send()
    for c in range(chunks):
        shift(z, c).wait_send()
    handed = ret.at[pl.ds(0, planes - 1)]
    within = dbuf.at[0, :, pl.ds(0, slots - capacity)]
    piece = ret.at[0, pl.ds(0, (local - 2) * capacity)]
    last = ret.at[0, pl.ds(0, capacity)]
    copied(handed, handed, rs).wait()
    copied(piece, piece, rs).wait()
    copied(within, within, ds).wait()

    @pl.when(edge)
    def _():
        copied(last, last, rs).wait()
        ids_to(2 * toward, id_s.at[1]).wait_send()
        edge_route.wait_send()

    @pl.when(middle)
    def _():
        for c in range(chunks):
            shift(near, c).wait_send()
        others = dbuf.at[pl.ds(0, planes - 1), :, pl.ds(0, slots - capacity)]
        copied(others, others, ds).wait()
        ahead = dbuf.at[pl.ds(planes, planes - 1)]
        copied(ahead, ahead, ds).wait()


def exchange(samples, ids, gate_weight, up, down, planes, gates, capacity):
    rows, share = samples.shape
    local = SIDES * gates
    total = planes * local
    width = share // CHUNKS
    depth, inner = up.shape[1:]
    outer = down.shape[2]
    out_width = outer // gates
    bf16, f32 = jnp.bfloat16, jnp.float32
    dma = pltpu.SemaphoreType.DMA
    vmem = pl.BlockSpec(memory_space=pltpu.VMEM)
    hbm = pl.BlockSpec(memory_space=pl.ANY)
    slots = local * capacity
    kinds = 2 * planes - 1
    return pl.pallas_call(
        functools.partial(exchange_kernel, gates, capacity),
        out_shape=jax.ShapeDtypeStruct((rows, out_width), bf16),
        in_specs=[hbm, vmem, vmem, hbm, hbm],
        out_specs=vmem,
        scratch_shapes=[
            pltpu.VMEM((planes, CHUNKS, rows, width), bf16),
            pltpu.VMEM((planes,) + ids.shape, jnp.int32),
            pltpu.VMEM((planes, total, rows), f32),
            pltpu.VMEM((rows, rows), bf16),
            pltpu.VMEM((kinds, slots, rows), bf16),
            pltpu.VMEM((kinds, CHUNKS, slots, width), bf16),
            pltpu.VMEM((planes, CHUNKS, gates, SIDES * capacity, width), bf16),
            pltpu.VMEM((depth, inner), bf16),
            pltpu.VMEM((inner, outer), bf16),
            pltpu.VMEM((planes, SIDES * capacity, inner), f32),
            pltpu.VMEM((planes, gates, SIDES * capacity, out_width), bf16),
            pltpu.VMEM((gates, total, rows), f32),
            pltpu.VMEM((total, rows), f32),
            pltpu.VMEM((total, rows), f32),
            pltpu.VMEM((planes, slots, out_width), bf16),
            pltpu.VMEM((planes, slots, out_width), bf16),
            pltpu.VMEM((slots, rows), bf16),
            pltpu.VMEM((2, rows, out_width), f32),
            pltpu.VMEM((rows, out_width), bf16),
            pltpu.VMEM((rows, out_width), bf16),
            dma((CHUNKS,)),
            dma((2,)),
            dma((planes, CHUNKS)),
            dma((planes, CHUNKS)),
            dma((2,)),
            dma((planes,)),
            dma,
            dma((planes, CHUNKS)),
            dma,
            dma((planes,)),
            dma((planes,)),
            dma((gates,)),
            dma((gates,)),
            dma,
            dma,
            dma,
            dma,
        ],
        compiler_params=pltpu.CompilerParams(
            collective_id=0, has_side_effects=True, vmem_limit_bytes=63 << 20
        ),
    )(samples, ids, gate_weight, up, down)


def in_one_kernel(samples, gate_weight, expert_ids, pad_mask, up_weight, down_weight):
    group_count = lax.axis_size("expert")
    gate_count = lax.axis_size("gate")
    expert_count = group_count * gate_count
    capacity = 4 * samples.shape[0] // expert_count
    ids = jnp.concatenate([expert_ids.T, pad_mask[None, :]], axis=0)
    ids = jnp.pad(ids, ((0, 8 - ids.shape[0]), (0, 0)))
    return exchange(
        samples,
        ids,
        gate_weight.T,
        up_weight,
        down_weight,
        group_count // SIDES,
        gate_count,
        capacity,
    )


def fits(samples, up_weight, down_weight):
    group_count = lax.axis_size("expert")
    capacity = 4 * samples.shape[0] // (group_count * lax.axis_size("gate"))
    planes = group_count // SIDES
    held = 2 * (planes * samples.size * 3 + up_weight.size + down_weight.size)
    return planes == 4 and group_count % SIDES == 0 and capacity % 16 == 0 and held < 40 << 20


def per_device(samples, gate_weight, expert_ids, pad_mask, up_weight, down_weight):
    if fits(samples, up_weight, down_weight):
        return in_one_kernel(
            samples, gate_weight, expert_ids, pad_mask, up_weight, down_weight
        )
    row_count, share = samples.shape
    group_count = lax.axis_size("expert")
    gate_count = lax.axis_size("gate")
    expert_count = group_count * gate_count
    capacity = 4 * row_count // expert_count
    partial = jnp.dot(samples, gate_weight, preferred_element_type=jnp.float32)
    logits = jnp.sum(lax.all_gather(partial, "gate"), axis=0)
    first, second, member, before = routing(expert_ids, expert_count)
    place = jnp.where(member, before, -1).T
    ranks = jnp.arange(capacity, dtype=jnp.int32)
    send = (place[:, None, :] == ranks[None, :, None]).astype(jnp.bfloat16)
    outgoing = jnp.dot(
        send.reshape(expert_count * capacity, row_count), samples, preferred_element_type=jnp.float32
    ).astype(jnp.bfloat16)
    incoming = lax.all_to_all(
        outgoing.reshape(expert_count, capacity, share),
        ("expert", "gate"),
        split_axis=0,
        concat_axis=0,
        tiled=True,
    ).reshape(group_count, gate_count, capacity, share)
    hidden = 0.0
    for g in range(gate_count):
        hidden += jnp.dot(
            incoming[:, g].reshape(group_count * capacity, share),
            up_weight[0, g * share : (g + 1) * share],
            preferred_element_type=jnp.float32,
        )
    active = jnp.maximum(hidden, 0.0).astype(jnp.bfloat16)
    expert_out = jnp.dot(active, down_weight[0], preferred_element_type=jnp.float32).astype(
        jnp.bfloat16
    )
    out_share = expert_out.shape[1] // gate_count
    outbound = expert_out.reshape(group_count, capacity, gate_count, out_share)
    outbound = outbound.transpose(0, 2, 1, 3).reshape(expert_count, capacity, out_share)
    returned = lax.all_to_all(
        outbound, ("expert", "gate"), split_axis=0, concat_axis=0, tiled=True
    ).reshape(expert_count * capacity, out_share)
    factor0, factor1 = factors(logits, first, second, pad_mask, expert_count)
    slots = jnp.arange(expert_count * capacity, dtype=jnp.int32)[None, :]
    mixed = 0.0
    for k, (chosen, factor) in enumerate(((first, factor0), (second, factor1))):
        rank = jnp.sum(jnp.where(chosen, before, 0), axis=1, keepdims=True)
        position = expert_ids[:, k : k + 1] * capacity + rank
        pick = (position == slots).astype(jnp.bfloat16)
        mixed += factor * jnp.dot(pick, returned, preferred_element_type=jnp.float32)
    return mixed.astype(jnp.bfloat16)


def solution(mesh):
    placed = (
        P("expert", "gate"),
        P("gate", None),
        P("expert", None),
        P("expert"),
        P(("expert", "gate"), None, None),
        P(("expert", "gate"), None, None),
    )
    return jax.shard_map(
        per_device, mesh=mesh, in_specs=placed, out_specs=P("expert", "gate"), check_vma=False
    )
```

```python
import functools

import jax
import jax.numpy as jnp
from jax import lax
from jax.experimental import pallas as pl
from jax.experimental.pallas import tpu as pltpu
from jax.sharding import PartitionSpec as P


MESH = pl.DeviceIdType.MESH
CHUNKS = 4
SIDES = 2
PARTS = 2


def routing(expert_ids, expert_count):
    row_count = expert_ids.shape[0]
    lanes = jnp.arange(expert_count, dtype=jnp.int32)[None, :]
    first = expert_ids[:, 0:1] == lanes
    second = expert_ids[:, 1:2] == lanes
    member = first | second
    rows = jnp.arange(row_count, dtype=jnp.int32)
    lower = (rows[:, None] > rows[None, :]).astype(jnp.bfloat16)
    before = jnp.dot(lower, member.astype(jnp.bfloat16), preferred_element_type=jnp.float32)
    before = before.astype(jnp.int32)
    return first, second, member, before


def factors(logits, first, second, pad_mask, expert_count):
    top = jnp.max(logits, axis=1, keepdims=True)
    terms = jnp.exp(logits - top)
    scale = pad_mask.astype(jnp.float32)[:, None] / jnp.sum(terms, axis=1, keepdims=True)
    factor0 = expert_count * jnp.sum(jnp.where(first, terms, 0.0), axis=1, keepdims=True) * scale
    factor1 = expert_count * jnp.sum(jnp.where(second, terms, 0.0), axis=1, keepdims=True) * scale
    return factor0, factor1


def copied(source, target, sem):
    return pltpu.make_async_copy(source, target, sem)


def sent(source, target, send_sem, recv_sem, device):
    return pltpu.make_async_remote_copy(
        src_ref=source,
        dst_ref=target,
        send_sem=send_sem,
        recv_sem=recv_sem,
        device_id=device,
        device_id_type=MESH,
    )


def table(values, index):
    out = values[0]
    for k in range(1, len(values)):
        out = jnp.where(index == k, values[k], out)
    return out


NONE, WAIT, END, LOCAL, EXPERT, LOGITS, FACTOR, JOIN_EDGE, JOIN, END_PART, EXPERT_PART, WEIGHTS = range(12)
OWN, EDGE, INNER, FAR = range(4)


def coded(*jobs):
    return [kind * 16 + rel * 4 + c for kind, rel, c in jobs]


MIDDLE_JOBS = coded(
    (END, OWN, 0),
    (LOGITS, OWN, 0),
    (LOCAL, OWN, 0),
    (LOCAL, OWN, 1),
    (LOCAL, OWN, 2),
    (LOCAL, OWN, 3),
    (END, OWN, 1),
    (WEIGHTS, OWN, 0),
    (EXPERT, OWN, 0),
    (FACTOR, OWN, 0),
    (WAIT, EDGE, 0),
    (LOCAL, EDGE, 0),
    (WAIT, INNER, 0),
    (END, INNER, 0),
    (LOCAL, INNER, 0),
    (EXPERT, OWN, 1),
    (EXPERT, OWN, 2),
    (WAIT, EDGE, 1),
    (LOCAL, EDGE, 1),
    (WAIT, INNER, 1),
    (END, INNER, 1),
    (LOCAL, INNER, 1),
    (EXPERT, OWN, 3),
    (EXPERT, EDGE, 0),
    (WAIT, EDGE, 2),
    (LOCAL, EDGE, 2),
    (WAIT, FAR, 0),
    (END, FAR, 0),
    (LOCAL, FAR, 0),
    (EXPERT, INNER, 0),
    (EXPERT, EDGE, 1),
    (WAIT, EDGE, 3),
    (LOCAL, EDGE, 3),
    (WAIT, FAR, 1),
    (END, FAR, 1),
    (LOCAL, FAR, 1),
    (EXPERT, INNER, 1),
    (WAIT, FAR, 2),
    (END, FAR, 2),
    (LOCAL, FAR, 2),
    (EXPERT, EDGE, 2),
    (WAIT, FAR, 3),
    (END, FAR, 3),
    (LOCAL, FAR, 3),
    (EXPERT, FAR, 0),
    (EXPERT, EDGE, 3),
    (EXPERT, FAR, 1),
    (WAIT, INNER, 2),
    (END, INNER, 2),
    (LOCAL, INNER, 2),
    (EXPERT, FAR, 2),
    (EXPERT, FAR, 3),
    (WAIT, INNER, 3),
    (END, INNER, 3),
    (LOCAL, INNER, 3),
    (END, OWN, 2),
    (END_PART, OWN, 0),
    (END_PART, OWN, 1),
    (EXPERT, INNER, 2),
    (EXPERT, INNER, 3),
    (JOIN_EDGE, OWN, 0),
    (JOIN_EDGE, INNER, 0),
    (JOIN_EDGE, FAR, 0),
    (JOIN, OWN, 0),
    (JOIN, INNER, 0),
    (JOIN, FAR, 0),
    (JOIN, EDGE, 0),
)
EDGE_JOBS = coded(
    (LOCAL, EDGE, 0),
    (LOGITS, EDGE, 0),
    (LOCAL, EDGE, 1),
    (LOCAL, EDGE, 2),
    (LOCAL, EDGE, 3),
    (WEIGHTS, EDGE, 0),
    (EXPERT, EDGE, 0),
    (FACTOR, EDGE, 0),
    (EXPERT, EDGE, 1),
    (EXPERT, OWN, 0),
    (EXPERT, EDGE, 2),
    (EXPERT, OWN, 1),
    (EXPERT, EDGE, 3),
    (EXPERT, INNER, 0),
    (EXPERT, INNER, 1),
    (EXPERT, FAR, 0),
    (EXPERT, FAR, 1),
    (EXPERT, FAR, 2),
    (EXPERT, FAR, 3),
    (EXPERT, INNER, 2),
    (EXPERT, INNER, 3),
    (EXPERT, OWN, 2),
    (EXPERT_PART, OWN, 0),
    (EXPERT_PART, OWN, 1),
    (JOIN, EDGE, 0),
)


def exchange_kernel(
    gates,
    capacity,
    samples,
    ids,
    pads,
    gate_weight,
    up,
    down,
    out,
    blocks,
    named,
    mask,
    gatev,
    places,
    lower,
    onehot,
    dbuf,
    inc,
    upv,
    downv,
    hidden,
    obuf,
    logits,
    factor,
    edge_factor,
    ret,
    edge_ret,
    select,
    mixed,
    part,
    taken,
    own_sem,
    w_sem,
    in_sem,
    raw_s,
    raw_r,
    id_s,
    id_r,
    ds,
    pr,
    ph,
    rs,
    rr,
    er,
    gs,
    gr,
    fs,
    fr,
    ts,
    tr,
):
    chunks = CHUNKS
    local = SIDES * gates
    planes = blocks.shape[0]
    total = planes * local
    rows = blocks.shape[2]
    width = blocks.shape[3]
    share = width * chunks
    slots = local * capacity
    few = capacity // PARTS
    bf16, f32 = jnp.bfloat16, jnp.float32
    e = lax.axis_index("expert")
    g = lax.axis_index("gate")
    z = e // SIDES
    y = lax.rem(e, SIDES)
    mine = y * gates + g
    low = z < planes // 2
    toward = jnp.where(low, 1, -1)
    near = jnp.where(low, 0, planes - 1)
    far = planes - 1 - near
    edge = z == near
    middle = jnp.logical_not(edge)
    mid = near + toward
    inner = z + toward

    def plane_of(rel):
        return table((mid, near, mid + toward, far), rel)

    def at(plane, i):
        return (plane * SIDES + i // gates, lax.rem(i, gates))

    barrier = pltpu.get_barrier_semaphore()

    def greet(d, carry):
        plane = z - 1 + d // local
        i = lax.rem(mine + d, local)

        @pl.when((plane >= 0) & (plane < planes) & (d != local))
        def _():
            pl.semaphore_signal(barrier, inc=1, device_id=at(plane, i), device_id_type=MESH)

        return carry

    with jax.named_scope("greet"):
        lax.fori_loop(0, 3 * local, greet, 0)
    greeted = jnp.where(edge, 2, 3) * local - 1

    inputs = (
        copied(ids, named.at[z], in_sem.at[0]),
        copied(pads, mask, in_sem.at[1]),
        copied(gate_weight, gatev, in_sem.at[2]),
    )
    for copy in inputs:
        copy.start()
    own = [
        copied(samples.at[:, pl.ds(c * width, width)], blocks.at[z, c], own_sem.at[c])
        for c in range(chunks)
    ]
    for copy in own:
        copy.start()
    weights = [copied(down.at[0], downv, w_sem.at[0])]
    for c in range(chunks):
        for k in range(gates):
            weights.append(
                copied(
                    up.at[0, pl.ds(k * share + c * width, width)],
                    upv.at[c, pl.ds(k * width, width)],
                    w_sem.at[1 + c * gates + k],
                )
            )

    earlier = lax.broadcasted_iota(jnp.int32, (rows, rows), 0)
    later = lax.broadcasted_iota(jnp.int32, (rows, rows), 1)
    with jax.named_scope("lower"):
        lower[...] = jnp.where(earlier < later, 1.0, 0.0).astype(bf16)

    def end_index(rel):
        return jnp.where(rel == OWN, planes, planes - 1 + rel)

    def prepare(j, rel):
        lanes = lax.broadcasted_iota(jnp.int32, (total, rows), 0)
        member = (named[j, 0:1, :] == lanes) | (named[j, 1:2, :] == lanes)
        flags = jnp.where(member, 1.0, 0.0).astype(bf16)
        before = jnp.dot(flags, lower[...], preferred_element_type=f32)
        places[j] = jnp.where(member, before, -1.0)
        ranks = lax.broadcasted_iota(jnp.int32, (capacity, rows), 0).astype(f32)

        def build(index, plane):
            def one(i, carry):
                line = places[j, pl.ds(plane * local + i, 1), :]
                found = jnp.where(line == ranks, 1.0, 0.0).astype(bf16)
                onehot[index, :, i] = found.reshape(PARTS, few, rows)
                return carry

            lax.fori_loop(0, local, one, 0)

        @pl.when(middle & (rel != EDGE))
        def _():
            build(end_index(rel), near)

        build(rel, z)

    with jax.named_scope("inputs"):
        for copy in inputs:
            copy.wait()
    with jax.named_scope("prepare"):
        prepare(z, jnp.where(edge, EDGE, OWN))
    with jax.named_scope("samples"):
        for copy in own:
            copy.wait()
    with jax.named_scope("barrier"):
        pl.semaphore_wait(barrier, greeted)

    def ids_on(j, sem):
        return sent(named.at[j], named.at[j], sem, id_r.at[j], at(inner, mine))

    def shift(j, c):
        return sent(
            blocks.at[j, c], blocks.at[j, c], raw_s.at[j, c], raw_r.at[j, c], at(inner, mine)
        )

    ids_on(z, id_s.at[0]).start()
    for c in range(2):
        shift(z, c).start()

    @pl.when(edge)
    def _():
        for c in range(2, chunks):
            shift(z, c).start()

    for copy in weights:
        copy.start()
    gate_routes = []
    for d in range(1, gates):
        t = lax.rem(g + d, gates)
        gate_routes.append(sent(logits.at[g], logits.at[g], gs.at[d - 1], gr.at[d - 1], (e, t)))
    edge_route = sent(factor, edge_factor, fs, fr, at(inner, mine))
    part_route = sent(part, taken, ts, tr, at(near, mine))

    def wait(j, rel, c):
        with jax.named_scope("wait_raw"):
            copied(blocks.at[j, c], blocks.at[j, c], raw_r.at[j, c]).wait()

        @pl.when(c == 0)
        def _():
            copied(named.at[j], named.at[j], id_r.at[j]).wait()

        @pl.when(rel == EDGE)
        def _():
            @pl.when(c == 0)
            def _():
                ids_on(j, id_s.at[1]).start()

            shift(j, c).start()

            @pl.when(c == chunks - 1)
            def _():
                for k in range(2, chunks):
                    shift(z, k).start()

        @pl.when(c == 0)
        def _():
            prepare(j, rel)

    def pick(index, part, j, c):
        dbuf[index, c, part] = (
            jnp.dot(
                onehot[index, part].reshape(local * few, rows),
                blocks[j, c],
                preferred_element_type=f32,
            )
            .astype(bf16)
            .reshape(local, few, width)
        )

    def dispatch(j, rel, c, to_end):
        index = jnp.where(to_end, end_index(rel), rel)
        plane = jnp.where(to_end, near, z)
        with jax.named_scope("pick"):
            for part in range(PARTS):
                pick(index, part, j, c)

        def give(d, carry):
            i = lax.rem(mine + d, local)
            piece = dbuf.at[index, c, :, i]
            place = inc.at[j, c, y, :, :, pl.ds(g * width, width)]
            here = jnp.logical_not(to_end) & (d == 0)

            @pl.when(here)
            def _():
                copied(piece, place, pr.at[j, c]).start()

            @pl.when(jnp.logical_not(here))
            def _():
                sent(piece, place, ds, pr.at[j, c], at(plane, i)).start()

            return carry

        lax.fori_loop(0, local, give, 0)

    def dispatch_part(part):
        c = chunks - 1
        pick(planes, part, z, c)

        def give(d, carry):
            i = lax.rem(mine + d, local)
            sent(
                dbuf.at[planes, c, part, i],
                inc.at[z, c, y, part, :, pl.ds(g * width, width)],
                ds,
                ph.at[part],
                at(near, i),
            ).start()
            return carry

        lax.fori_loop(0, local, give, 0)

    def give_back(j, part):
        ends = (j == 0) | (j == planes - 1)
        joined = ends & (j != z)
        plane = jnp.where(joined, jnp.where(j == 0, 1, planes - 2), j)

        def hand(d, carry):
            i = lax.rem(mine + d, local)
            side, k = i // gates, lax.rem(i, gates)
            here = (plane == z) & (d == 0)

            def hand_to(buffer, sem):
                if part is None:
                    block, spot = obuf.at[j, k, side], buffer.at[z, mine]
                else:
                    block, spot = obuf.at[j, k, side, part], buffer.at[z, mine, part]

                @pl.when(here)
                def _():
                    copied(block, spot, sem.at[z]).start()

                @pl.when(jnp.logical_not(here))
                def _():
                    sent(block, spot, rs, sem.at[z], at(plane, i)).start()

            @pl.when(joined)
            def _():
                hand_to(edge_ret, er)

            @pl.when(jnp.logical_not(joined))
            def _():
                hand_to(ret, rr)

            return carry

        lax.fori_loop(0, local, hand, 0)

    tile = 256
    inner_tiles = [slice(n, n + tile) for n in range(0, hidden.shape[4], tile)]
    out_width = downv.shape[1] // gates

    def expert(j, c):
        with jax.named_scope("wait_inc"):
            copied(inc.at[j, c], inc.at[j, c], pr.at[j, c]).wait()
        taken_in = inc[j, c].reshape(SIDES * capacity, share)
        for cols in inner_tiles:
            acc = jnp.dot(taken_in, upv[c, :, cols], preferred_element_type=f32)
            acc = acc.reshape(SIDES, PARTS, few, tile)

            @pl.when(c == 0)
            def _():
                hidden[j, :, :, :, cols] = acc

            @pl.when(c != 0)
            def _():
                hidden[j, :, :, :, cols] += acc

        @pl.when(c == chunks - 1)
        def _():
            active = jnp.maximum(hidden[j], 0.0).astype(bf16).reshape(SIDES * capacity, -1)
            for k in range(gates):
                obuf[j, k] = (
                    jnp.dot(
                        active,
                        downv[:, k * out_width : (k + 1) * out_width],
                        preferred_element_type=f32,
                    )
                    .astype(bf16)
                    .reshape(SIDES, PARTS, few, out_width)
                )
            with jax.named_scope("back"):
                give_back(j, None)

    def expert_part(j, part):
        c = chunks - 1
        with jax.named_scope("wait_part"):
            arriving = inc.at[j, c, :, part]
            copied(arriving, arriving, ph.at[part]).wait()
        taken_in = inc[j, c, :, part].reshape(SIDES * few, share)
        active = []
        for cols in inner_tiles:
            acc = jnp.dot(taken_in, upv[c, :, cols], preferred_element_type=f32)
            acc += hidden[j, :, part, :, cols].reshape(SIDES * few, tile)
            active.append(jnp.maximum(acc, 0.0).astype(bf16))
        active = jnp.concatenate(active, axis=1)
        for k in range(gates):
            obuf[j, k, :, part] = (
                jnp.dot(
                    active,
                    downv[:, k * out_width : (k + 1) * out_width],
                    preferred_element_type=f32,
                )
                .astype(bf16)
                .reshape(SIDES, few, out_width)
            )
        with jax.named_scope("back"):
            give_back(j, part)

    def gate_logits():
        partial = 0.0
        for c in range(chunks):
            partial += lax.dot_general(
                gatev[:, c * width : (c + 1) * width],
                blocks[z, c],
                (((1,), (1,)), ((), ())),
                preferred_element_type=f32,
            )
        logits[g] = partial
        for copy in gate_routes:
            copy.start()

    def gate_factor():
        with jax.named_scope("wait_gate"):
            for copy in gate_routes:
                copy.wait_recv()
        summed = logits[0]
        for k in range(1, gates):
            summed += logits[k]
        top = jnp.max(summed, axis=0, keepdims=True)
        terms = jnp.exp(summed - top)
        scale = mask[...].astype(f32).reshape(1, rows) / jnp.sum(terms, axis=0, keepdims=True)
        factor[...] = total * terms * scale

        @pl.when(edge)
        def _():
            edge_route.start()

    def join(j, p, weight, returned, sem, index, first):
        ranks = lax.broadcasted_iota(jnp.int32, (capacity, rows), 0).astype(f32)

        def one(i, carry):
            line = places[j, pl.ds(p * local + i, 1), :]
            scale = weight[pl.ds(p * local + i, 1), :]
            select[pl.ds(pl.multiple_of(i * capacity, capacity), capacity), :] = jnp.where(
                line == ranks, scale, 0.0
            ).astype(bf16)
            return carry

        lax.fori_loop(0, local, one, 0)
        with jax.named_scope("wait_ret"):
            copied(returned.at[p], returned.at[p], sem.at[p]).wait()
        found = lax.dot_general(
            select[...],
            returned[p].reshape(slots, out_width),
            (((0,), (0,)), ((), ())),
            preferred_element_type=f32,
        )

        @pl.when(first)
        def _():
            mixed[index] = found

        @pl.when(jnp.logical_not(first))
        def _():
            mixed[index] += found

    def job(t, carry):
        code = jnp.where(edge, table(EDGE_JOBS, t), table(MIDDLE_JOBS, t))
        kind, rel, c = code // 16, lax.rem(code // 4, 4), lax.rem(code, 4)
        j = plane_of(rel)

        @pl.when(kind == WAIT)
        def _():
            wait(j, rel, c)

        @pl.when((kind == END) | (kind == LOCAL))
        def _():
            dispatch(j, rel, c, kind == END)

        @pl.when(kind == EXPERT)
        def _():
            expert(j, c)

        @pl.when(kind == END_PART)
        def _():
            dispatch_part(c)

        @pl.when(kind == EXPERT_PART)
        def _():
            expert_part(j, c)

        @pl.when(kind == WEIGHTS)
        def _():
            with jax.named_scope("wait_w"):
                for copy in weights:
                    copy.wait()

        @pl.when(kind == LOGITS)
        def _():
            gate_logits()

        @pl.when(kind == FACTOR)
        def _():
            gate_factor()

        @pl.when(kind == JOIN_EDGE)
        def _():
            @pl.when(rel == OWN)
            def _():
                copied(edge_factor, edge_factor, fr).wait()

            join(near, j, edge_factor, edge_ret, er, 0, rel == OWN)

            @pl.when(rel == FAR)
            def _():
                part[...] = mixed[0].astype(bf16)
                part_route.start()

        @pl.when(kind == JOIN)
        def _():
            join(z, j, factor, ret, rr, 1, edge | (rel == OWN))

        return carry

    lax.fori_loop(0, jnp.where(edge, len(EDGE_JOBS), len(MIDDLE_JOBS)), job, 0)

    @pl.when(edge)
    def _():
        with jax.named_scope("wait_taken"):
            copied(taken, taken, tr).wait()
        out[...] = (mixed[1] + taken[...].astype(f32)).astype(bf16)

    @pl.when(middle)
    def _():
        out[...] = mixed[1].astype(bf16)

    for copy in gate_routes:
        copy.wait_send()
    ids_on(z, id_s.at[0]).wait_send()
    for c in range(chunks):
        shift(z, c).wait_send()
    within = dbuf.at[EDGE, :, :, pl.ds(0, local - 1)]
    copied(within, within, ds).wait()
    handed = ret.at[pl.ds(0, planes - 1)]
    few_more = ret.at[0, pl.ds(0, local - 2)]
    one_more = ret.at[0, 0]
    copied(handed, handed, rs).wait()
    copied(few_more, few_more, rs).wait()

    @pl.when(edge)
    def _():
        copied(one_more, one_more, rs).wait()
        edge_route.wait_send()

    @pl.when(middle)
    def _():
        part_route.wait_send()
        ids_on(near, id_s.at[1]).wait_send()
        for c in range(chunks):
            shift(near, c).wait_send()
        others = dbuf.at[pl.ds(0, planes - 1), :, :, pl.ds(0, local - 1)]
        copied(others, others, ds).wait()
        ahead = dbuf.at[pl.ds(planes, planes - 1)]
        copied(ahead, ahead, ds).wait()


def exchange(samples, ids, pads, gate_weight, up, down, planes, gates, capacity):
    rows, share = samples.shape
    local = SIDES * gates
    total = planes * local
    width = share // CHUNKS
    depth, inner = up.shape[1:]
    outer = down.shape[2]
    out_width = outer // gates
    bf16, f32 = jnp.bfloat16, jnp.float32
    dma = pltpu.SemaphoreType.DMA
    hbm = pl.BlockSpec(memory_space=pl.ANY)
    slots = local * capacity
    few = capacity // PARTS
    kinds = 2 * planes - 1
    return pl.pallas_call(
        functools.partial(exchange_kernel, gates, capacity),
        out_shape=pltpu.VMEM((rows, out_width), bf16),
        in_specs=[hbm] * 6,
        out_specs=pl.BlockSpec(memory_space=pltpu.VMEM),
        scratch_shapes=[
            pltpu.VMEM((planes, CHUNKS, rows, width), bf16),
            pltpu.VMEM((planes,) + ids.shape, jnp.int32),
            pltpu.VMEM(pads.shape, jnp.int32),
            pltpu.VMEM(gate_weight.shape, bf16),
            pltpu.VMEM((planes, total, rows), f32),
            pltpu.VMEM((rows, rows), bf16),
            pltpu.VMEM((kinds, PARTS, local, few, rows), bf16),
            pltpu.VMEM((kinds, CHUNKS, PARTS, local, few, width), bf16),
            pltpu.VMEM((planes, CHUNKS, SIDES, PARTS, few, gates * width), bf16),
            pltpu.VMEM((CHUNKS, depth // CHUNKS, inner), bf16),
            pltpu.VMEM((inner, outer), bf16),
            pltpu.VMEM((planes, SIDES, PARTS, few, inner), f32),
            pltpu.VMEM((planes, gates, SIDES, PARTS, few, out_width), bf16),
            pltpu.VMEM((gates, total, rows), f32),
            pltpu.VMEM((total, rows), f32),
            pltpu.VMEM((total, rows), f32),
            pltpu.VMEM((planes, local, PARTS, few, out_width), bf16),
            pltpu.VMEM((planes, local, PARTS, few, out_width), bf16),
            pltpu.VMEM((slots, rows), bf16),
            pltpu.VMEM((2, rows, out_width), f32),
            pltpu.VMEM((rows, out_width), bf16),
            pltpu.VMEM((rows, out_width), bf16),
            dma((CHUNKS,)),
            dma((1 + CHUNKS * gates,)),
            dma((3,)),
            dma((planes, CHUNKS)),
            dma((planes, CHUNKS)),
            dma((2,)),
            dma((planes,)),
            dma,
            dma((planes, CHUNKS)),
            dma((PARTS,)),
            dma,
            dma((planes,)),
            dma((planes,)),
            dma((gates,)),
            dma((gates,)),
            dma,
            dma,
            dma,
            dma,
        ],
        compiler_params=pltpu.CompilerParams(
            collective_id=0, has_side_effects=True, vmem_limit_bytes=58 << 20
        ),
    )(samples, ids, pads, gate_weight, up, down)


def in_one_kernel(samples, gate_weight, expert_ids, pad_mask, up_weight, down_weight):
    group_count = lax.axis_size("expert")
    gate_count = lax.axis_size("gate")
    expert_count = group_count * gate_count
    return exchange(
        samples,
        expert_ids.T,
        pad_mask,
        gate_weight.T,
        up_weight,
        down_weight,
        group_count // SIDES,
        gate_count,
        4 * samples.shape[0] // expert_count,
    )


def fits(samples, up_weight, down_weight):
    group_count = lax.axis_size("expert")
    capacity = 4 * samples.shape[0] // (group_count * lax.axis_size("gate"))
    planes = group_count // SIDES
    held = 2 * (planes * samples.size * 3 + up_weight.size + down_weight.size)
    return planes == 4 and group_count % SIDES == 0 and capacity % (16 * PARTS) == 0 and held < 40 << 20


def per_device(samples, gate_weight, expert_ids, pad_mask, up_weight, down_weight):
    if fits(samples, up_weight, down_weight):
        return in_one_kernel(
            samples, gate_weight, expert_ids, pad_mask, up_weight, down_weight
        )
    row_count, share = samples.shape
    group_count = lax.axis_size("expert")
    gate_count = lax.axis_size("gate")
    expert_count = group_count * gate_count
    capacity = 4 * row_count // expert_count
    partial = jnp.dot(samples, gate_weight, preferred_element_type=jnp.float32)
    logits = jnp.sum(lax.all_gather(partial, "gate"), axis=0)
    first, second, member, before = routing(expert_ids, expert_count)
    place = jnp.where(member, before, -1).T
    ranks = jnp.arange(capacity, dtype=jnp.int32)
    send = (place[:, None, :] == ranks[None, :, None]).astype(jnp.bfloat16)
    outgoing = jnp.dot(
        send.reshape(expert_count * capacity, row_count), samples, preferred_element_type=jnp.float32
    ).astype(jnp.bfloat16)
    incoming = lax.all_to_all(
        outgoing.reshape(expert_count, capacity, share),
        ("expert", "gate"),
        split_axis=0,
        concat_axis=0,
        tiled=True,
    ).reshape(group_count, gate_count, capacity, share)
    hidden = 0.0
    for g in range(gate_count):
        hidden += jnp.dot(
            incoming[:, g].reshape(group_count * capacity, share),
            up_weight[0, g * share : (g + 1) * share],
            preferred_element_type=jnp.float32,
        )
    active = jnp.maximum(hidden, 0.0).astype(jnp.bfloat16)
    expert_out = jnp.dot(active, down_weight[0], preferred_element_type=jnp.float32).astype(
        jnp.bfloat16
    )
    out_share = expert_out.shape[1] // gate_count
    outbound = expert_out.reshape(group_count, capacity, gate_count, out_share)
    outbound = outbound.transpose(0, 2, 1, 3).reshape(expert_count, capacity, out_share)
    returned = lax.all_to_all(
        outbound, ("expert", "gate"), split_axis=0, concat_axis=0, tiled=True
    ).reshape(expert_count * capacity, out_share)
    factor0, factor1 = factors(logits, first, second, pad_mask, expert_count)
    slots = jnp.arange(expert_count * capacity, dtype=jnp.int32)[None, :]
    mixed = 0.0
    for k, (chosen, factor) in enumerate(((first, factor0), (second, factor1))):
        rank = jnp.sum(jnp.where(chosen, before, 0), axis=1, keepdims=True)
        position = expert_ids[:, k : k + 1] * capacity + rank
        pick = (position == slots).astype(jnp.bfloat16)
        mixed += factor * jnp.dot(pick, returned, preferred_element_type=jnp.float32)
    return mixed.astype(jnp.bfloat16)


def solution(mesh):
    placed = (
        P("expert", "gate"),
        P("gate", None),
        P("expert", None),
        P("expert"),
        P(("expert", "gate"), None, None),
        P(("expert", "gate"), None, None),
    )
    return jax.shard_map(
        per_device, mesh=mesh, in_specs=placed, out_specs=P("expert", "gate"), check_vma=False
    )
```

```python
import functools

import jax
import jax.numpy as jnp
from jax import lax
from jax.experimental import pallas as pl
from jax.experimental.pallas import tpu as pltpu
from jax.sharding import PartitionSpec as P


MESH = pl.DeviceIdType.MESH
CHUNKS = 4
SIDES = 2
PARTS = 3
STRIDE = 5


def routing(expert_ids, expert_count):
    row_count = expert_ids.shape[0]
    lanes = jnp.arange(expert_count, dtype=jnp.int32)[None, :]
    first = expert_ids[:, 0:1] == lanes
    second = expert_ids[:, 1:2] == lanes
    member = first | second
    rows = jnp.arange(row_count, dtype=jnp.int32)
    lower = (rows[:, None] > rows[None, :]).astype(jnp.bfloat16)
    before = jnp.dot(lower, member.astype(jnp.bfloat16), preferred_element_type=jnp.float32)
    before = before.astype(jnp.int32)
    return first, second, member, before


def factors(logits, first, second, pad_mask, expert_count):
    top = jnp.max(logits, axis=1, keepdims=True)
    terms = jnp.exp(logits - top)
    scale = pad_mask.astype(jnp.float32)[:, None] / jnp.sum(terms, axis=1, keepdims=True)
    factor0 = expert_count * jnp.sum(jnp.where(first, terms, 0.0), axis=1, keepdims=True) * scale
    factor1 = expert_count * jnp.sum(jnp.where(second, terms, 0.0), axis=1, keepdims=True) * scale
    return factor0, factor1


def copied(source, target, sem):
    return pltpu.make_async_copy(source, target, sem)


def sent(source, target, send_sem, recv_sem, device):
    return pltpu.make_async_remote_copy(
        src_ref=source,
        dst_ref=target,
        send_sem=send_sem,
        recv_sem=recv_sem,
        device_id=device,
        device_id_type=MESH,
    )


def table(values, index):
    out = values[0]
    for k in range(1, len(values)):
        out = jnp.where(index == k, values[k], out)
    return out


NONE, WAIT, END, LOCAL, EXPERT, LOGITS, FACTOR, JOIN_EDGE, JOIN, END_PART, EXPERT_PART, WEIGHTS, BACK = range(13)
OWN, EDGE, INNER, FAR = range(4)


def coded(*jobs):
    return [kind * 16 + rel * 4 + c for kind, rel, c in jobs]


MIDDLE_JOBS = coded(
    (END, OWN, 0),
    (LOGITS, OWN, 0),
    (LOCAL, OWN, 0),
    (LOCAL, OWN, 1),
    (LOCAL, OWN, 2),
    (LOCAL, OWN, 3),
    (END, OWN, 1),
    (WEIGHTS, OWN, 0),
    (EXPERT, OWN, 0),
    (FACTOR, OWN, 0),
    (WAIT, EDGE, 0),
    (LOCAL, EDGE, 0),
    (WAIT, INNER, 0),
    (END, INNER, 0),
    (LOCAL, INNER, 0),
    (EXPERT, OWN, 1),
    (EXPERT, OWN, 2),
    (WAIT, EDGE, 1),
    (LOCAL, EDGE, 1),
    (WAIT, INNER, 1),
    (END, INNER, 1),
    (LOCAL, INNER, 1),
    (EXPERT, OWN, 3),
    (EXPERT, EDGE, 0),
    (WAIT, EDGE, 2),
    (LOCAL, EDGE, 2),
    (WAIT, FAR, 0),
    (END, FAR, 0),
    (LOCAL, FAR, 0),
    (EXPERT, INNER, 0),
    (EXPERT, EDGE, 1),
    (WAIT, EDGE, 3),
    (LOCAL, EDGE, 3),
    (WAIT, FAR, 1),
    (END, FAR, 1),
    (LOCAL, FAR, 1),
    (EXPERT, INNER, 1),
    (WAIT, FAR, 2),
    (END, FAR, 2),
    (LOCAL, FAR, 2),
    (EXPERT, EDGE, 2),
    (WAIT, FAR, 3),
    (END, FAR, 3),
    (LOCAL, FAR, 3),
    (EXPERT, FAR, 0),
    (EXPERT, EDGE, 3),
    (EXPERT, FAR, 1),
    (WAIT, INNER, 2),
    (END, INNER, 2),
    (LOCAL, INNER, 2),
    (EXPERT, FAR, 2),
    (EXPERT, FAR, 3),
    (BACK, FAR, 0),
    (WAIT, INNER, 3),
    (END, INNER, 3),
    (LOCAL, INNER, 3),
    (END, OWN, 2),
    (END_PART, OWN, 0),
    (END_PART, OWN, 1),
    (END_PART, OWN, 2),
    (BACK, EDGE, 0),
    (BACK, OWN, 0),
    (EXPERT, INNER, 2),
    (EXPERT, INNER, 3),
    (BACK, INNER, 0),
    (JOIN_EDGE, OWN, 0),
    (JOIN_EDGE, INNER, 0),
    (JOIN_EDGE, FAR, 0),
    (JOIN, OWN, 0),
    (JOIN, INNER, 0),
    (JOIN, FAR, 0),
    (JOIN, EDGE, 0),
)
EDGE_JOBS = coded(
    (LOCAL, EDGE, 0),
    (LOGITS, EDGE, 0),
    (LOCAL, EDGE, 1),
    (LOCAL, EDGE, 2),
    (LOCAL, EDGE, 3),
    (WEIGHTS, EDGE, 0),
    (EXPERT, EDGE, 0),
    (FACTOR, EDGE, 0),
    (EXPERT, EDGE, 1),
    (EXPERT, OWN, 0),
    (EXPERT, EDGE, 2),
    (EXPERT, OWN, 1),
    (EXPERT, EDGE, 3),
    (BACK, EDGE, 0),
    (EXPERT, INNER, 0),
    (EXPERT, INNER, 1),
    (EXPERT, FAR, 0),
    (EXPERT, FAR, 1),
    (EXPERT, FAR, 2),
    (EXPERT, FAR, 3),
    (BACK, FAR, 0),
    (EXPERT, INNER, 2),
    (EXPERT, INNER, 3),
    (BACK, INNER, 0),
    (EXPERT, OWN, 2),
    (EXPERT_PART, OWN, 0),
    (EXPERT_PART, OWN, 1),
    (EXPERT_PART, OWN, 2),
    (JOIN, EDGE, 0),
)


def exchange_kernel(
    gates,
    capacity,
    samples,
    ids,
    pads,
    gate_weight,
    up,
    down,
    out,
    blocks,
    named,
    mask,
    gatev,
    places,
    lower,
    onehot,
    dbuf,
    inc,
    upv,
    downv,
    hidden,
    obuf,
    logits,
    factor,
    edge_factor,
    ret,
    edge_ret,
    select,
    mixed,
    part,
    taken,
    own_sem,
    w_sem,
    in_sem,
    raw_s,
    raw_r,
    id_s,
    id_r,
    ds,
    pr,
    ph,
    rs,
    rr,
    er,
    gs,
    gr,
    fs,
    fr,
    ts,
    tr,
):
    chunks = CHUNKS
    local = SIDES * gates
    planes = blocks.shape[0]
    total = planes * local
    rows = blocks.shape[2]
    width = blocks.shape[3]
    share = width * chunks
    slots = local * capacity
    few = capacity // PARTS
    bf16, f32 = jnp.bfloat16, jnp.float32
    e = lax.axis_index("expert")
    g = lax.axis_index("gate")
    z = e // SIDES
    y = lax.rem(e, SIDES)
    mine = y * gates + g
    low = z < planes // 2
    toward = jnp.where(low, 1, -1)
    near = jnp.where(low, 0, planes - 1)
    far = planes - 1 - near
    edge = z == near
    middle = jnp.logical_not(edge)
    mid = near + toward
    inner = z + toward

    def plane_of(rel):
        return table((mid, near, mid + toward, far), rel)

    def at(plane, i):
        return (plane * SIDES + i // gates, lax.rem(i, gates))

    barrier = pltpu.get_barrier_semaphore()

    def greet(d, carry):
        plane = z - 1 + d // local
        i = lax.rem(mine + d, local)

        @pl.when((plane >= 0) & (plane < planes) & (d != local))
        def _():
            pl.semaphore_signal(barrier, inc=1, device_id=at(plane, i), device_id_type=MESH)

        return carry

    with jax.named_scope("greet"):
        lax.fori_loop(0, 3 * local, greet, 0)
    greeted = jnp.where(edge, 2, 3) * local - 1

    inputs = (
        copied(ids, named.at[z], in_sem.at[0]),
        copied(pads, mask, in_sem.at[1]),
        copied(gate_weight, gatev, in_sem.at[2]),
    )
    for copy in inputs:
        copy.start()
    own = [
        copied(samples.at[:, pl.ds(c * width, width)], blocks.at[z, c], own_sem.at[c])
        for c in range(chunks)
    ]
    for copy in own:
        copy.start()
    weights = [copied(down.at[0], downv, w_sem.at[0])]
    for c in range(chunks):
        for k in range(gates):
            weights.append(
                copied(
                    up.at[0, pl.ds(k * share + c * width, width)],
                    upv.at[c, pl.ds(k * width, width)],
                    w_sem.at[1 + c * gates + k],
                )
            )

    earlier = lax.broadcasted_iota(jnp.int32, (rows, rows), 0)
    later = lax.broadcasted_iota(jnp.int32, (rows, rows), 1)
    with jax.named_scope("lower"):
        lower[...] = jnp.where(earlier < later, 1.0, 0.0).astype(bf16)

    def end_index(rel):
        return jnp.where(rel == OWN, planes, planes - 1 + rel)

    def prepare(j, rel):
        lanes = lax.broadcasted_iota(jnp.int32, (total, rows), 0)
        member = (named[j, 0:1, :] == lanes) | (named[j, 1:2, :] == lanes)
        flags = jnp.where(member, 1.0, 0.0).astype(bf16)
        before = jnp.dot(flags, lower[...], preferred_element_type=f32)
        places[j] = jnp.where(member, before, -1.0)
        ranks = lax.broadcasted_iota(jnp.int32, (capacity, rows), 0).astype(f32)

        def build(index, plane):
            def one(i, carry):
                line = places[j, pl.ds(plane * local + i, 1), :]
                found = jnp.where(line == ranks, 1.0, 0.0).astype(bf16)
                onehot[index, :, i] = found.reshape(PARTS, few, rows)
                return carry

            lax.fori_loop(0, local, one, 0)

        @pl.when(middle & (rel != EDGE))
        def _():
            build(end_index(rel), near)

        build(rel, z)

    def pick(index, part, j, c):
        dbuf[index, c, part] = (
            jnp.dot(
                onehot[index, part].reshape(local * few, rows),
                blocks[j, c],
                preferred_element_type=f32,
            )
            .astype(bf16)
            .reshape(local, few, width)
        )

    with jax.named_scope("inputs"):
        for copy in inputs:
            copy.wait()
    with jax.named_scope("prepare"):
        prepare(z, jnp.where(edge, EDGE, OWN))
    with jax.named_scope("samples"):
        for copy in own:
            copy.wait()
    for q in range(PARTS):
        pick(jnp.where(edge, EDGE, planes), q, z, 0)
    with jax.named_scope("barrier"):
        pl.semaphore_wait(barrier, greeted)

    def ids_on(j, sem):
        return sent(named.at[j], named.at[j], sem, id_r.at[j], at(inner, mine))

    def shift(j, c):
        return sent(
            blocks.at[j, c], blocks.at[j, c], raw_s.at[j, c], raw_r.at[j, c], at(inner, mine)
        )

    ids_on(z, id_s.at[0]).start()
    for c in range(2):
        shift(z, c).start()

    @pl.when(edge)
    def _():
        for c in range(2, chunks):
            shift(z, c).start()

    for copy in weights:
        copy.start()
    gate_routes = []
    for d in range(1, gates):
        t = lax.rem(g + d, gates)
        gate_routes.append(sent(logits.at[g], logits.at[g], gs.at[d - 1], gr.at[d - 1], (e, t)))
    edge_route = sent(factor, edge_factor, fs, fr, at(inner, mine))
    part_route = sent(part, taken, ts, tr, at(near, mine))

    def wait(j, rel, c):
        with jax.named_scope("wait_raw"):
            copied(blocks.at[j, c], blocks.at[j, c], raw_r.at[j, c]).wait()

        @pl.when(c == 0)
        def _():
            copied(named.at[j], named.at[j], id_r.at[j]).wait()

        @pl.when(rel == EDGE)
        def _():
            @pl.when(c == 0)
            def _():
                ids_on(j, id_s.at[1]).start()

            shift(j, c).start()

            @pl.when(c == chunks - 1)
            def _():
                for k in range(2, chunks):
                    shift(z, k).start()

        @pl.when(c == 0)
        def _():
            prepare(j, rel)

    def dispatch(j, rel, c, to_end, fresh):
        index = jnp.where(to_end, end_index(rel), rel)
        plane = jnp.where(to_end, near, z)

        @pl.when(fresh)
        def _():
            with jax.named_scope("pick"):
                for part in range(PARTS):
                    pick(index, part, j, c)

        def give(d, carry):
            i = lax.rem(mine + STRIDE * d, local)
            piece = dbuf.at[index, c, :, i]
            place = inc.at[j, c, y, :, :, pl.ds(g * width, width)]
            here = jnp.logical_not(to_end) & (d == 0)

            @pl.when(here)
            def _():
                copied(piece, place, pr.at[j, c]).start()

            @pl.when(jnp.logical_not(here))
            def _():
                sent(piece, place, ds, pr.at[j, c], at(plane, i)).start()

            return carry

        lax.fori_loop(0, local, give, 0)

    def dispatch_part(part):
        c = chunks - 1
        pick(planes, part, z, c)

        def give(d, carry):
            i = lax.rem(mine + STRIDE * d, local)
            sent(
                dbuf.at[planes, c, part, i],
                inc.at[z, c, y, part, :, pl.ds(g * width, width)],
                ds,
                ph.at[part],
                at(near, i),
            ).start()
            return carry

        lax.fori_loop(0, local, give, 0)

    def give_back(j, part):
        ends = (j == 0) | (j == planes - 1)
        joined = ends & (j != z)
        plane = jnp.where(joined, jnp.where(j == 0, 1, planes - 2), j)

        def hand(d, carry):
            i = lax.rem(mine + d, local)
            side, k = i // gates, lax.rem(i, gates)
            here = (plane == z) & (d == 0)

            def hand_to(buffer, sem):
                if part is None:
                    block, spot = obuf.at[j, k, side], buffer.at[z, mine]
                else:
                    block, spot = obuf.at[j, k, side, part], buffer.at[z, mine, part]

                @pl.when(here)
                def _():
                    copied(block, spot, sem.at[z]).start()

                @pl.when(jnp.logical_not(here))
                def _():
                    sent(block, spot, rs, sem.at[z], at(plane, i)).start()

            @pl.when(joined)
            def _():
                hand_to(edge_ret, er)

            @pl.when(jnp.logical_not(joined))
            def _():
                hand_to(ret, rr)

            return carry

        lax.fori_loop(0, local, hand, 0)

    tile = 256
    inner_tiles = [slice(n, n + tile) for n in range(0, hidden.shape[4], tile)]
    out_width = downv.shape[1] // gates

    def expert(j, c):
        with jax.named_scope("wait_inc"):
            copied(inc.at[j, c], inc.at[j, c], pr.at[j, c]).wait()
        taken_in = inc[j, c].reshape(SIDES * capacity, share)
        for cols in inner_tiles:
            acc = jnp.dot(taken_in, upv[c, :, cols], preferred_element_type=f32)
            acc = acc.reshape(SIDES, PARTS, few, tile)

            @pl.when(c == 0)
            def _():
                hidden[j, :, :, :, cols] = acc

            @pl.when(c != 0)
            def _():
                hidden[j, :, :, :, cols] += acc

    def project(j):
        active = jnp.maximum(hidden[j], 0.0).astype(bf16).reshape(SIDES * capacity, -1)
        for k in range(gates):
            obuf[j, k] = (
                jnp.dot(
                    active,
                    downv[:, k * out_width : (k + 1) * out_width],
                    preferred_element_type=f32,
                )
                .astype(bf16)
                .reshape(SIDES, PARTS, few, out_width)
            )
        with jax.named_scope("back"):
            give_back(j, None)

    def expert_part(j, part):
        c = chunks - 1
        with jax.named_scope("wait_part"):
            arriving = inc.at[j, c, :, part]
            copied(arriving, arriving, ph.at[part]).wait()
        taken_in = inc[j, c, :, part].reshape(SIDES * few, share)
        active = []
        for cols in inner_tiles:
            acc = jnp.dot(taken_in, upv[c, :, cols], preferred_element_type=f32)
            acc += hidden[j, :, part, :, cols].reshape(SIDES * few, tile)
            active.append(jnp.maximum(acc, 0.0).astype(bf16))
        active = jnp.concatenate(active, axis=1)
        for k in range(gates):
            obuf[j, k, :, part] = (
                jnp.dot(
                    active,
                    downv[:, k * out_width : (k + 1) * out_width],
                    preferred_element_type=f32,
                )
                .astype(bf16)
                .reshape(SIDES, few, out_width)
            )
        with jax.named_scope("back"):
            give_back(j, part)

    def gate_logits():
        partial = 0.0
        for c in range(chunks):
            partial += lax.dot_general(
                gatev[:, c * width : (c + 1) * width],
                blocks[z, c],
                (((1,), (1,)), ((), ())),
                preferred_element_type=f32,
            )
        logits[g] = partial
        for copy in gate_routes:
            copy.start()

    def gate_factor():
        with jax.named_scope("wait_gate"):
            for copy in gate_routes:
                copy.wait_recv()
        summed = logits[0]
        for k in range(1, gates):
            summed += logits[k]
        top = jnp.max(summed, axis=0, keepdims=True)
        terms = jnp.exp(summed - top)
        scale = mask[...].astype(f32).reshape(1, rows) / jnp.sum(terms, axis=0, keepdims=True)
        factor[...] = total * terms * scale

        @pl.when(edge)
        def _():
            edge_route.start()

    def join(j, p, weight, returned, sem, index, first):
        ranks = lax.broadcasted_iota(jnp.int32, (capacity, rows), 0).astype(f32)

        def one(i, carry):
            line = places[j, pl.ds(p * local + i, 1), :]
            scale = weight[pl.ds(p * local + i, 1), :]
            select[pl.ds(pl.multiple_of(i * capacity, capacity), capacity), :] = jnp.where(
                line == ranks, scale, 0.0
            ).astype(bf16)
            return carry

        lax.fori_loop(0, local, one, 0)
        with jax.named_scope("wait_ret"):
            copied(returned.at[p], returned.at[p], sem.at[p]).wait()
        found = lax.dot_general(
            select[...],
            returned[p].reshape(slots, out_width),
            (((0,), (0,)), ((), ())),
            preferred_element_type=f32,
        )

        @pl.when(first)
        def _():
            mixed[index] = found

        @pl.when(jnp.logical_not(first))
        def _():
            mixed[index] += found

    def job(t, carry):
        code = jnp.where(edge, table(EDGE_JOBS, t), table(MIDDLE_JOBS, t))
        kind, rel, c = code // 16, lax.rem(code // 4, 4), lax.rem(code, 4)
        j = plane_of(rel)

        @pl.when(kind == WAIT)
        def _():
            wait(j, rel, c)

        @pl.when((kind == END) | (kind == LOCAL))
        def _():
            dispatch(j, rel, c, kind == END, t > 0)

        @pl.when(kind == EXPERT)
        def _():
            expert(j, c)

        @pl.when(kind == BACK)
        def _():
            project(j)

        @pl.when(kind == END_PART)
        def _():
            dispatch_part(c)

        @pl.when(kind == EXPERT_PART)
        def _():
            expert_part(j, c)

        @pl.when(kind == WEIGHTS)
        def _():
            with jax.named_scope("wait_w"):
                for copy in weights:
                    copy.wait()

        @pl.when(kind == LOGITS)
        def _():
            gate_logits()

        @pl.when(kind == FACTOR)
        def _():
            gate_factor()

        @pl.when(kind == JOIN_EDGE)
        def _():
            @pl.when(rel == OWN)
            def _():
                copied(edge_factor, edge_factor, fr).wait()

            join(near, j, edge_factor, edge_ret, er, 0, rel == OWN)

            @pl.when(rel == FAR)
            def _():
                part[...] = mixed[0].astype(bf16)
                part_route.start()

        @pl.when(kind == JOIN)
        def _():
            join(z, j, factor, ret, rr, 1, edge | (rel == OWN))

        return carry

    lax.fori_loop(0, jnp.where(edge, len(EDGE_JOBS), len(MIDDLE_JOBS)), job, 0)

    @pl.when(edge)
    def _():
        with jax.named_scope("wait_taken"):
            copied(taken, taken, tr).wait()
        out[...] = (mixed[1] + taken[...].astype(f32)).astype(bf16)

    @pl.when(middle)
    def _():
        out[...] = mixed[1].astype(bf16)

    for copy in gate_routes:
        copy.wait_send()
    ids_on(z, id_s.at[0]).wait_send()
    for c in range(chunks):
        shift(z, c).wait_send()
    within = dbuf.at[EDGE, :, :, pl.ds(0, local - 1)]
    copied(within, within, ds).wait()
    handed = ret.at[pl.ds(0, planes - 1)]
    few_more = ret.at[0, pl.ds(0, local - 2)]
    one_more = ret.at[0, 0]
    copied(handed, handed, rs).wait()
    copied(few_more, few_more, rs).wait()

    @pl.when(edge)
    def _():
        copied(one_more, one_more, rs).wait()
        edge_route.wait_send()

    @pl.when(middle)
    def _():
        part_route.wait_send()
        ids_on(near, id_s.at[1]).wait_send()
        for c in range(chunks):
            shift(near, c).wait_send()
        others = dbuf.at[pl.ds(0, planes - 1), :, :, pl.ds(0, local - 1)]
        copied(others, others, ds).wait()
        ahead = dbuf.at[pl.ds(planes, planes - 1)]
        copied(ahead, ahead, ds).wait()


def exchange(samples, ids, pads, gate_weight, up, down, planes, gates, capacity):
    rows, share = samples.shape
    local = SIDES * gates
    total = planes * local
    width = share // CHUNKS
    depth, inner = up.shape[1:]
    outer = down.shape[2]
    out_width = outer // gates
    bf16, f32 = jnp.bfloat16, jnp.float32
    dma = pltpu.SemaphoreType.DMA
    hbm = pl.BlockSpec(memory_space=pl.ANY)
    slots = local * capacity
    few = capacity // PARTS
    kinds = 2 * planes - 1
    return pl.pallas_call(
        functools.partial(exchange_kernel, gates, capacity),
        out_shape=pltpu.VMEM((rows, out_width), bf16),
        in_specs=[hbm] * 6,
        out_specs=pl.BlockSpec(memory_space=pltpu.VMEM),
        scratch_shapes=[
            pltpu.VMEM((planes, CHUNKS, rows, width), bf16),
            pltpu.VMEM((planes,) + ids.shape, jnp.int32),
            pltpu.VMEM(pads.shape, jnp.int32),
            pltpu.VMEM(gate_weight.shape, bf16),
            pltpu.VMEM((planes, total, rows), f32),
            pltpu.VMEM((rows, rows), bf16),
            pltpu.VMEM((kinds, PARTS, local, few, rows), bf16),
            pltpu.VMEM((kinds, CHUNKS, PARTS, local, few, width), bf16),
            pltpu.VMEM((planes, CHUNKS, SIDES, PARTS, few, gates * width), bf16),
            pltpu.VMEM((CHUNKS, depth // CHUNKS, inner), bf16),
            pltpu.VMEM((inner, outer), bf16),
            pltpu.VMEM((planes, SIDES, PARTS, few, inner), f32),
            pltpu.VMEM((planes, gates, SIDES, PARTS, few, out_width), bf16),
            pltpu.VMEM((gates, total, rows), f32),
            pltpu.VMEM((total, rows), f32),
            pltpu.VMEM((total, rows), f32),
            pltpu.VMEM((planes, local, PARTS, few, out_width), bf16),
            pltpu.VMEM((planes, local, PARTS, few, out_width), bf16),
            pltpu.VMEM((slots, rows), bf16),
            pltpu.VMEM((2, rows, out_width), f32),
            pltpu.VMEM((rows, out_width), bf16),
            pltpu.VMEM((rows, out_width), bf16),
            dma((CHUNKS,)),
            dma((1 + CHUNKS * gates,)),
            dma((3,)),
            dma((planes, CHUNKS)),
            dma((planes, CHUNKS)),
            dma((2,)),
            dma((planes,)),
            dma,
            dma((planes, CHUNKS)),
            dma((PARTS,)),
            dma,
            dma((planes,)),
            dma((planes,)),
            dma((gates,)),
            dma((gates,)),
            dma,
            dma,
            dma,
            dma,
        ],
        compiler_params=pltpu.CompilerParams(
            collective_id=0, has_side_effects=True, vmem_limit_bytes=58 << 20
        ),
    )(samples, ids, pads, gate_weight, up, down)


def in_one_kernel(samples, gate_weight, expert_ids, pad_mask, up_weight, down_weight):
    group_count = lax.axis_size("expert")
    gate_count = lax.axis_size("gate")
    expert_count = group_count * gate_count
    return exchange(
        samples,
        expert_ids.T,
        pad_mask,
        gate_weight.T,
        up_weight,
        down_weight,
        group_count // SIDES,
        gate_count,
        4 * samples.shape[0] // expert_count,
    )


def fits(samples, up_weight, down_weight):
    group_count = lax.axis_size("expert")
    capacity = 4 * samples.shape[0] // (group_count * lax.axis_size("gate"))
    planes = group_count // SIDES
    held = 2 * (planes * samples.size * 3 + up_weight.size + down_weight.size)
    return planes == 4 and group_count % SIDES == 0 and capacity % (16 * PARTS) == 0 and held < 40 << 20


def per_device(samples, gate_weight, expert_ids, pad_mask, up_weight, down_weight):
    if fits(samples, up_weight, down_weight):
        return in_one_kernel(
            samples, gate_weight, expert_ids, pad_mask, up_weight, down_weight
        )
    row_count, share = samples.shape
    group_count = lax.axis_size("expert")
    gate_count = lax.axis_size("gate")
    expert_count = group_count * gate_count
    capacity = 4 * row_count // expert_count
    partial = jnp.dot(samples, gate_weight, preferred_element_type=jnp.float32)
    logits = jnp.sum(lax.all_gather(partial, "gate"), axis=0)
    first, second, member, before = routing(expert_ids, expert_count)
    place = jnp.where(member, before, -1).T
    ranks = jnp.arange(capacity, dtype=jnp.int32)
    send = (place[:, None, :] == ranks[None, :, None]).astype(jnp.bfloat16)
    outgoing = jnp.dot(
        send.reshape(expert_count * capacity, row_count), samples, preferred_element_type=jnp.float32
    ).astype(jnp.bfloat16)
    incoming = lax.all_to_all(
        outgoing.reshape(expert_count, capacity, share),
        ("expert", "gate"),
        split_axis=0,
        concat_axis=0,
        tiled=True,
    ).reshape(group_count, gate_count, capacity, share)
    hidden = 0.0
    for g in range(gate_count):
        hidden += jnp.dot(
            incoming[:, g].reshape(group_count * capacity, share),
            up_weight[0, g * share : (g + 1) * share],
            preferred_element_type=jnp.float32,
        )
    active = jnp.maximum(hidden, 0.0).astype(jnp.bfloat16)
    expert_out = jnp.dot(active, down_weight[0], preferred_element_type=jnp.float32).astype(
        jnp.bfloat16
    )
    out_share = expert_out.shape[1] // gate_count
    outbound = expert_out.reshape(group_count, capacity, gate_count, out_share)
    outbound = outbound.transpose(0, 2, 1, 3).reshape(expert_count, capacity, out_share)
    returned = lax.all_to_all(
        outbound, ("expert", "gate"), split_axis=0, concat_axis=0, tiled=True
    ).reshape(expert_count * capacity, out_share)
    factor0, factor1 = factors(logits, first, second, pad_mask, expert_count)
    slots = jnp.arange(expert_count * capacity, dtype=jnp.int32)[None, :]
    mixed = 0.0
    for k, (chosen, factor) in enumerate(((first, factor0), (second, factor1))):
        rank = jnp.sum(jnp.where(chosen, before, 0), axis=1, keepdims=True)
        position = expert_ids[:, k : k + 1] * capacity + rank
        pick = (position == slots).astype(jnp.bfloat16)
        mixed += factor * jnp.dot(pick, returned, preferred_element_type=jnp.float32)
    return mixed.astype(jnp.bfloat16)


def solution(mesh):
    placed = (
        P("expert", "gate"),
        P("gate", None),
        P("expert", None),
        P("expert"),
        P(("expert", "gate"), None, None),
        P(("expert", "gate"), None, None),
    )
    return jax.shard_map(
        per_device, mesh=mesh, in_specs=placed, out_specs=P("expert", "gate"), check_vma=False
    )
```

```python
import functools

import jax
import jax.numpy as jnp
from jax import lax
from jax.experimental import pallas as pl
from jax.experimental.pallas import tpu as pltpu
from jax.sharding import PartitionSpec as P


MESH = pl.DeviceIdType.MESH
CHUNKS = 4
SIDES = 2
PARTS = 3
STRIDE = 5


def routing(expert_ids, expert_count):
    row_count = expert_ids.shape[0]
    lanes = jnp.arange(expert_count, dtype=jnp.int32)[None, :]
    first = expert_ids[:, 0:1] == lanes
    second = expert_ids[:, 1:2] == lanes
    member = first | second
    rows = jnp.arange(row_count, dtype=jnp.int32)
    lower = (rows[:, None] > rows[None, :]).astype(jnp.bfloat16)
    before = jnp.dot(lower, member.astype(jnp.bfloat16), preferred_element_type=jnp.float32)
    before = before.astype(jnp.int32)
    return first, second, member, before


def factors(logits, first, second, pad_mask, expert_count):
    top = jnp.max(logits, axis=1, keepdims=True)
    terms = jnp.exp(logits - top)
    scale = pad_mask.astype(jnp.float32)[:, None] / jnp.sum(terms, axis=1, keepdims=True)
    factor0 = expert_count * jnp.sum(jnp.where(first, terms, 0.0), axis=1, keepdims=True) * scale
    factor1 = expert_count * jnp.sum(jnp.where(second, terms, 0.0), axis=1, keepdims=True) * scale
    return factor0, factor1


def copied(source, target, sem):
    return pltpu.make_async_copy(source, target, sem)


def sent(source, target, send_sem, recv_sem, device):
    return pltpu.make_async_remote_copy(
        src_ref=source,
        dst_ref=target,
        send_sem=send_sem,
        recv_sem=recv_sem,
        device_id=device,
        device_id_type=MESH,
    )


def table(values, index):
    out = values[0]
    for k in range(1, len(values)):
        out = jnp.where(index == k, values[k], out)
    return out


NONE, WAIT, END, LOCAL, EXPERT, LOGITS, FACTOR, JOIN_EDGE, JOIN, END_PART, EXPERT_PART, WEIGHTS, BACK, SETTLE = range(14)
OWN, EDGE, INNER, FAR = range(4)


def coded(*jobs):
    return [kind * 16 + rel * 4 + c for kind, rel, c in jobs]


MIDDLE_JOBS = coded(
    (LOGITS, OWN, 0),
    (LOCAL, OWN, 0),
    (LOCAL, OWN, 1),
    (LOCAL, OWN, 2),
    (LOCAL, OWN, 3),
    (END, OWN, 1),
    (WEIGHTS, OWN, 0),
    (EXPERT, OWN, 0),
    (FACTOR, OWN, 0),
    (WAIT, EDGE, 0),
    (LOCAL, EDGE, 0),
    (WAIT, INNER, 0),
    (END, INNER, 0),
    (LOCAL, INNER, 0),
    (EXPERT, OWN, 1),
    (EXPERT, OWN, 2),
    (WAIT, EDGE, 1),
    (LOCAL, EDGE, 1),
    (WAIT, INNER, 1),
    (END, INNER, 1),
    (LOCAL, INNER, 1),
    (EXPERT, OWN, 3),
    (EXPERT, EDGE, 0),
    (WAIT, EDGE, 2),
    (LOCAL, EDGE, 2),
    (WAIT, FAR, 0),
    (END, FAR, 0),
    (LOCAL, FAR, 0),
    (EXPERT, INNER, 0),
    (EXPERT, EDGE, 1),
    (WAIT, EDGE, 3),
    (LOCAL, EDGE, 3),
    (WAIT, FAR, 1),
    (END, FAR, 1),
    (LOCAL, FAR, 1),
    (EXPERT, INNER, 1),
    (WAIT, FAR, 2),
    (END, FAR, 2),
    (LOCAL, FAR, 2),
    (EXPERT, EDGE, 2),
    (WAIT, FAR, 3),
    (END, FAR, 3),
    (LOCAL, FAR, 3),
    (EXPERT, FAR, 0),
    (EXPERT, EDGE, 3),
    (EXPERT, FAR, 1),
    (WAIT, INNER, 2),
    (END, INNER, 2),
    (LOCAL, INNER, 2),
    (EXPERT, FAR, 2),
    (EXPERT, FAR, 3),
    (BACK, FAR, 0),
    (WAIT, INNER, 3),
    (END, INNER, 3),
    (LOCAL, INNER, 3),
    (END, OWN, 2),
    (END_PART, OWN, 0),
    (END_PART, OWN, 1),
    (END_PART, OWN, 2),
    (BACK, EDGE, 0),
    (BACK, OWN, 0),
    (EXPERT, INNER, 2),
    (EXPERT, INNER, 3),
    (BACK, INNER, 0),
    (JOIN_EDGE, OWN, 0),
    (JOIN_EDGE, INNER, 0),
    (JOIN_EDGE, FAR, 0),
    (JOIN, OWN, 0),
    (JOIN, INNER, 0),
    (JOIN, FAR, 0),
    (SETTLE, OWN, 0),
    (JOIN, EDGE, 0),
)
EDGE_JOBS = coded(
    (LOGITS, EDGE, 0),
    (LOCAL, EDGE, 1),
    (LOCAL, EDGE, 2),
    (LOCAL, EDGE, 3),
    (WEIGHTS, EDGE, 0),
    (EXPERT, EDGE, 0),
    (FACTOR, EDGE, 0),
    (EXPERT, EDGE, 1),
    (EXPERT, OWN, 0),
    (EXPERT, EDGE, 2),
    (EXPERT, OWN, 1),
    (EXPERT, EDGE, 3),
    (BACK, EDGE, 0),
    (EXPERT, INNER, 0),
    (EXPERT, INNER, 1),
    (EXPERT, FAR, 0),
    (EXPERT, FAR, 1),
    (EXPERT, FAR, 2),
    (EXPERT, FAR, 3),
    (BACK, FAR, 0),
    (EXPERT, INNER, 2),
    (EXPERT, INNER, 3),
    (BACK, INNER, 0),
    (EXPERT, OWN, 2),
    (EXPERT_PART, OWN, 0),
    (EXPERT_PART, OWN, 1),
    (EXPERT_PART, OWN, 2),
    (JOIN, EDGE, 0),
    (SETTLE, OWN, 0),
)


def exchange_kernel(
    gates,
    capacity,
    samples,
    ids,
    pads,
    gate_weight,
    up,
    down,
    out,
    blocks,
    named,
    mask,
    gatev,
    places,
    lower,
    onehot,
    dbuf,
    inc,
    upv,
    downv,
    hidden,
    obuf,
    logits,
    factor,
    edge_factor,
    ret,
    edge_ret,
    select,
    mixed,
    part,
    taken,
    own_sem,
    w_sem,
    in_sem,
    raw_s,
    raw_r,
    id_s,
    id_r,
    ds,
    pr,
    ph,
    rs,
    rr,
    er,
    gs,
    gr,
    fs,
    fr,
    ts,
    tr,
):
    chunks = CHUNKS
    local = SIDES * gates
    planes = blocks.shape[0]
    total = planes * local
    rows = blocks.shape[2]
    width = blocks.shape[3]
    share = width * chunks
    slots = local * capacity
    few = capacity // PARTS
    bf16, f32 = jnp.bfloat16, jnp.float32
    e = lax.axis_index("expert")
    g = lax.axis_index("gate")
    z = e // SIDES
    y = lax.rem(e, SIDES)
    mine = y * gates + g
    low = z < planes // 2
    toward = jnp.where(low, 1, -1)
    near = jnp.where(low, 0, planes - 1)
    far = planes - 1 - near
    edge = z == near
    middle = jnp.logical_not(edge)
    mid = near + toward
    inner = z + toward

    def plane_of(rel):
        return table((mid, near, mid + toward, far), rel)

    def at(plane, i):
        return (plane * SIDES + i // gates, lax.rem(i, gates))

    barrier = pltpu.get_barrier_semaphore()

    inputs = (
        copied(ids, named.at[z], in_sem.at[0]),
        copied(pads, mask, in_sem.at[1]),
        copied(gate_weight, gatev, in_sem.at[2]),
    )
    for copy in inputs:
        copy.start()
    own = [
        copied(samples.at[:, pl.ds(c * width, width)], blocks.at[z, c], own_sem.at[c])
        for c in range(chunks)
    ]
    for copy in own:
        copy.start()
    def greet(d, carry):
        plane = z + table((toward, -toward, 0), d // local)
        i = lax.rem(mine + d, local)

        @pl.when((plane >= 0) & (plane < planes) & (d != 2 * local))
        def _():
            pl.semaphore_signal(barrier, inc=1, device_id=at(plane, i), device_id_type=MESH)

        return carry

    with jax.named_scope("greet"):
        lax.fori_loop(0, 3 * local, greet, 0)
    greeted = jnp.where(edge, 2, 3) * local - 1

    weights = [copied(down.at[0], downv, w_sem.at[0])]
    for c in range(chunks):
        for k in range(gates):
            weights.append(
                copied(
                    up.at[0, pl.ds(k * share + c * width, width)],
                    upv.at[c, pl.ds(k * width, width)],
                    w_sem.at[1],
                )
            )

    earlier = lax.broadcasted_iota(jnp.int32, (rows, rows), 0)
    later = lax.broadcasted_iota(jnp.int32, (rows, rows), 1)
    with jax.named_scope("lower"):
        lower[...] = jnp.where(earlier < later, 1.0, 0.0).astype(bf16)

    def end_index(rel):
        return jnp.where(rel == OWN, planes, planes - 1 + rel)

    def locate(j):
        lanes = lax.broadcasted_iota(jnp.int32, (total, rows), 0)
        member = (named[j, 0:1, :] == lanes) | (named[j, 1:2, :] == lanes)
        flags = jnp.where(member, 1.0, 0.0).astype(bf16)
        before = jnp.dot(flags, lower[...], preferred_element_type=f32)
        places[j] = jnp.where(member, before, -1.0)

    def build(j, index, plane):
        ranks = lax.broadcasted_iota(jnp.int32, (capacity, rows), 0).astype(f32)

        def one(i, carry):
            line = places[j, pl.ds(plane * local + i, 1), :]
            found = jnp.where(line == ranks, 1.0, 0.0).astype(bf16)
            onehot[index, :, i] = found.reshape(PARTS, few, rows)
            return carry

        lax.fori_loop(0, local, one, 0)

    def pick(index, part, j, c):
        dbuf[index, c, part] = (
            jnp.dot(
                onehot[index, part].reshape(local * few, rows),
                blocks[j, c],
                preferred_element_type=f32,
            )
            .astype(bf16)
            .reshape(local, few, width)
        )

    def hand_out(j, rel, c, to_end):
        index = jnp.where(to_end, end_index(rel), rel)
        plane = jnp.where(to_end, near, z)

        def give(d, carry):
            i = lax.rem(mine + STRIDE * d, local)
            piece = dbuf.at[index, c, :, i]
            place = inc.at[j, c, y, :, :, pl.ds(g * width, width)]
            here = jnp.logical_not(to_end) & (d == 0)

            @pl.when(here)
            def _():
                copied(piece, place, pr.at[j, c]).start()

            @pl.when(jnp.logical_not(here))
            def _():
                sent(piece, place, ds, pr.at[j, c], at(plane, i)).start()

            return carry

        lax.fori_loop(0, local, give, 0)

    with jax.named_scope("inputs"):
        for copy in inputs:
            copy.wait()
    first = jnp.where(edge, EDGE, planes)
    with jax.named_scope("prepare"):
        locate(z)
        build(z, first, near)
    with jax.named_scope("samples"):
        for copy in own:
            copy.wait()
    for q in range(PARTS):
        pick(first, q, z, 0)
    with jax.named_scope("barrier"):
        pl.semaphore_wait(barrier, greeted)
    hand_out(z, jnp.where(edge, EDGE, OWN), 0, middle)

    def ids_on(j, sem):
        return sent(named.at[j], named.at[j], sem, id_r.at[j], at(inner, mine))

    def shift(j, c):
        return sent(
            blocks.at[j, c], blocks.at[j, c], raw_s, raw_r.at[j, c], at(inner, mine)
        )

    ids_on(z, id_s.at[0]).start()
    for c in range(2):
        shift(z, c).start()

    @pl.when(edge)
    def _():
        for c in range(2, chunks):
            shift(z, c).start()

    for copy in weights:
        copy.start()

    @pl.when(middle)
    def _():
        build(z, OWN, z)

    gate_routes = []
    for d in range(1, gates):
        t = lax.rem(g + d, gates)
        gate_routes.append(sent(logits.at[g], logits.at[g], gs.at[d - 1], gr.at[d - 1], (e, t)))
    edge_route = sent(factor, edge_factor, fs, fr, at(inner, mine))
    part_route = sent(part, taken, ts, tr, at(near, mine))

    def wait(j, rel, c):
        with jax.named_scope("wait_raw"):
            copied(blocks.at[j, c], blocks.at[j, c], raw_r.at[j, c]).wait()

        @pl.when(c == 0)
        def _():
            copied(named.at[j], named.at[j], id_r.at[j]).wait()

        @pl.when(rel == EDGE)
        def _():
            @pl.when(c == 0)
            def _():
                ids_on(j, id_s.at[1]).start()

            shift(j, c).start()

            @pl.when(c == chunks - 1)
            def _():
                for k in range(2, chunks):
                    shift(z, k).start()

        @pl.when(c == 0)
        def _():
            locate(j)

            @pl.when(rel != EDGE)
            def _():
                build(j, end_index(rel), near)

            build(j, rel, z)

    def dispatch(j, rel, c, to_end):
        index = jnp.where(to_end, end_index(rel), rel)
        with jax.named_scope("pick"):
            for part in range(PARTS):
                pick(index, part, j, c)
        hand_out(j, rel, c, to_end)

    def dispatch_part(part):
        c = chunks - 1
        pick(planes, part, z, c)

        def give(d, carry):
            i = lax.rem(mine + STRIDE * d, local)
            sent(
                dbuf.at[planes, c, part, i],
                inc.at[z, c, y, part, :, pl.ds(g * width, width)],
                ds,
                ph.at[part],
                at(near, i),
            ).start()
            return carry

        lax.fori_loop(0, local, give, 0)

    def give_back(j, part):
        ends = (j == 0) | (j == planes - 1)
        joined = ends & (j != z)
        plane = jnp.where(joined, jnp.where(j == 0, 1, planes - 2), j)

        def hand(d, carry):
            i = lax.rem(mine + d, local)
            side, k = i // gates, lax.rem(i, gates)
            here = (plane == z) & (d == 0)

            def hand_to(buffer, sem):
                if part is None:
                    block, spot = obuf.at[j, k, side], buffer.at[z, mine]
                else:
                    block, spot = obuf.at[j, k, side, part], buffer.at[z, mine, part]

                @pl.when(here)
                def _():
                    copied(block, spot, sem.at[z]).start()

                @pl.when(jnp.logical_not(here))
                def _():
                    sent(block, spot, rs, sem.at[z], at(plane, i)).start()

            @pl.when(joined)
            def _():
                hand_to(edge_ret, er)

            @pl.when(jnp.logical_not(joined))
            def _():
                hand_to(ret, rr)

            return carry

        lax.fori_loop(0, local, hand, 0)

    tile = 256
    inner_tiles = [slice(n, n + tile) for n in range(0, hidden.shape[4], tile)]
    out_width = downv.shape[1] // gates

    def expert(j, c):
        with jax.named_scope("wait_inc"):
            copied(inc.at[j, c], inc.at[j, c], pr.at[j, c]).wait()
        taken_in = inc[j, c].reshape(SIDES * capacity, share)
        for cols in inner_tiles:
            acc = jnp.dot(taken_in, upv[c, :, cols], preferred_element_type=f32)
            acc = acc.reshape(SIDES, PARTS, few, tile)

            @pl.when(c == 0)
            def _():
                hidden[j, :, :, :, cols] = acc

            @pl.when(c != 0)
            def _():
                hidden[j, :, :, :, cols] += acc

    def project(j):
        active = jnp.maximum(hidden[j], 0.0).astype(bf16).reshape(SIDES * capacity, -1)
        for k in range(gates):
            obuf[j, k] = (
                jnp.dot(
                    active,
                    downv[:, k * out_width : (k + 1) * out_width],
                    preferred_element_type=f32,
                )
                .astype(bf16)
                .reshape(SIDES, PARTS, few, out_width)
            )
        with jax.named_scope("back"):
            give_back(j, None)

    def expert_part(j, part):
        c = chunks - 1
        with jax.named_scope("wait_part"):
            arriving = inc.at[j, c, :, part]
            copied(arriving, arriving, ph.at[part]).wait()
        taken_in = inc[j, c, :, part].reshape(SIDES * few, share)
        active = []
        for cols in inner_tiles:
            acc = jnp.dot(taken_in, upv[c, :, cols], preferred_element_type=f32)
            acc += hidden[j, :, part, :, cols].reshape(SIDES * few, tile)
            active.append(jnp.maximum(acc, 0.0).astype(bf16))
        active = jnp.concatenate(active, axis=1)
        for k in range(gates):
            obuf[j, k, :, part] = (
                jnp.dot(
                    active,
                    downv[:, k * out_width : (k + 1) * out_width],
                    preferred_element_type=f32,
                )
                .astype(bf16)
                .reshape(SIDES, few, out_width)
            )
        with jax.named_scope("back"):
            give_back(j, part)

    def gate_logits():
        partial = 0.0
        for c in range(chunks):
            partial += lax.dot_general(
                gatev[:, c * width : (c + 1) * width],
                blocks[z, c],
                (((1,), (1,)), ((), ())),
                preferred_element_type=f32,
            )
        logits[g] = partial
        for copy in gate_routes:
            copy.start()

    def gate_factor():
        with jax.named_scope("wait_gate"):
            for copy in gate_routes:
                copy.wait_recv()
        summed = logits[0]
        for k in range(1, gates):
            summed += logits[k]
        top = jnp.max(summed, axis=0, keepdims=True)
        terms = jnp.exp(summed - top)
        scale = mask[...].astype(f32).reshape(1, rows) / jnp.sum(terms, axis=0, keepdims=True)
        factor[...] = total * terms * scale

        @pl.when(edge)
        def _():
            edge_route.start()

    def join(j, p, weight, returned, sem, index, first):
        ranks = lax.broadcasted_iota(jnp.int32, (capacity, rows), 0).astype(f32)

        def one(i, carry):
            line = places[j, pl.ds(p * local + i, 1), :]
            scale = weight[pl.ds(p * local + i, 1), :]
            select[pl.ds(pl.multiple_of(i * capacity, capacity), capacity), :] = jnp.where(
                line == ranks, scale, 0.0
            ).astype(bf16)
            return carry

        lax.fori_loop(0, local, one, 0)
        with jax.named_scope("wait_ret"):
            copied(returned.at[p], returned.at[p], sem.at[p]).wait()
        found = lax.dot_general(
            select[...],
            returned[p].reshape(slots, out_width),
            (((0,), (0,)), ((), ())),
            preferred_element_type=f32,
        )

        @pl.when(first)
        def _():
            mixed[index] = found

        @pl.when(jnp.logical_not(first))
        def _():
            mixed[index] += found

    def settle():
        for copy in gate_routes:
            copy.wait_send()
        ids_on(z, id_s.at[0]).wait_send()
        copied(blocks.at[z], blocks.at[z], raw_s).wait()
        within = dbuf.at[EDGE, :, :, pl.ds(0, local - 1)]
        copied(within, within, ds).wait()

        @pl.when(middle)
        def _():
            ids_on(near, id_s.at[1]).wait_send()
            copied(blocks.at[near], blocks.at[near], raw_s).wait()
            others = dbuf.at[pl.ds(0, planes - 1), :, :, pl.ds(0, local - 1)]
            copied(others, others, ds).wait()
            ahead = dbuf.at[pl.ds(planes, planes - 1)]
            copied(ahead, ahead, ds).wait()

    def job(t, carry):
        code = jnp.where(edge, table(EDGE_JOBS, t), table(MIDDLE_JOBS, t))
        kind, rel, c = code // 16, lax.rem(code // 4, 4), lax.rem(code, 4)
        j = plane_of(rel)

        @pl.when(kind == WAIT)
        def _():
            wait(j, rel, c)

        @pl.when((kind == END) | (kind == LOCAL))
        def _():
            dispatch(j, rel, c, kind == END)

        @pl.when(kind == EXPERT)
        def _():
            expert(j, c)

        @pl.when(kind == BACK)
        def _():
            project(j)

        @pl.when(kind == END_PART)
        def _():
            dispatch_part(c)

        @pl.when(kind == EXPERT_PART)
        def _():
            expert_part(j, c)

        @pl.when(kind == WEIGHTS)
        def _():
            with jax.named_scope("wait_w"):
                weights[0].wait()
                copied(upv, upv, w_sem.at[1]).wait()

        @pl.when(kind == LOGITS)
        def _():
            gate_logits()

        @pl.when(kind == FACTOR)
        def _():
            gate_factor()

        @pl.when(kind == JOIN_EDGE)
        def _():
            @pl.when(rel == OWN)
            def _():
                copied(edge_factor, edge_factor, fr).wait()

            join(near, j, edge_factor, edge_ret, er, 0, rel == OWN)

            @pl.when(rel == FAR)
            def _():
                part[...] = mixed[0].astype(bf16)
                part_route.start()

        @pl.when(kind == SETTLE)
        def _():
            settle()

        @pl.when(kind == JOIN)
        def _():
            join(z, j, factor, ret, rr, 1, edge | (rel == OWN))

        return carry

    lax.fori_loop(0, jnp.where(edge, len(EDGE_JOBS), len(MIDDLE_JOBS)), job, 0)

    @pl.when(edge)
    def _():
        with jax.named_scope("wait_taken"):
            copied(taken, taken, tr).wait()
        with jax.named_scope("fin_add"):
            out[...] = (mixed[1] + taken[...].astype(f32)).astype(bf16)

    @pl.when(middle)
    def _():
        with jax.named_scope("fin_add"):
            out[...] = mixed[1].astype(bf16)

    handed = ret.at[pl.ds(0, planes - 1)]
    few_more = ret.at[0, pl.ds(0, local - 2)]
    one_more = ret.at[0, 0]
    copied(handed, handed, rs).wait()
    copied(few_more, few_more, rs).wait()

    @pl.when(edge)
    def _():
        copied(one_more, one_more, rs).wait()
        edge_route.wait_send()

    @pl.when(middle)
    def _():
        part_route.wait_send()


def exchange(samples, ids, pads, gate_weight, up, down, planes, gates, capacity):
    rows, share = samples.shape
    local = SIDES * gates
    total = planes * local
    width = share // CHUNKS
    depth, inner = up.shape[1:]
    outer = down.shape[2]
    out_width = outer // gates
    bf16, f32 = jnp.bfloat16, jnp.float32
    dma = pltpu.SemaphoreType.DMA
    hbm = pl.BlockSpec(memory_space=pl.ANY)
    slots = local * capacity
    few = capacity // PARTS
    kinds = 2 * planes - 1
    return pl.pallas_call(
        functools.partial(exchange_kernel, gates, capacity),
        out_shape=pltpu.VMEM((rows, out_width), bf16),
        in_specs=[hbm] * 6,
        out_specs=pl.BlockSpec(memory_space=pltpu.VMEM),
        scratch_shapes=[
            pltpu.VMEM((planes, CHUNKS, rows, width), bf16),
            pltpu.VMEM((planes,) + ids.shape, jnp.int32),
            pltpu.VMEM(pads.shape, jnp.int32),
            pltpu.VMEM(gate_weight.shape, bf16),
            pltpu.VMEM((planes, total, rows), f32),
            pltpu.VMEM((rows, rows), bf16),
            pltpu.VMEM((kinds, PARTS, local, few, rows), bf16),
            pltpu.VMEM((kinds, CHUNKS, PARTS, local, few, width), bf16),
            pltpu.VMEM((planes, CHUNKS, SIDES, PARTS, few, gates * width), bf16),
            pltpu.VMEM((CHUNKS, depth // CHUNKS, inner), bf16),
            pltpu.VMEM((inner, outer), bf16),
            pltpu.VMEM((planes, SIDES, PARTS, few, inner), f32),
            pltpu.VMEM((planes, gates, SIDES, PARTS, few, out_width), bf16),
            pltpu.VMEM((gates, total, rows), f32),
            pltpu.VMEM((total, rows), f32),
            pltpu.VMEM((total, rows), f32),
            pltpu.VMEM((planes, local, PARTS, few, out_width), bf16),
            pltpu.VMEM((planes, local, PARTS, few, out_width), bf16),
            pltpu.VMEM((slots, rows), bf16),
            pltpu.VMEM((2, rows, out_width), f32),
            pltpu.VMEM((rows, out_width), bf16),
            pltpu.VMEM((rows, out_width), bf16),
            dma((CHUNKS,)),
            dma((2,)),
            dma((3,)),
            dma,
            dma((planes, CHUNKS)),
            dma((2,)),
            dma((planes,)),
            dma,
            dma((planes, CHUNKS)),
            dma((PARTS,)),
            dma,
            dma((planes,)),
            dma((planes,)),
            dma((gates,)),
            dma((gates,)),
            dma,
            dma,
            dma,
            dma,
        ],
        compiler_params=pltpu.CompilerParams(
            collective_id=0, has_side_effects=True, vmem_limit_bytes=58 << 20
        ),
    )(samples, ids, pads, gate_weight, up, down)


def in_one_kernel(samples, gate_weight, expert_ids, pad_mask, up_weight, down_weight):
    group_count = lax.axis_size("expert")
    gate_count = lax.axis_size("gate")
    expert_count = group_count * gate_count
    return exchange(
        samples,
        expert_ids.T,
        pad_mask,
        gate_weight.T,
        up_weight,
        down_weight,
        group_count // SIDES,
        gate_count,
        4 * samples.shape[0] // expert_count,
    )


def fits(samples, up_weight, down_weight):
    group_count = lax.axis_size("expert")
    capacity = 4 * samples.shape[0] // (group_count * lax.axis_size("gate"))
    planes = group_count // SIDES
    held = 2 * (planes * samples.size * 3 + up_weight.size + down_weight.size)
    return planes == 4 and group_count % SIDES == 0 and capacity % (16 * PARTS) == 0 and held < 40 << 20


def per_device(samples, gate_weight, expert_ids, pad_mask, up_weight, down_weight):
    if fits(samples, up_weight, down_weight):
        return in_one_kernel(
            samples, gate_weight, expert_ids, pad_mask, up_weight, down_weight
        )
    row_count, share = samples.shape
    group_count = lax.axis_size("expert")
    gate_count = lax.axis_size("gate")
    expert_count = group_count * gate_count
    capacity = 4 * row_count // expert_count
    partial = jnp.dot(samples, gate_weight, preferred_element_type=jnp.float32)
    logits = jnp.sum(lax.all_gather(partial, "gate"), axis=0)
    first, second, member, before = routing(expert_ids, expert_count)
    place = jnp.where(member, before, -1).T
    ranks = jnp.arange(capacity, dtype=jnp.int32)
    send = (place[:, None, :] == ranks[None, :, None]).astype(jnp.bfloat16)
    outgoing = jnp.dot(
        send.reshape(expert_count * capacity, row_count), samples, preferred_element_type=jnp.float32
    ).astype(jnp.bfloat16)
    incoming = lax.all_to_all(
        outgoing.reshape(expert_count, capacity, share),
        ("expert", "gate"),
        split_axis=0,
        concat_axis=0,
        tiled=True,
    ).reshape(group_count, gate_count, capacity, share)
    hidden = 0.0
    for g in range(gate_count):
        hidden += jnp.dot(
            incoming[:, g].reshape(group_count * capacity, share),
            up_weight[0, g * share : (g + 1) * share],
            preferred_element_type=jnp.float32,
        )
    active = jnp.maximum(hidden, 0.0).astype(jnp.bfloat16)
    expert_out = jnp.dot(active, down_weight[0], preferred_element_type=jnp.float32).astype(
        jnp.bfloat16
    )
    out_share = expert_out.shape[1] // gate_count
    outbound = expert_out.reshape(group_count, capacity, gate_count, out_share)
    outbound = outbound.transpose(0, 2, 1, 3).reshape(expert_count, capacity, out_share)
    returned = lax.all_to_all(
        outbound, ("expert", "gate"), split_axis=0, concat_axis=0, tiled=True
    ).reshape(expert_count * capacity, out_share)
    factor0, factor1 = factors(logits, first, second, pad_mask, expert_count)
    slots = jnp.arange(expert_count * capacity, dtype=jnp.int32)[None, :]
    mixed = 0.0
    for k, (chosen, factor) in enumerate(((first, factor0), (second, factor1))):
        rank = jnp.sum(jnp.where(chosen, before, 0), axis=1, keepdims=True)
        position = expert_ids[:, k : k + 1] * capacity + rank
        pick = (position == slots).astype(jnp.bfloat16)
        mixed += factor * jnp.dot(pick, returned, preferred_element_type=jnp.float32)
    return mixed.astype(jnp.bfloat16)


def solution(mesh):
    placed = (
        P("expert", "gate"),
        P("gate", None),
        P("expert", None),
        P("expert"),
        P(("expert", "gate"), None, None),
        P(("expert", "gate"), None, None),
    )
    return jax.shard_map(
        per_device, mesh=mesh, in_specs=placed, out_specs=P("expert", "gate"), check_vma=False
    )
```

```python
import functools

import jax
import jax.numpy as jnp
from jax import lax
from jax.experimental import pallas as pl
from jax.experimental.pallas import tpu as pltpu
from jax.sharding import PartitionSpec as P


MESH = pl.DeviceIdType.MESH
CHUNKS = 4
SIDES = 2
PARTS = 3
STRIDE = 5


def routing(expert_ids, expert_count):
    row_count = expert_ids.shape[0]
    lanes = jnp.arange(expert_count, dtype=jnp.int32)[None, :]
    first = expert_ids[:, 0:1] == lanes
    second = expert_ids[:, 1:2] == lanes
    member = first | second
    rows = jnp.arange(row_count, dtype=jnp.int32)
    lower = (rows[:, None] > rows[None, :]).astype(jnp.bfloat16)
    before = jnp.dot(lower, member.astype(jnp.bfloat16), preferred_element_type=jnp.float32)
    before = before.astype(jnp.int32)
    return first, second, member, before


def factors(logits, first, second, pad_mask, expert_count):
    top = jnp.max(logits, axis=1, keepdims=True)
    terms = jnp.exp(logits - top)
    scale = pad_mask.astype(jnp.float32)[:, None] / jnp.sum(terms, axis=1, keepdims=True)
    factor0 = expert_count * jnp.sum(jnp.where(first, terms, 0.0), axis=1, keepdims=True) * scale
    factor1 = expert_count * jnp.sum(jnp.where(second, terms, 0.0), axis=1, keepdims=True) * scale
    return factor0, factor1


def copied(source, target, sem):
    return pltpu.make_async_copy(source, target, sem)


def sent(source, target, send_sem, recv_sem, device):
    return pltpu.make_async_remote_copy(
        src_ref=source,
        dst_ref=target,
        send_sem=send_sem,
        recv_sem=recv_sem,
        device_id=device,
        device_id_type=MESH,
    )


def table(values, index):
    out = values[0]
    for k in range(1, len(values)):
        out = jnp.where(index == k, values[k], out)
    return out


NONE, WAIT, END, LOCAL, EXPERT, LOGITS, FACTOR, JOIN_EDGE, JOIN, END_PART, EXPERT_PART, WEIGHTS, BACK, SETTLE, OPEN = range(15)
OWN, EDGE, INNER, FAR = range(4)


def coded(*jobs):
    return [kind * 16 + rel * 4 + c for kind, rel, c in jobs]


MIDDLE_JOBS = coded(
    (LOGITS, OWN, 0),
    (LOCAL, OWN, 0),
    (OPEN, OWN, 0),
    (LOCAL, OWN, 1),
    (LOCAL, OWN, 2),
    (LOCAL, OWN, 3),
    (END, OWN, 1),
    (WEIGHTS, OWN, 0),
    (EXPERT, OWN, 0),
    (FACTOR, OWN, 0),
    (WAIT, EDGE, 0),
    (LOCAL, EDGE, 0),
    (WAIT, INNER, 0),
    (END, INNER, 0),
    (LOCAL, INNER, 0),
    (EXPERT, OWN, 1),
    (EXPERT, OWN, 2),
    (WAIT, EDGE, 1),
    (LOCAL, EDGE, 1),
    (WAIT, INNER, 1),
    (END, INNER, 1),
    (LOCAL, INNER, 1),
    (EXPERT, OWN, 3),
    (EXPERT, EDGE, 0),
    (WAIT, EDGE, 2),
    (LOCAL, EDGE, 2),
    (WAIT, FAR, 0),
    (END, FAR, 0),
    (LOCAL, FAR, 0),
    (EXPERT, INNER, 0),
    (EXPERT, EDGE, 1),
    (WAIT, EDGE, 3),
    (LOCAL, EDGE, 3),
    (WAIT, FAR, 1),
    (END, FAR, 1),
    (LOCAL, FAR, 1),
    (EXPERT, INNER, 1),
    (WAIT, FAR, 2),
    (END, FAR, 2),
    (LOCAL, FAR, 2),
    (EXPERT, EDGE, 2),
    (WAIT, FAR, 3),
    (END, FAR, 3),
    (LOCAL, FAR, 3),
    (EXPERT, FAR, 0),
    (EXPERT, EDGE, 3),
    (EXPERT, FAR, 1),
    (WAIT, INNER, 2),
    (END, INNER, 2),
    (LOCAL, INNER, 2),
    (EXPERT, FAR, 2),
    (EXPERT, FAR, 3),
    (BACK, FAR, 0),
    (WAIT, INNER, 3),
    (END, INNER, 3),
    (LOCAL, INNER, 3),
    (END, OWN, 2),
    (END_PART, OWN, 0),
    (END_PART, OWN, 1),
    (END_PART, OWN, 2),
    (BACK, EDGE, 0),
    (BACK, OWN, 0),
    (EXPERT, INNER, 2),
    (EXPERT, INNER, 3),
    (BACK, INNER, 0),
    (JOIN_EDGE, OWN, 0),
    (JOIN_EDGE, INNER, 0),
    (JOIN_EDGE, FAR, 0),
    (JOIN, OWN, 0),
    (JOIN, INNER, 0),
    (JOIN, FAR, 0),
    (SETTLE, OWN, 0),
    (JOIN, EDGE, 0),
)
EDGE_JOBS = coded(
    (LOGITS, EDGE, 0),
    (LOCAL, EDGE, 1),
    (LOCAL, EDGE, 2),
    (LOCAL, EDGE, 3),
    (WEIGHTS, EDGE, 0),
    (EXPERT, EDGE, 0),
    (FACTOR, EDGE, 0),
    (EXPERT, EDGE, 1),
    (EXPERT, OWN, 0),
    (EXPERT, EDGE, 2),
    (EXPERT, OWN, 1),
    (EXPERT, EDGE, 3),
    (BACK, EDGE, 0),
    (EXPERT, INNER, 0),
    (EXPERT, INNER, 1),
    (EXPERT, FAR, 0),
    (EXPERT, FAR, 1),
    (EXPERT, FAR, 2),
    (EXPERT, FAR, 3),
    (BACK, FAR, 0),
    (EXPERT, INNER, 2),
    (EXPERT, INNER, 3),
    (BACK, INNER, 0),
    (EXPERT, OWN, 2),
    (EXPERT_PART, OWN, 0),
    (EXPERT_PART, OWN, 1),
    (EXPERT_PART, OWN, 2),
    (JOIN, EDGE, 0),
    (SETTLE, OWN, 0),
)


def exchange_kernel(
    gates,
    capacity,
    samples,
    ids,
    pads,
    gate_weight,
    up,
    down,
    out,
    blocks,
    named,
    mask,
    gatev,
    places,
    lower,
    onehot,
    dbuf,
    inc,
    upv,
    downv,
    hidden,
    obuf,
    logits,
    factor,
    edge_factor,
    ret,
    edge_ret,
    select,
    mixed,
    part,
    taken,
    own_sem,
    in_sem,
    ss,
    raw_r,
    id_r,
    pr,
    rr,
    er,
    gr,
    fr,
):
    chunks = CHUNKS
    local = SIDES * gates
    planes = blocks.shape[0]
    total = planes * local
    rows = blocks.shape[2]
    width = blocks.shape[3]
    share = width * chunks
    slots = local * capacity
    few = capacity // PARTS
    bf16, f32 = jnp.bfloat16, jnp.float32
    e = lax.axis_index("expert")
    g = lax.axis_index("gate")
    z = e // SIDES
    y = lax.rem(e, SIDES)
    mine = y * gates + g
    low = z < planes // 2
    toward = jnp.where(low, 1, -1)
    near = jnp.where(low, 0, planes - 1)
    far = planes - 1 - near
    edge = z == near
    middle = jnp.logical_not(edge)
    mid = near + toward
    inner = z + toward

    def plane_of(rel):
        return table((mid, near, mid + toward, far), rel)

    def at(plane, i):
        return (plane * SIDES + i // gates, lax.rem(i, gates))

    barrier = pltpu.get_barrier_semaphore()

    inputs = (
        copied(ids, named.at[z], in_sem.at[0]),
        copied(pads, mask, in_sem.at[1]),
        copied(gate_weight, gatev, in_sem.at[2]),
    )
    for copy in inputs:
        copy.start()
    own = [
        copied(samples.at[:, pl.ds(c * width, width)], blocks.at[z, c], own_sem)
        for c in range(chunks)
    ]
    for copy in own:
        copy.start()
    def greet(d, carry):
        plane = z + table((toward, -toward, 0), d // local)
        i = lax.rem(mine + d, local)

        told = (plane >= 0) & (plane < planes) & (d != 2 * local)

        @pl.when(told & (edge | low | (plane != inner)))
        def _():
            pl.semaphore_signal(barrier, inc=1, device_id=at(plane, i), device_id_type=MESH)

        return carry

    with jax.named_scope("greet"):
        lax.fori_loop(0, 3 * local, greet, 0)
    greeted = jnp.where(edge | low, 2, 3) * local - 1
    late = middle & low

    weights = [copied(down.at[0], downv, in_sem.at[0])]
    for c in range(chunks):
        for k in range(gates):
            weights.append(
                copied(
                    up.at[0, pl.ds(k * share + c * width, width)],
                    upv.at[c, pl.ds(k * width, width)],
                    own_sem,
                )
            )

    earlier = lax.broadcasted_iota(jnp.int32, (rows, rows), 0)
    later = lax.broadcasted_iota(jnp.int32, (rows, rows), 1)
    with jax.named_scope("lower"):
        lower[...] = jnp.where(earlier < later, 1.0, 0.0).astype(bf16)

    def end_index(rel):
        return jnp.where(rel == OWN, planes, planes - 1 + rel)

    def locate(j):
        lanes = lax.broadcasted_iota(jnp.int32, (total, rows), 0)
        member = (named[j, 0:1, :] == lanes) | (named[j, 1:2, :] == lanes)
        flags = jnp.where(member, 1.0, 0.0).astype(bf16)
        before = jnp.dot(flags, lower[...], preferred_element_type=f32)
        places[j] = jnp.where(member, before, -1.0)

    def build(j, index, plane):
        ranks = lax.broadcasted_iota(jnp.int32, (capacity, rows), 0).astype(f32)

        def one(i, carry):
            line = places[j, pl.ds(plane * local + i, 1), :]
            found = jnp.where(line == ranks, 1.0, 0.0).astype(bf16)
            onehot[index, :, i] = found.reshape(PARTS, few, rows)
            return carry

        lax.fori_loop(0, local, one, 0)

    def pick(index, part, j, c):
        dbuf[index, c, part] = (
            jnp.dot(
                onehot[index, part].reshape(local * few, rows),
                blocks[j, c],
                preferred_element_type=f32,
            )
            .astype(bf16)
            .reshape(local, few, width)
        )

    def hand_out(j, rel, c, to_end):
        index = jnp.where(to_end, end_index(rel), rel)
        plane = jnp.where(to_end, near, z)

        def give(d, carry):
            i = lax.rem(mine + STRIDE * d, local)
            piece = dbuf.at[index, c, :, i]
            place = inc.at[j, c, y, :, :, pl.ds(g * width, width)]
            here = jnp.logical_not(to_end) & (d == 0)

            @pl.when(here)
            def _():
                copied(piece, place, pr.at[j, c]).start()

            @pl.when(jnp.logical_not(here))
            def _():
                sent(piece, place, ss, pr.at[j, c], at(plane, i)).start()

            return carry

        lax.fori_loop(0, local, give, 0)

    with jax.named_scope("inputs"):
        for copy in inputs:
            copy.wait()
    first = jnp.where(edge, EDGE, planes)
    with jax.named_scope("prepare"):
        locate(z)
        build(z, first, near)
    with jax.named_scope("samples"):
        copied(blocks.at[z], blocks.at[z], own_sem).wait()
    for q in range(PARTS):
        pick(first, q, z, 0)
    with jax.named_scope("barrier"):
        pl.semaphore_wait(barrier, greeted)
    hand_out(z, jnp.where(edge, EDGE, OWN), 0, middle)

    def ids_on(j):
        return sent(named.at[j], named.at[j], ss, id_r.at[j], at(inner, mine))

    def shift(j, c):
        return sent(
            blocks.at[j, c], blocks.at[j, c], ss, raw_r.at[j, c], at(inner, mine)
        )

    def open_inner():
        ids_on(z).start()
        for c in range(2):
            shift(z, c).start()

    @pl.when(jnp.logical_not(late))
    def _():
        open_inner()

    @pl.when(edge)
    def _():
        for c in range(2, chunks):
            shift(z, c).start()

    for copy in weights:
        copy.start()

    @pl.when(middle)
    def _():
        build(z, OWN, z)

    gate_routes = []
    for d in range(1, gates):
        t = lax.rem(g + d, gates)
        gate_routes.append(sent(logits.at[g], logits.at[g], ss, gr, (e, t)))
    edge_route = sent(factor, edge_factor, ss, fr, at(inner, mine))
    part_route = sent(part, taken, ss, fr, at(near, mine))

    def wait(j, rel, c):
        with jax.named_scope("wait_raw"):
            copied(blocks.at[j, c], blocks.at[j, c], raw_r.at[j, c]).wait()

        @pl.when((c == 0) & jnp.logical_not(late & (rel == INNER)))
        def _():
            copied(named.at[j], named.at[j], id_r.at[j]).wait()

        @pl.when(rel == EDGE)
        def _():
            @pl.when(c == 0)
            def _():
                ids_on(j).start()

            shift(j, c).start()

            @pl.when(c == chunks - 1)
            def _():
                for k in range(2, chunks):
                    shift(z, k).start()

        @pl.when(c == 0)
        def _():
            locate(j)

            @pl.when(rel != EDGE)
            def _():
                build(j, end_index(rel), near)

            build(j, rel, z)

    def dispatch(j, rel, c, to_end):
        index = jnp.where(to_end, end_index(rel), rel)
        with jax.named_scope("pick"):
            for part in range(PARTS):
                pick(index, part, j, c)
        hand_out(j, rel, c, to_end)

    def dispatch_part(part):
        c = chunks - 1
        pick(planes, part, z, c)

        def give(d, carry):
            i = lax.rem(mine + STRIDE * d, local)
            sent(
                dbuf.at[planes, c, part, i],
                inc.at[z, c, y, part, :, pl.ds(g * width, width)],
                ss,
                raw_r.at[near, part],
                at(near, i),
            ).start()
            return carry

        lax.fori_loop(0, local, give, 0)

    def give_back(j, part):
        ends = (j == 0) | (j == planes - 1)
        joined = ends & (j != z)
        plane = jnp.where(joined, jnp.where(j == 0, 1, planes - 2), j)

        def hand(d, carry):
            i = lax.rem(mine + d, local)
            side, k = i // gates, lax.rem(i, gates)
            here = (plane == z) & (d == 0)

            def hand_to(buffer, sem):
                if part is None:
                    block, spot = obuf.at[j, k, side], buffer.at[z, mine]
                else:
                    block, spot = obuf.at[j, k, side, part], buffer.at[z, mine, part]

                @pl.when(here)
                def _():
                    copied(block, spot, sem.at[z]).start()

                @pl.when(jnp.logical_not(here))
                def _():
                    sent(block, spot, ss, sem.at[z], at(plane, i)).start()

            @pl.when(joined)
            def _():
                hand_to(edge_ret, er)

            @pl.when(jnp.logical_not(joined))
            def _():
                hand_to(ret, rr)

            return carry

        lax.fori_loop(0, local, hand, 0)

    tile = 256
    inner_tiles = [slice(n, n + tile) for n in range(0, hidden.shape[4], tile)]
    out_width = downv.shape[1] // gates

    def expert(j, c):
        with jax.named_scope("wait_inc"):
            copied(inc.at[j, c], inc.at[j, c], pr.at[j, c]).wait()
        taken_in = inc[j, c].reshape(SIDES * capacity, share)
        for cols in inner_tiles:
            acc = jnp.dot(taken_in, upv[c, :, cols], preferred_element_type=f32)
            acc = acc.reshape(SIDES, PARTS, few, tile)

            @pl.when(c == 0)
            def _():
                hidden[j, :, :, :, cols] = acc

            @pl.when(c != 0)
            def _():
                hidden[j, :, :, :, cols] += acc

    def project(j):
        active = jnp.maximum(hidden[j], 0.0).astype(bf16).reshape(SIDES * capacity, -1)
        for k in range(gates):
            obuf[j, k] = (
                jnp.dot(
                    active,
                    downv[:, k * out_width : (k + 1) * out_width],
                    preferred_element_type=f32,
                )
                .astype(bf16)
                .reshape(SIDES, PARTS, few, out_width)
            )
        with jax.named_scope("back"):
            give_back(j, None)

    def expert_part(j, part):
        c = chunks - 1
        with jax.named_scope("wait_part"):
            arriving = inc.at[j, c, :, part]
            copied(arriving, arriving, raw_r.at[near, part]).wait()
        taken_in = inc[j, c, :, part].reshape(SIDES * few, share)
        active = []
        for cols in inner_tiles:
            acc = jnp.dot(taken_in, upv[c, :, cols], preferred_element_type=f32)
            acc += hidden[j, :, part, :, cols].reshape(SIDES * few, tile)
            active.append(jnp.maximum(acc, 0.0).astype(bf16))
        active = jnp.concatenate(active, axis=1)
        for k in range(gates):
            obuf[j, k, :, part] = (
                jnp.dot(
                    active,
                    downv[:, k * out_width : (k + 1) * out_width],
                    preferred_element_type=f32,
                )
                .astype(bf16)
                .reshape(SIDES, few, out_width)
            )
        with jax.named_scope("back"):
            give_back(j, part)

    def gate_logits():
        partial = 0.0
        for c in range(chunks):
            partial += lax.dot_general(
                gatev[:, c * width : (c + 1) * width],
                blocks[z, c],
                (((1,), (1,)), ((), ())),
                preferred_element_type=f32,
            )
        logits[g] = partial
        for copy in gate_routes:
            copy.start()

    def gate_factor():
        with jax.named_scope("wait_gate"):
            others = logits.at[pl.ds(0, gates - 1)]
            copied(others, others, gr).wait()
        summed = logits[0]
        for k in range(1, gates):
            summed += logits[k]
        top = jnp.max(summed, axis=0, keepdims=True)
        terms = jnp.exp(summed - top)
        scale = mask[...].astype(f32).reshape(1, rows) / jnp.sum(terms, axis=0, keepdims=True)
        factor[...] = total * terms * scale

        @pl.when(edge)
        def _():
            edge_route.start()

    def join(j, p, weight, returned, sem, index, first):
        ranks = lax.broadcasted_iota(jnp.int32, (capacity, rows), 0).astype(f32)

        def one(i, carry):
            line = places[j, pl.ds(p * local + i, 1), :]
            scale = weight[pl.ds(p * local + i, 1), :]
            select[pl.ds(pl.multiple_of(i * capacity, capacity), capacity), :] = jnp.where(
                line == ranks, scale, 0.0
            ).astype(bf16)
            return carry

        lax.fori_loop(0, local, one, 0)
        with jax.named_scope("wait_ret"):
            copied(returned.at[p], returned.at[p], sem.at[p]).wait()
        found = lax.dot_general(
            select[...],
            returned[p].reshape(slots, out_width),
            (((0,), (0,)), ((), ())),
            preferred_element_type=f32,
        )

        @pl.when(first)
        def _():
            mixed[index] = found

        @pl.when(jnp.logical_not(first))
        def _():
            mixed[index] += found

    def settle():
        others = logits.at[pl.ds(0, gates - 1)]
        copied(others, others, ss).wait()
        ids_on(z).wait_send()
        copied(blocks.at[z], blocks.at[z], ss).wait()
        within = dbuf.at[EDGE, :, :, pl.ds(0, local - 1)]
        copied(within, within, ss).wait()

        @pl.when(middle)
        def _():
            ids_on(near).wait_send()
            copied(blocks.at[near], blocks.at[near], ss).wait()
            more = dbuf.at[pl.ds(0, planes - 1), :, :, pl.ds(0, local - 1)]
            copied(more, more, ss).wait()
            ahead = dbuf.at[pl.ds(planes, planes - 1)]
            copied(ahead, ahead, ss).wait()

    def job(t, carry):
        code = jnp.where(edge, table(EDGE_JOBS, t), table(MIDDLE_JOBS, t))
        kind, rel, c = code // 16, lax.rem(code // 4, 4), lax.rem(code, 4)
        j = plane_of(rel)

        @pl.when(kind == WAIT)
        def _():
            wait(j, rel, c)

        @pl.when((kind == END) | (kind == LOCAL))
        def _():
            dispatch(j, rel, c, kind == END)

        @pl.when(kind == EXPERT)
        def _():
            expert(j, c)

        @pl.when(kind == BACK)
        def _():
            project(j)

        @pl.when(kind == END_PART)
        def _():
            dispatch_part(c)

        @pl.when(kind == EXPERT_PART)
        def _():
            expert_part(j, c)

        @pl.when(kind == WEIGHTS)
        def _():
            with jax.named_scope("wait_w"):
                weights[0].wait()
                copied(upv, upv, own_sem).wait()

        @pl.when(kind == LOGITS)
        def _():
            gate_logits()

        @pl.when(kind == FACTOR)
        def _():
            gate_factor()

        @pl.when(kind == JOIN_EDGE)
        def _():
            @pl.when(rel == OWN)
            def _():
                copied(edge_factor, edge_factor, fr).wait()

            join(near, j, edge_factor, edge_ret, er, 0, rel == OWN)

            @pl.when(rel == FAR)
            def _():
                part[...] = mixed[0].astype(bf16)
                part_route.start()

        @pl.when((kind == OPEN) & late)
        def _():
            copied(named.at[inner], named.at[inner], id_r.at[inner]).wait()
            open_inner()

        @pl.when(kind == SETTLE)
        def _():
            settle()

        @pl.when(kind == JOIN)
        def _():
            join(z, j, factor, ret, rr, 1, edge | (rel == OWN))

        return carry

    lax.fori_loop(0, jnp.where(edge, len(EDGE_JOBS), len(MIDDLE_JOBS)), job, 0)

    @pl.when(edge)
    def _():
        with jax.named_scope("wait_taken"):
            copied(taken, taken, fr).wait()
        with jax.named_scope("fin_add"):
            out[...] = (mixed[1] + taken[...].astype(f32)).astype(bf16)

    @pl.when(middle)
    def _():
        with jax.named_scope("fin_add"):
            out[...] = mixed[1].astype(bf16)

    handed = ret.at[pl.ds(0, planes - 1)]
    few_more = ret.at[0, pl.ds(0, local - 2)]
    one_more = ret.at[0, 0]
    copied(handed, handed, ss).wait()
    copied(few_more, few_more, ss).wait()

    @pl.when(edge)
    def _():
        copied(one_more, one_more, ss).wait()
        edge_route.wait_send()

    @pl.when(middle)
    def _():
        part_route.wait_send()


def exchange(samples, ids, pads, gate_weight, up, down, planes, gates, capacity):
    rows, share = samples.shape
    local = SIDES * gates
    total = planes * local
    width = share // CHUNKS
    depth, inner = up.shape[1:]
    outer = down.shape[2]
    out_width = outer // gates
    bf16, f32 = jnp.bfloat16, jnp.float32
    dma = pltpu.SemaphoreType.DMA
    hbm = pl.BlockSpec(memory_space=pl.ANY)
    slots = local * capacity
    few = capacity // PARTS
    kinds = 2 * planes - 1
    return pl.pallas_call(
        functools.partial(exchange_kernel, gates, capacity),
        out_shape=pltpu.VMEM((rows, out_width), bf16),
        in_specs=[hbm] * 6,
        out_specs=pl.BlockSpec(memory_space=pltpu.VMEM),
        scratch_shapes=[
            pltpu.VMEM((planes, CHUNKS, rows, width), bf16),
            pltpu.VMEM((planes,) + ids.shape, jnp.int32),
            pltpu.VMEM(pads.shape, jnp.int32),
            pltpu.VMEM(gate_weight.shape, bf16),
            pltpu.VMEM((planes, total, rows), f32),
            pltpu.VMEM((rows, rows), bf16),
            pltpu.VMEM((kinds, PARTS, local, few, rows), bf16),
            pltpu.VMEM((kinds, CHUNKS, PARTS, local, few, width), bf16),
            pltpu.VMEM((planes, CHUNKS, SIDES, PARTS, few, gates * width), bf16),
            pltpu.VMEM((CHUNKS, depth // CHUNKS, inner), bf16),
            pltpu.VMEM((inner, outer), bf16),
            pltpu.VMEM((planes, SIDES, PARTS, few, inner), f32),
            pltpu.VMEM((planes, gates, SIDES, PARTS, few, out_width), bf16),
            pltpu.VMEM((gates, total, rows), f32),
            pltpu.VMEM((total, rows), f32),
            pltpu.VMEM((total, rows), f32),
            pltpu.VMEM((planes, local, PARTS, few, out_width), bf16),
            pltpu.VMEM((planes, local, PARTS, few, out_width), bf16),
            pltpu.VMEM((slots, rows), bf16),
            pltpu.VMEM((2, rows, out_width), f32),
            pltpu.VMEM((rows, out_width), bf16),
            pltpu.VMEM((rows, out_width), bf16),
            dma,
            dma((3,)),
            dma,
            dma((planes, CHUNKS)),
            dma((planes,)),
            dma((planes, CHUNKS)),
            dma((planes,)),
            dma((planes,)),
            dma,
            dma,
        ],
        compiler_params=pltpu.CompilerParams(
            collective_id=0, has_side_effects=True, vmem_limit_bytes=58 << 20
        ),
    )(samples, ids, pads, gate_weight, up, down)


def in_one_kernel(samples, gate_weight, expert_ids, pad_mask, up_weight, down_weight):
    group_count = lax.axis_size("expert")
    gate_count = lax.axis_size("gate")
    expert_count = group_count * gate_count
    return exchange(
        samples,
        expert_ids.T,
        pad_mask,
        gate_weight.T,
        up_weight,
        down_weight,
        group_count // SIDES,
        gate_count,
        4 * samples.shape[0] // expert_count,
    )


def fits(samples, up_weight, down_weight):
    group_count = lax.axis_size("expert")
    capacity = 4 * samples.shape[0] // (group_count * lax.axis_size("gate"))
    planes = group_count // SIDES
    held = 2 * (planes * samples.size * 3 + up_weight.size + down_weight.size)
    return planes == 4 and group_count % SIDES == 0 and capacity % (16 * PARTS) == 0 and held < 40 << 20


def per_device(samples, gate_weight, expert_ids, pad_mask, up_weight, down_weight):
    if fits(samples, up_weight, down_weight):
        return in_one_kernel(
            samples, gate_weight, expert_ids, pad_mask, up_weight, down_weight
        )
    row_count, share = samples.shape
    group_count = lax.axis_size("expert")
    gate_count = lax.axis_size("gate")
    expert_count = group_count * gate_count
    capacity = 4 * row_count // expert_count
    partial = jnp.dot(samples, gate_weight, preferred_element_type=jnp.float32)
    logits = jnp.sum(lax.all_gather(partial, "gate"), axis=0)
    first, second, member, before = routing(expert_ids, expert_count)
    place = jnp.where(member, before, -1).T
    ranks = jnp.arange(capacity, dtype=jnp.int32)
    send = (place[:, None, :] == ranks[None, :, None]).astype(jnp.bfloat16)
    outgoing = jnp.dot(
        send.reshape(expert_count * capacity, row_count), samples, preferred_element_type=jnp.float32
    ).astype(jnp.bfloat16)
    incoming = lax.all_to_all(
        outgoing.reshape(expert_count, capacity, share),
        ("expert", "gate"),
        split_axis=0,
        concat_axis=0,
        tiled=True,
    ).reshape(group_count, gate_count, capacity, share)
    hidden = 0.0
    for g in range(gate_count):
        hidden += jnp.dot(
            incoming[:, g].reshape(group_count * capacity, share),
            up_weight[0, g * share : (g + 1) * share],
            preferred_element_type=jnp.float32,
        )
    active = jnp.maximum(hidden, 0.0).astype(jnp.bfloat16)
    expert_out = jnp.dot(active, down_weight[0], preferred_element_type=jnp.float32).astype(
        jnp.bfloat16
    )
    out_share = expert_out.shape[1] // gate_count
    outbound = expert_out.reshape(group_count, capacity, gate_count, out_share)
    outbound = outbound.transpose(0, 2, 1, 3).reshape(expert_count, capacity, out_share)
    returned = lax.all_to_all(
        outbound, ("expert", "gate"), split_axis=0, concat_axis=0, tiled=True
    ).reshape(expert_count * capacity, out_share)
    factor0, factor1 = factors(logits, first, second, pad_mask, expert_count)
    slots = jnp.arange(expert_count * capacity, dtype=jnp.int32)[None, :]
    mixed = 0.0
    for k, (chosen, factor) in enumerate(((first, factor0), (second, factor1))):
        rank = jnp.sum(jnp.where(chosen, before, 0), axis=1, keepdims=True)
        position = expert_ids[:, k : k + 1] * capacity + rank
        pick = (position == slots).astype(jnp.bfloat16)
        mixed += factor * jnp.dot(pick, returned, preferred_element_type=jnp.float32)
    return mixed.astype(jnp.bfloat16)


def solution(mesh):
    placed = (
        P("expert", "gate"),
        P("gate", None),
        P("expert", None),
        P("expert"),
        P(("expert", "gate"), None, None),
        P(("expert", "gate"), None, None),
    )
    return jax.shard_map(
        per_device, mesh=mesh, in_specs=placed, out_specs=P("expert", "gate"), check_vma=False
    )
```

```python
import functools

import jax
import jax.numpy as jnp
from jax import lax
from jax.experimental import pallas as pl
from jax.experimental.pallas import tpu as pltpu
from jax.sharding import PartitionSpec as P


MESH = pl.DeviceIdType.MESH
CHUNKS = 4
SIDES = 2
PARTS = 3
STRIDE = 5


def routing(expert_ids, expert_count):
    row_count = expert_ids.shape[0]
    lanes = jnp.arange(expert_count, dtype=jnp.int32)[None, :]
    first = expert_ids[:, 0:1] == lanes
    second = expert_ids[:, 1:2] == lanes
    member = first | second
    rows = jnp.arange(row_count, dtype=jnp.int32)
    lower = (rows[:, None] > rows[None, :]).astype(jnp.bfloat16)
    before = jnp.dot(lower, member.astype(jnp.bfloat16), preferred_element_type=jnp.float32)
    before = before.astype(jnp.int32)
    return first, second, member, before


def factors(logits, first, second, pad_mask, expert_count):
    top = jnp.max(logits, axis=1, keepdims=True)
    terms = jnp.exp(logits - top)
    scale = pad_mask.astype(jnp.float32)[:, None] / jnp.sum(terms, axis=1, keepdims=True)
    factor0 = expert_count * jnp.sum(jnp.where(first, terms, 0.0), axis=1, keepdims=True) * scale
    factor1 = expert_count * jnp.sum(jnp.where(second, terms, 0.0), axis=1, keepdims=True) * scale
    return factor0, factor1


def copied(source, target, sem):
    return pltpu.make_async_copy(source, target, sem)


def sent(source, target, send_sem, recv_sem, device):
    return pltpu.make_async_remote_copy(
        src_ref=source,
        dst_ref=target,
        send_sem=send_sem,
        recv_sem=recv_sem,
        device_id=device,
        device_id_type=MESH,
    )


def table(values, index):
    out = values[0]
    for k in range(1, len(values)):
        out = jnp.where(index == k, values[k], out)
    return out


NONE, WAIT, END, LOCAL, EXPERT, LOGITS, FACTOR, JOIN_EDGE, JOIN, END_PART, EXPERT_PART, WEIGHTS, BACK, SETTLE, OPEN = range(15)
OWN, EDGE, INNER, FAR = range(4)


def coded(*jobs):
    return [kind * 16 + rel * 4 + c for kind, rel, c in jobs]


MIDDLE_JOBS = coded(
    (LOGITS, OWN, 0),
    (LOCAL, OWN, 0),
    (OPEN, OWN, 0),
    (LOCAL, OWN, 1),
    (LOCAL, OWN, 2),
    (LOCAL, OWN, 3),
    (END, OWN, 1),
    (WEIGHTS, OWN, 0),
    (EXPERT, OWN, 0),
    (FACTOR, OWN, 0),
    (WAIT, EDGE, 0),
    (LOCAL, EDGE, 0),
    (WAIT, INNER, 0),
    (END, INNER, 0),
    (LOCAL, INNER, 0),
    (EXPERT, OWN, 1),
    (EXPERT, OWN, 2),
    (WAIT, EDGE, 1),
    (LOCAL, EDGE, 1),
    (WAIT, INNER, 1),
    (END, INNER, 1),
    (LOCAL, INNER, 1),
    (EXPERT, OWN, 3),
    (EXPERT, EDGE, 0),
    (WAIT, EDGE, 2),
    (LOCAL, EDGE, 2),
    (WAIT, FAR, 0),
    (END, FAR, 0),
    (LOCAL, FAR, 0),
    (EXPERT, INNER, 0),
    (EXPERT, EDGE, 1),
    (WAIT, EDGE, 3),
    (LOCAL, EDGE, 3),
    (WAIT, FAR, 1),
    (END, FAR, 1),
    (LOCAL, FAR, 1),
    (EXPERT, INNER, 1),
    (WAIT, FAR, 2),
    (END, FAR, 2),
    (LOCAL, FAR, 2),
    (EXPERT, EDGE, 2),
    (WAIT, FAR, 3),
    (END, FAR, 3),
    (LOCAL, FAR, 3),
    (EXPERT, FAR, 0),
    (EXPERT, EDGE, 3),
    (EXPERT, FAR, 1),
    (WAIT, INNER, 2),
    (END, INNER, 2),
    (LOCAL, INNER, 2),
    (EXPERT, FAR, 2),
    (EXPERT, FAR, 3),
    (BACK, FAR, 0),
    (WAIT, INNER, 3),
    (END, INNER, 3),
    (LOCAL, INNER, 3),
    (END, OWN, 2),
    (END_PART, OWN, 0),
    (END_PART, OWN, 1),
    (END_PART, OWN, 2),
    (BACK, EDGE, 0),
    (BACK, OWN, 0),
    (EXPERT, INNER, 2),
    (EXPERT, INNER, 3),
    (BACK, INNER, 0),
    (JOIN_EDGE, OWN, 0),
    (JOIN_EDGE, INNER, 0),
    (JOIN_EDGE, FAR, 0),
    (JOIN, OWN, 0),
    (JOIN, INNER, 0),
    (JOIN, FAR, 0),
    (SETTLE, OWN, 0),
    (JOIN, EDGE, 0),
)
EDGE_JOBS = coded(
    (LOGITS, EDGE, 0),
    (LOCAL, EDGE, 1),
    (LOCAL, EDGE, 2),
    (LOCAL, EDGE, 3),
    (WEIGHTS, EDGE, 0),
    (EXPERT, EDGE, 0),
    (FACTOR, EDGE, 0),
    (EXPERT, EDGE, 1),
    (EXPERT, OWN, 0),
    (EXPERT, EDGE, 2),
    (EXPERT, OWN, 1),
    (EXPERT, EDGE, 3),
    (BACK, EDGE, 0),
    (EXPERT, INNER, 0),
    (EXPERT, INNER, 1),
    (EXPERT, FAR, 0),
    (EXPERT, FAR, 1),
    (EXPERT, FAR, 2),
    (EXPERT, FAR, 3),
    (BACK, FAR, 0),
    (EXPERT, INNER, 2),
    (EXPERT, INNER, 3),
    (BACK, INNER, 0),
    (EXPERT, OWN, 2),
    (EXPERT_PART, OWN, 0),
    (EXPERT_PART, OWN, 1),
    (EXPERT_PART, OWN, 2),
    (JOIN, EDGE, 0),
    (SETTLE, OWN, 0),
)


def exchange_kernel(
    gates,
    capacity,
    samples,
    ids,
    pads,
    gate_weight,
    up,
    down,
    out,
    blocks,
    named,
    mask,
    gatev,
    places,
    lower,
    onehot,
    dbuf,
    inc,
    upv,
    downv,
    hidden,
    obuf,
    logits,
    factor,
    edge_factor,
    ret,
    edge_ret,
    select,
    mixed,
    part,
    taken,
    own_sem,
    in_sem,
    ss,
    raw_r,
    id_r,
    pr,
    rr,
    er,
    gr,
    fr,
):
    chunks = CHUNKS
    local = SIDES * gates
    planes = blocks.shape[0]
    total = planes * local
    rows = blocks.shape[2]
    width = blocks.shape[3]
    share = width * chunks
    slots = local * capacity
    few = capacity // PARTS
    bf16, f32 = jnp.bfloat16, jnp.float32
    e = lax.axis_index("expert")
    g = lax.axis_index("gate")
    z = e // SIDES
    y = lax.rem(e, SIDES)
    mine = y * gates + g
    low = z < planes // 2
    toward = jnp.where(low, 1, -1)
    near = jnp.where(low, 0, planes - 1)
    far = planes - 1 - near
    edge = z == near
    middle = jnp.logical_not(edge)
    mid = near + toward
    inner = z + toward

    def plane_of(rel):
        return table((mid, near, mid + toward, far), rel)

    def row(j, reader):
        return lax.rem(j - reader + planes, planes) - 1

    def at(plane, i):
        return (plane * SIDES + i // gates, lax.rem(i, gates))

    barrier = pltpu.get_barrier_semaphore()

    inputs = (
        copied(ids, named.at[z], in_sem.at[0]),
        copied(pads, mask, in_sem.at[1]),
        copied(gate_weight, gatev, in_sem.at[2]),
    )
    for copy in inputs:
        copy.start()
    own = [
        copied(samples.at[:, pl.ds(c * width, width)], blocks.at[z, c], own_sem)
        for c in range(chunks)
    ]
    for copy in own:
        copy.start()
    greeting = (
        jnp.where(edge, toward, 0),
        jnp.where(edge, 0, -toward),
        jnp.where(edge, -toward, toward),
    )

    def greet(d, carry):
        plane = z + table(greeting, d // local)
        i = lax.rem(mine + d, local)

        told = (plane >= 0) & (plane < planes) & ((plane != z) | (i != mine))

        @pl.when(told & (edge | low | (plane != inner)))
        def _():
            pl.semaphore_signal(barrier, inc=1, device_id=at(plane, i), device_id_type=MESH)

        return carry

    with jax.named_scope("greet"):
        lax.fori_loop(0, 3 * local, greet, 0)
    greeted = jnp.where(edge | low, 2, 3) * local - 1
    late = middle & low

    weights = [copied(down.at[0], downv, in_sem.at[0])]
    for c in range(chunks):
        for k in range(gates):
            weights.append(
                copied(
                    up.at[0, pl.ds(k * share + c * width, width)],
                    upv.at[c, pl.ds(k * width, width)],
                    own_sem,
                )
            )

    earlier = lax.broadcasted_iota(jnp.int32, (rows, rows), 0)
    later = lax.broadcasted_iota(jnp.int32, (rows, rows), 1)
    with jax.named_scope("lower"):
        lower[...] = jnp.where(earlier < later, 1.0, 0.0).astype(bf16)

    def end_index(rel):
        return jnp.where(rel == OWN, planes, planes - 1 + rel)

    def locate(j):
        lanes = lax.broadcasted_iota(jnp.int32, (total, rows), 0)
        member = (named[j, 0:1, :] == lanes) | (named[j, 1:2, :] == lanes)
        flags = jnp.where(member, 1.0, 0.0).astype(bf16)
        before = jnp.dot(flags, lower[...], preferred_element_type=f32)
        places[j] = jnp.where(member, before, -1.0)

    def build(j, index, plane):
        ranks = lax.broadcasted_iota(jnp.int32, (capacity, rows), 0).astype(f32)

        def one(i, carry):
            line = places[j, pl.ds(plane * local + i, 1), :]
            found = jnp.where(line == ranks, 1.0, 0.0).astype(bf16)
            onehot[index, :, i] = found.reshape(PARTS, few, rows)
            return carry

        lax.fori_loop(0, local, one, 0)

    def pick(index, part, j, c):
        dbuf[index, c, part] = (
            jnp.dot(
                onehot[index, part].reshape(local * few, rows),
                blocks[j, c],
                preferred_element_type=f32,
            )
            .astype(bf16)
            .reshape(local, few, width)
        )

    def hand_out(j, rel, c, to_end):
        index = jnp.where(to_end, end_index(rel), rel)
        plane = jnp.where(to_end, near, z)

        def give(d, carry):
            i = lax.rem(mine + STRIDE * d, local)
            piece = dbuf.at[index, c, :, i]
            place = inc.at[j, c, y, :, :, pl.ds(g * width, width)]
            here = jnp.logical_not(to_end) & (d == 0)

            @pl.when(here)
            def _():
                copied(piece, place, pr.at[j, c]).start()

            @pl.when(jnp.logical_not(here))
            def _():
                sent(piece, place, ss, pr.at[j, c], at(plane, i)).start()

            return carry

        lax.fori_loop(0, local, give, 0)

    with jax.named_scope("inputs"):
        for copy in inputs:
            copy.wait()
    first = jnp.where(edge, EDGE, planes)
    with jax.named_scope("prepare"):
        locate(z)
        build(z, first, near)
    with jax.named_scope("samples"):
        copied(blocks.at[z], blocks.at[z], own_sem).wait()
    for q in range(PARTS):
        pick(first, q, z, 0)
    with jax.named_scope("barrier"):
        pl.semaphore_wait(barrier, greeted)
    hand_out(z, jnp.where(edge, EDGE, OWN), 0, middle)

    def ids_on(j):
        return sent(named.at[j], named.at[j], ss, id_r.at[row(j, inner)], at(inner, mine))

    def shift(j, c):
        return sent(
            blocks.at[j, c], blocks.at[j, c], ss, raw_r.at[row(j, inner), c], at(inner, mine)
        )

    def open_inner():
        ids_on(z).start()
        for c in range(2):
            shift(z, c).start()

    @pl.when(jnp.logical_not(late))
    def _():
        open_inner()

    @pl.when(edge)
    def _():
        for c in range(2, chunks):
            shift(z, c).start()

    for copy in weights:
        copy.start()

    @pl.when(middle)
    def _():
        build(z, OWN, z)

    gate_routes = []
    for d in range(1, gates):
        t = lax.rem(g + d, gates)
        gate_routes.append(sent(logits.at[g], logits.at[g], ss, gr, (e, t)))
    edge_route = sent(factor, edge_factor, ss, fr, at(inner, mine))
    part_route = sent(part, taken, ss, fr, at(near, mine))

    def wait(j, rel, c):
        with jax.named_scope("wait_raw"):
            copied(blocks.at[j, c], blocks.at[j, c], raw_r.at[row(j, z), c]).wait()

        @pl.when((c == 0) & jnp.logical_not(late & (rel == INNER)))
        def _():
            copied(named.at[j], named.at[j], id_r.at[row(j, z)]).wait()

        @pl.when(rel == EDGE)
        def _():
            @pl.when(c == 0)
            def _():
                ids_on(j).start()

            shift(j, c).start()

            @pl.when(c == chunks - 1)
            def _():
                for k in range(2, chunks):
                    shift(z, k).start()

        @pl.when(c == 0)
        def _():
            locate(j)

            @pl.when(rel != EDGE)
            def _():
                build(j, end_index(rel), near)

            build(j, rel, z)

    def dispatch(j, rel, c, to_end):
        index = jnp.where(to_end, end_index(rel), rel)
        with jax.named_scope("pick"):
            for part in range(PARTS):
                pick(index, part, j, c)
        hand_out(j, rel, c, to_end)

    def dispatch_part(part):
        c = chunks - 1
        pick(planes, part, z, c)

        def give(d, carry):
            i = lax.rem(mine + STRIDE * d, local)
            sent(
                dbuf.at[planes, c, part, i],
                inc.at[z, c, y, part, :, pl.ds(g * width, width)],
                ss,
                raw_r.at[row(z, near), part],
                at(near, i),
            ).start()
            return carry

        lax.fori_loop(0, local, give, 0)

    def give_back(j, part):
        ends = (j == 0) | (j == planes - 1)
        joined = ends & (j != z)
        plane = jnp.where(joined, jnp.where(j == 0, 1, planes - 2), j)

        def hand(d, carry):
            i = lax.rem(mine + d, local)
            side, k = i // gates, lax.rem(i, gates)
            here = (plane == z) & (d == 0)

            def hand_to(buffer, sem):
                if part is None:
                    block, spot = obuf.at[j, k, side], buffer.at[z, mine]
                else:
                    block, spot = obuf.at[j, k, side, part], buffer.at[z, mine, part]

                @pl.when(here)
                def _():
                    copied(block, spot, sem).start()

                @pl.when(jnp.logical_not(here))
                def _():
                    sent(block, spot, ss, sem, at(plane, i)).start()

            @pl.when(joined)
            def _():
                hand_to(edge_ret, er)

            @pl.when(jnp.logical_not(joined))
            def _():
                hand_to(ret, rr.at[z])

            return carry

        lax.fori_loop(0, local, hand, 0)

    tile = 256
    inner_tiles = [slice(n, n + tile) for n in range(0, hidden.shape[4], tile)]
    out_width = downv.shape[1] // gates

    def expert(j, c):
        with jax.named_scope("wait_inc"):
            copied(inc.at[j, c], inc.at[j, c], pr.at[j, c]).wait()
        taken_in = inc[j, c].reshape(SIDES * capacity, share)
        for cols in inner_tiles:
            acc = jnp.dot(taken_in, upv[c, :, cols], preferred_element_type=f32)
            acc = acc.reshape(SIDES, PARTS, few, tile)

            @pl.when(c == 0)
            def _():
                hidden[j, :, :, :, cols] = acc

            @pl.when(c != 0)
            def _():
                hidden[j, :, :, :, cols] += acc

    def project(j):
        active = jnp.maximum(hidden[j], 0.0).astype(bf16).reshape(SIDES * capacity, -1)
        for k in range(gates):
            obuf[j, k] = (
                jnp.dot(
                    active,
                    downv[:, k * out_width : (k + 1) * out_width],
                    preferred_element_type=f32,
                )
                .astype(bf16)
                .reshape(SIDES, PARTS, few, out_width)
            )
        with jax.named_scope("back"):
            give_back(j, None)

    def expert_part(j, part):
        c = chunks - 1
        with jax.named_scope("wait_part"):
            arriving = inc.at[j, c, :, part]
            copied(arriving, arriving, raw_r.at[row(j, z), part]).wait()
        taken_in = inc[j, c, :, part].reshape(SIDES * few, share)
        active = []
        for cols in inner_tiles:
            acc = jnp.dot(taken_in, upv[c, :, cols], preferred_element_type=f32)
            acc += hidden[j, :, part, :, cols].reshape(SIDES * few, tile)
            active.append(jnp.maximum(acc, 0.0).astype(bf16))
        active = jnp.concatenate(active, axis=1)
        for k in range(gates):
            obuf[j, k, :, part] = (
                jnp.dot(
                    active,
                    downv[:, k * out_width : (k + 1) * out_width],
                    preferred_element_type=f32,
                )
                .astype(bf16)
                .reshape(SIDES, few, out_width)
            )
        with jax.named_scope("back"):
            give_back(j, part)

    def gate_logits():
        partial = 0.0
        for c in range(chunks):
            partial += lax.dot_general(
                gatev[:, c * width : (c + 1) * width],
                blocks[z, c],
                (((1,), (1,)), ((), ())),
                preferred_element_type=f32,
            )
        logits[g] = partial
        for copy in gate_routes:
            copy.start()

    def gate_factor():
        with jax.named_scope("wait_gate"):
            others = logits.at[pl.ds(0, gates - 1)]
            copied(others, others, gr).wait()
        summed = logits[0]
        for k in range(1, gates):
            summed += logits[k]
        top = jnp.max(summed, axis=0, keepdims=True)
        terms = jnp.exp(summed - top)
        scale = mask[...].astype(f32).reshape(1, rows) / jnp.sum(terms, axis=0, keepdims=True)
        factor[...] = total * terms * scale

        @pl.when(edge)
        def _():
            edge_route.start()

    def join(j, p, weight, returned, index, first):
        ranks = lax.broadcasted_iota(jnp.int32, (capacity, rows), 0).astype(f32)

        def one(i, carry):
            line = places[j, pl.ds(p * local + i, 1), :]
            scale = weight[pl.ds(p * local + i, 1), :]
            select[pl.ds(pl.multiple_of(i * capacity, capacity), capacity), :] = jnp.where(
                line == ranks, scale, 0.0
            ).astype(bf16)
            return carry

        lax.fori_loop(0, local, one, 0)
        if returned is ret:
            with jax.named_scope("wait_ret"):
                copied(ret.at[p], ret.at[p], rr.at[p]).wait()
        found = lax.dot_general(
            select[...],
            returned[p].reshape(slots, out_width),
            (((0,), (0,)), ((), ())),
            preferred_element_type=f32,
        )

        @pl.when(first)
        def _():
            mixed[index] = found

        @pl.when(jnp.logical_not(first))
        def _():
            mixed[index] += found

    def settle():
        others = logits.at[pl.ds(0, gates - 1)]
        copied(others, others, ss).wait()
        ids_on(z).wait_send()
        copied(blocks.at[z], blocks.at[z], ss).wait()
        within = dbuf.at[EDGE, :, :, pl.ds(0, local - 1)]
        copied(within, within, ss).wait()

        @pl.when(middle)
        def _():
            ids_on(near).wait_send()
            copied(blocks.at[near], blocks.at[near], ss).wait()
            more = dbuf.at[pl.ds(0, planes - 1), :, :, pl.ds(0, local - 1)]
            copied(more, more, ss).wait()
            ahead = dbuf.at[pl.ds(planes, planes - 1)]
            copied(ahead, ahead, ss).wait()

    def job(t, carry):
        code = jnp.where(edge, table(EDGE_JOBS, t), table(MIDDLE_JOBS, t))
        kind, rel, c = code // 16, lax.rem(code // 4, 4), lax.rem(code, 4)
        j = plane_of(rel)

        @pl.when(kind == WAIT)
        def _():
            wait(j, rel, c)

        @pl.when((kind == END) | (kind == LOCAL))
        def _():
            dispatch(j, rel, c, kind == END)

        @pl.when(kind == EXPERT)
        def _():
            expert(j, c)

        @pl.when(kind == BACK)
        def _():
            project(j)

        @pl.when(kind == END_PART)
        def _():
            dispatch_part(c)

        @pl.when(kind == EXPERT_PART)
        def _():
            expert_part(j, c)

        @pl.when(kind == WEIGHTS)
        def _():
            with jax.named_scope("wait_w"):
                weights[0].wait()
                copied(upv, upv, own_sem).wait()

        @pl.when(kind == LOGITS)
        def _():
            gate_logits()

        @pl.when(kind == FACTOR)
        def _():
            gate_factor()

        @pl.when(kind == JOIN_EDGE)
        def _():
            @pl.when(rel == OWN)
            def _():
                copied(edge_factor, edge_factor, fr).wait()
                joined = edge_ret.at[pl.ds(0, planes - 1)]
                copied(joined, joined, er).wait()

            join(near, j, edge_factor, edge_ret, 0, rel == OWN)

            @pl.when(rel == FAR)
            def _():
                part[...] = mixed[0].astype(bf16)
                part_route.start()

        @pl.when((kind == OPEN) & late)
        def _():
            copied(named.at[inner], named.at[inner], id_r.at[row(inner, z)]).wait()
            open_inner()

        @pl.when(kind == SETTLE)
        def _():
            settle()

        @pl.when(kind == JOIN)
        def _():
            join(z, j, factor, ret, 1, edge | (rel == OWN))

        return carry

    lax.fori_loop(0, jnp.where(edge, len(EDGE_JOBS), len(MIDDLE_JOBS)), job, 0)

    @pl.when(edge)
    def _():
        with jax.named_scope("wait_taken"):
            copied(taken, taken, fr).wait()
        with jax.named_scope("fin_add"):
            out[...] = (mixed[1] + taken[...].astype(f32)).astype(bf16)

    @pl.when(middle)
    def _():
        with jax.named_scope("fin_add"):
            out[...] = mixed[1].astype(bf16)

    handed = ret.at[pl.ds(0, planes - 1)]
    few_more = ret.at[0, pl.ds(0, local - 2)]
    one_more = ret.at[0, 0]
    copied(handed, handed, ss).wait()
    copied(few_more, few_more, ss).wait()

    @pl.when(edge)
    def _():
        copied(one_more, one_more, ss).wait()
        edge_route.wait_send()

    @pl.when(middle)
    def _():
        part_route.wait_send()


def exchange(samples, ids, pads, gate_weight, up, down, planes, gates, capacity):
    rows, share = samples.shape
    local = SIDES * gates
    total = planes * local
    width = share // CHUNKS
    depth, inner = up.shape[1:]
    outer = down.shape[2]
    out_width = outer // gates
    bf16, f32 = jnp.bfloat16, jnp.float32
    dma = pltpu.SemaphoreType.DMA
    hbm = pl.BlockSpec(memory_space=pl.ANY)
    slots = local * capacity
    few = capacity // PARTS
    kinds = 2 * planes - 1
    return pl.pallas_call(
        functools.partial(exchange_kernel, gates, capacity),
        out_shape=pltpu.VMEM((rows, out_width), bf16),
        in_specs=[hbm] * 6,
        out_specs=pl.BlockSpec(memory_space=pltpu.VMEM),
        scratch_shapes=[
            pltpu.VMEM((planes, CHUNKS, rows, width), bf16),
            pltpu.VMEM((planes,) + ids.shape, jnp.int32),
            pltpu.VMEM(pads.shape, jnp.int32),
            pltpu.VMEM(gate_weight.shape, bf16),
            pltpu.VMEM((planes, total, rows), f32),
            pltpu.VMEM((rows, rows), bf16),
            pltpu.VMEM((kinds, PARTS, local, few, rows), bf16),
            pltpu.VMEM((kinds, CHUNKS, PARTS, local, few, width), bf16),
            pltpu.VMEM((planes, CHUNKS, SIDES, PARTS, few, gates * width), bf16),
            pltpu.VMEM((CHUNKS, depth // CHUNKS, inner), bf16),
            pltpu.VMEM((inner, outer), bf16),
            pltpu.VMEM((planes, SIDES, PARTS, few, inner), f32),
            pltpu.VMEM((planes, gates, SIDES, PARTS, few, out_width), bf16),
            pltpu.VMEM((gates, total, rows), f32),
            pltpu.VMEM((total, rows), f32),
            pltpu.VMEM((total, rows), f32),
            pltpu.VMEM((planes, local, PARTS, few, out_width), bf16),
            pltpu.VMEM((planes, local, PARTS, few, out_width), bf16),
            pltpu.VMEM((slots, rows), bf16),
            pltpu.VMEM((2, rows, out_width), f32),
            pltpu.VMEM((rows, out_width), bf16),
            pltpu.VMEM((rows, out_width), bf16),
            dma,
            dma((3,)),
            dma,
            dma((planes - 1, CHUNKS)),
            dma((planes - 1,)),
            dma((planes, CHUNKS)),
            dma((planes,)),
            dma,
            dma,
            dma,
        ],
        compiler_params=pltpu.CompilerParams(
            collective_id=0, has_side_effects=True, vmem_limit_bytes=58 << 20
        ),
    )(samples, ids, pads, gate_weight, up, down)


def in_one_kernel(samples, gate_weight, expert_ids, pad_mask, up_weight, down_weight):
    group_count = lax.axis_size("expert")
    gate_count = lax.axis_size("gate")
    expert_count = group_count * gate_count
    return exchange(
        samples,
        expert_ids.T,
        pad_mask,
        gate_weight.T,
        up_weight,
        down_weight,
        group_count // SIDES,
        gate_count,
        4 * samples.shape[0] // expert_count,
    )


def fits(samples, up_weight, down_weight):
    group_count = lax.axis_size("expert")
    capacity = 4 * samples.shape[0] // (group_count * lax.axis_size("gate"))
    planes = group_count // SIDES
    held = 2 * (planes * samples.size * 3 + up_weight.size + down_weight.size)
    return planes == 4 and group_count % SIDES == 0 and capacity % (16 * PARTS) == 0 and held < 40 << 20


def per_device(samples, gate_weight, expert_ids, pad_mask, up_weight, down_weight):
    if fits(samples, up_weight, down_weight):
        return in_one_kernel(
            samples, gate_weight, expert_ids, pad_mask, up_weight, down_weight
        )
    row_count, share = samples.shape
    group_count = lax.axis_size("expert")
    gate_count = lax.axis_size("gate")
    expert_count = group_count * gate_count
    capacity = 4 * row_count // expert_count
    partial = jnp.dot(samples, gate_weight, preferred_element_type=jnp.float32)
    logits = jnp.sum(lax.all_gather(partial, "gate"), axis=0)
    first, second, member, before = routing(expert_ids, expert_count)
    place = jnp.where(member, before, -1).T
    ranks = jnp.arange(capacity, dtype=jnp.int32)
    send = (place[:, None, :] == ranks[None, :, None]).astype(jnp.bfloat16)
    outgoing = jnp.dot(
        send.reshape(expert_count * capacity, row_count), samples, preferred_element_type=jnp.float32
    ).astype(jnp.bfloat16)
    incoming = lax.all_to_all(
        outgoing.reshape(expert_count, capacity, share),
        ("expert", "gate"),
        split_axis=0,
        concat_axis=0,
        tiled=True,
    ).reshape(group_count, gate_count, capacity, share)
    hidden = 0.0
    for g in range(gate_count):
        hidden += jnp.dot(
            incoming[:, g].reshape(group_count * capacity, share),
            up_weight[0, g * share : (g + 1) * share],
            preferred_element_type=jnp.float32,
        )
    active = jnp.maximum(hidden, 0.0).astype(jnp.bfloat16)
    expert_out = jnp.dot(active, down_weight[0], preferred_element_type=jnp.float32).astype(
        jnp.bfloat16
    )
    out_share = expert_out.shape[1] // gate_count
    outbound = expert_out.reshape(group_count, capacity, gate_count, out_share)
    outbound = outbound.transpose(0, 2, 1, 3).reshape(expert_count, capacity, out_share)
    returned = lax.all_to_all(
        outbound, ("expert", "gate"), split_axis=0, concat_axis=0, tiled=True
    ).reshape(expert_count * capacity, out_share)
    factor0, factor1 = factors(logits, first, second, pad_mask, expert_count)
    slots = jnp.arange(expert_count * capacity, dtype=jnp.int32)[None, :]
    mixed = 0.0
    for k, (chosen, factor) in enumerate(((first, factor0), (second, factor1))):
        rank = jnp.sum(jnp.where(chosen, before, 0), axis=1, keepdims=True)
        position = expert_ids[:, k : k + 1] * capacity + rank
        pick = (position == slots).astype(jnp.bfloat16)
        mixed += factor * jnp.dot(pick, returned, preferred_element_type=jnp.float32)
    return mixed.astype(jnp.bfloat16)


def solution(mesh):
    placed = (
        P("expert", "gate"),
        P("gate", None),
        P("expert", None),
        P("expert"),
        P(("expert", "gate"), None, None),
        P(("expert", "gate"), None, None),
    )
    return jax.shard_map(
        per_device, mesh=mesh, in_specs=placed, out_specs=P("expert", "gate"), check_vma=False
    )
```

```python
import functools

import jax
import jax.numpy as jnp
from jax import lax
from jax.experimental import pallas as pl
from jax.experimental.pallas import tpu as pltpu
from jax.sharding import PartitionSpec as P


MESH = pl.DeviceIdType.MESH
CHUNKS = 4
SIDES = 2
PARTS = 3
STRIDE = 5


def routing(expert_ids, expert_count):
    row_count = expert_ids.shape[0]
    lanes = jnp.arange(expert_count, dtype=jnp.int32)[None, :]
    first = expert_ids[:, 0:1] == lanes
    second = expert_ids[:, 1:2] == lanes
    member = first | second
    rows = jnp.arange(row_count, dtype=jnp.int32)
    lower = (rows[:, None] > rows[None, :]).astype(jnp.bfloat16)
    before = jnp.dot(lower, member.astype(jnp.bfloat16), preferred_element_type=jnp.float32)
    before = before.astype(jnp.int32)
    return first, second, member, before


def factors(logits, first, second, pad_mask, expert_count):
    top = jnp.max(logits, axis=1, keepdims=True)
    terms = jnp.exp(logits - top)
    scale = pad_mask.astype(jnp.float32)[:, None] / jnp.sum(terms, axis=1, keepdims=True)
    factor0 = expert_count * jnp.sum(jnp.where(first, terms, 0.0), axis=1, keepdims=True) * scale
    factor1 = expert_count * jnp.sum(jnp.where(second, terms, 0.0), axis=1, keepdims=True) * scale
    return factor0, factor1


def copied(source, target, sem):
    return pltpu.make_async_copy(source, target, sem)


def sent(source, target, send_sem, recv_sem, device):
    return pltpu.make_async_remote_copy(
        src_ref=source,
        dst_ref=target,
        send_sem=send_sem,
        recv_sem=recv_sem,
        device_id=device,
        device_id_type=MESH,
    )


def table(values, index):
    out = values[0]
    for k in range(1, len(values)):
        out = jnp.where(index == k, values[k], out)
    return out


NONE, WAIT, END, LOCAL, EXPERT, LOGITS, FACTOR, JOIN_EDGE, JOIN, END_PART, EXPERT_PART, WEIGHTS, BACK, SETTLE, OPEN = range(15)
OWN, EDGE, INNER, FAR = range(4)


def coded(*jobs):
    return [kind * 16 + rel * 4 + c for kind, rel, c in jobs]


MIDDLE_JOBS = coded(
    (LOGITS, OWN, 0),
    (LOCAL, OWN, 0),
    (OPEN, OWN, 0),
    (LOCAL, OWN, 1),
    (LOCAL, OWN, 2),
    (LOCAL, OWN, 3),
    (END, OWN, 1),
    (WEIGHTS, OWN, 0),
    (EXPERT, OWN, 0),
    (FACTOR, OWN, 0),
    (WAIT, EDGE, 0),
    (LOCAL, EDGE, 0),
    (WAIT, INNER, 0),
    (END, INNER, 0),
    (LOCAL, INNER, 0),
    (EXPERT, OWN, 1),
    (EXPERT, OWN, 2),
    (WAIT, EDGE, 1),
    (LOCAL, EDGE, 1),
    (WAIT, INNER, 1),
    (END, INNER, 1),
    (LOCAL, INNER, 1),
    (EXPERT, OWN, 3),
    (EXPERT, EDGE, 0),
    (WAIT, EDGE, 2),
    (LOCAL, EDGE, 2),
    (WAIT, FAR, 0),
    (END, FAR, 0),
    (LOCAL, FAR, 0),
    (EXPERT, INNER, 0),
    (EXPERT, EDGE, 1),
    (WAIT, EDGE, 3),
    (LOCAL, EDGE, 3),
    (WAIT, FAR, 1),
    (END, FAR, 1),
    (LOCAL, FAR, 1),
    (EXPERT, INNER, 1),
    (WAIT, FAR, 2),
    (END, FAR, 2),
    (LOCAL, FAR, 2),
    (EXPERT, EDGE, 2),
    (WAIT, FAR, 3),
    (END, FAR, 3),
    (LOCAL, FAR, 3),
    (EXPERT, FAR, 0),
    (EXPERT, EDGE, 3),
    (EXPERT, FAR, 1),
    (WAIT, INNER, 2),
    (END, INNER, 2),
    (LOCAL, INNER, 2),
    (EXPERT, FAR, 2),
    (EXPERT, FAR, 3),
    (BACK, FAR, 0),
    (WAIT, INNER, 3),
    (END, INNER, 3),
    (LOCAL, INNER, 3),
    (END, OWN, 2),
    (END_PART, OWN, 0),
    (END_PART, OWN, 1),
    (END_PART, OWN, 2),
    (BACK, EDGE, 0),
    (BACK, OWN, 0),
    (EXPERT, INNER, 2),
    (EXPERT, INNER, 3),
    (BACK, INNER, 0),
    (JOIN_EDGE, OWN, 0),
    (JOIN_EDGE, INNER, 0),
    (JOIN_EDGE, FAR, 0),
    (JOIN, OWN, 0),
    (JOIN, INNER, 0),
    (JOIN, FAR, 0),
    (SETTLE, OWN, 0),
    (JOIN, EDGE, 0),
)
EDGE_JOBS = coded(
    (LOGITS, EDGE, 0),
    (LOCAL, EDGE, 1),
    (LOCAL, EDGE, 2),
    (LOCAL, EDGE, 3),
    (WEIGHTS, EDGE, 0),
    (EXPERT, EDGE, 0),
    (FACTOR, EDGE, 0),
    (EXPERT, EDGE, 1),
    (EXPERT, OWN, 0),
    (EXPERT, EDGE, 2),
    (EXPERT, OWN, 1),
    (EXPERT, EDGE, 3),
    (BACK, EDGE, 0),
    (EXPERT, INNER, 0),
    (EXPERT, INNER, 1),
    (EXPERT, FAR, 0),
    (EXPERT, FAR, 1),
    (EXPERT, FAR, 2),
    (EXPERT, FAR, 3),
    (BACK, FAR, 0),
    (EXPERT, INNER, 2),
    (EXPERT, INNER, 3),
    (BACK, INNER, 0),
    (EXPERT, OWN, 2),
    (EXPERT_PART, OWN, 0),
    (EXPERT_PART, OWN, 1),
    (EXPERT_PART, OWN, 2),
    (JOIN, EDGE, 0),
    (SETTLE, OWN, 0),
)


def exchange_kernel(
    gates,
    capacity,
    samples,
    ids,
    pads,
    gate_weight,
    up,
    down,
    out,
    blocks,
    named,
    mask,
    gatev,
    places,
    lower,
    onehot,
    dbuf,
    inc,
    upv,
    downv,
    hidden,
    obuf,
    logits,
    factor,
    edge_factor,
    ret,
    edge_ret,
    select,
    mixed,
    part,
    taken,
    own_sem,
    in_sem,
    ss,
    raw_r,
    id_r,
    pr,
    rr,
    er,
    gr,
    fr,
):
    chunks = CHUNKS
    local = SIDES * gates
    planes = blocks.shape[0]
    total = planes * local
    rows = blocks.shape[2]
    width = blocks.shape[3]
    share = width * chunks
    slots = local * capacity
    few = capacity // PARTS
    bf16, f32 = jnp.bfloat16, jnp.float32
    e = lax.axis_index("expert")
    g = lax.axis_index("gate")
    z = e // SIDES
    y = lax.rem(e, SIDES)
    mine = y * gates + g
    low = z < planes // 2
    toward = jnp.where(low, 1, -1)
    near = jnp.where(low, 0, planes - 1)
    far = planes - 1 - near
    edge = z == near
    middle = jnp.logical_not(edge)
    mid = near + toward
    inner = z + toward

    def plane_of(rel):
        return table((mid, near, mid + toward, far), rel)

    def row(j, reader):
        return lax.rem(j - reader + planes, planes) - 1

    def at(plane, i):
        return (plane * SIDES + i // gates, lax.rem(i, gates))

    barrier = pltpu.get_barrier_semaphore()

    inputs = (
        copied(ids, named.at[z], in_sem.at[0]),
        copied(pads, mask, in_sem.at[1]),
        copied(gate_weight, gatev, in_sem.at[2]),
    )
    for copy in inputs:
        copy.start()
    own = [
        copied(samples.at[:, pl.ds(c * width, width)], blocks.at[z, c], own_sem)
        for c in range(chunks)
    ]
    for copy in own:
        copy.start()
    greeting = (
        jnp.where(edge, toward, 0),
        jnp.where(edge, 0, -toward),
        jnp.where(edge, -toward, toward),
    )

    def greet(d, carry):
        plane = z + table(greeting, d // local)
        i = lax.rem(mine + d, local)

        told = (plane >= 0) & (plane < planes) & ((plane != z) | (i != mine))

        @pl.when(told & (edge | low | (plane != inner)))
        def _():
            pl.semaphore_signal(barrier, inc=1, device_id=at(plane, i), device_id_type=MESH)

        return carry

    with jax.named_scope("greet"):
        lax.fori_loop(0, 3 * local, greet, 0)
    greeted = jnp.where(edge | low, 2, 3) * local - 1
    late = middle & low

    weights = [copied(down.at[0], downv, in_sem.at[0])]
    for c in range(chunks):
        for k in range(gates):
            weights.append(
                copied(
                    up.at[0, pl.ds(k * share + c * width, width)],
                    upv.at[c, pl.ds(k * width, width)],
                    own_sem,
                )
            )

    earlier = lax.broadcasted_iota(jnp.int32, (rows, rows), 0)
    later = lax.broadcasted_iota(jnp.int32, (rows, rows), 1)
    with jax.named_scope("lower"):
        lower[...] = jnp.where(earlier < later, 1.0, 0.0).astype(bf16)

    def end_index(rel):
        return jnp.where(rel == OWN, planes, planes - 1 + rel)

    def locate(j):
        lanes = lax.broadcasted_iota(jnp.int32, (total, rows), 0)
        member = (named[j, 0:1, :] == lanes) | (named[j, 1:2, :] == lanes)
        flags = jnp.where(member, 1.0, 0.0).astype(bf16)
        before = jnp.dot(flags, lower[...], preferred_element_type=f32)
        places[j] = jnp.where(member, before, -1.0)

    def build(j, index, plane):
        ranks = lax.broadcasted_iota(jnp.int32, (capacity, rows), 0).astype(f32)

        def one(i, carry):
            line = places[j, pl.ds(plane * local + i, 1), :]
            found = jnp.where(line == ranks, 1.0, 0.0).astype(bf16)
            onehot[index, :, i] = found.reshape(PARTS, few, rows)
            return carry

        lax.fori_loop(0, local, one, 0)

    def pick(index, part, j, c):
        dbuf[index, c, part] = (
            jnp.dot(
                onehot[index, part].reshape(local * few, rows),
                blocks[j, c],
                preferred_element_type=f32,
            )
            .astype(bf16)
            .reshape(local, few, width)
        )

    def hand_out(j, rel, c, to_end):
        index = jnp.where(to_end, end_index(rel), rel)
        plane = jnp.where(to_end, near, z)

        def give(d, carry):
            i = lax.rem(mine + STRIDE * d, local)
            piece = dbuf.at[index, c, :, i]
            place = inc.at[j, c, y, :, :, pl.ds(g * width, width)]
            here = jnp.logical_not(to_end) & (d == 0)

            @pl.when(here)
            def _():
                copied(piece, place, pr.at[j, c]).start()

            @pl.when(jnp.logical_not(here))
            def _():
                sent(piece, place, ss, pr.at[j, c], at(plane, i)).start()

            return carry

        lax.fori_loop(0, local, give, 0)

    with jax.named_scope("inputs"):
        for copy in inputs:
            copy.wait()
    first = jnp.where(edge, EDGE, planes)
    with jax.named_scope("prepare"):
        locate(z)
        build(z, first, near)
    with jax.named_scope("samples"):
        copied(blocks.at[z], blocks.at[z], own_sem).wait()
    for q in range(PARTS):
        pick(first, q, z, 0)
    with jax.named_scope("barrier"):
        pl.semaphore_wait(barrier, greeted)
    hand_out(z, jnp.where(edge, EDGE, OWN), 0, middle)

    def ids_on(j):
        return sent(named.at[j], named.at[j], ss, id_r.at[row(j, inner)], at(inner, mine))

    def shift(j, c):
        return sent(
            blocks.at[j, c], blocks.at[j, c], ss, raw_r.at[row(j, inner), c], at(inner, mine)
        )

    def open_inner():
        ids_on(z).start()
        for c in range(2):
            shift(z, c).start()

    @pl.when(jnp.logical_not(late))
    def _():
        open_inner()

    @pl.when(edge)
    def _():
        for c in range(2, chunks):
            shift(z, c).start()

    for copy in weights:
        copy.start()

    @pl.when(middle)
    def _():
        build(z, OWN, z)

    gate_routes = []
    for d in range(1, gates):
        t = lax.rem(g + d, gates)
        gate_routes.append(sent(logits.at[g], logits.at[g], ss, gr, (e, t)))
    edge_route = sent(factor, edge_factor, ss, fr, at(inner, mine))
    part_route = sent(part, taken, ss, fr, at(near, mine))

    def wait(j, rel, c):
        with jax.named_scope("wait_raw"):
            copied(blocks.at[j, c], blocks.at[j, c], raw_r.at[row(j, z), c]).wait()

        @pl.when((c == 0) & jnp.logical_not(late & (rel == INNER)))
        def _():
            copied(named.at[j], named.at[j], id_r.at[row(j, z)]).wait()

        @pl.when(rel == EDGE)
        def _():
            @pl.when(c == 0)
            def _():
                ids_on(j).start()

            shift(j, c).start()

            @pl.when(c == chunks - 1)
            def _():
                for k in range(2, chunks):
                    shift(z, k).start()

        @pl.when(c == 0)
        def _():
            locate(j)

            @pl.when(rel != EDGE)
            def _():
                build(j, end_index(rel), near)

            build(j, rel, z)

    def dispatch(j, rel, c, to_end):
        index = jnp.where(to_end, end_index(rel), rel)
        with jax.named_scope("pick"):
            for part in range(PARTS):
                pick(index, part, j, c)
        hand_out(j, rel, c, to_end)

    def dispatch_part(part):
        c = chunks - 1
        pick(planes, part, z, c)

        def give(d, carry):
            i = lax.rem(mine + STRIDE * d, local)
            sent(
                dbuf.at[planes, c, part, i],
                inc.at[z, c, y, part, :, pl.ds(g * width, width)],
                ss,
                raw_r.at[row(z, near), part],
                at(near, i),
            ).start()
            return carry

        lax.fori_loop(0, local, give, 0)

    def give_back(j, part):
        ends = (j == 0) | (j == planes - 1)
        joined = ends & (j != z)
        plane = jnp.where(joined, jnp.where(j == 0, 1, planes - 2), j)

        def hand(d, carry):
            i = lax.rem(mine + STRIDE * d, local)
            side, k = i // gates, lax.rem(i, gates)
            here = (plane == z) & (d == 0)

            def hand_to(buffer, sem):
                if part is None:
                    block, spot = obuf.at[j, k, side], buffer.at[z, mine]
                else:
                    block, spot = obuf.at[j, k, side, part], buffer.at[z, mine, part]

                @pl.when(here)
                def _():
                    copied(block, spot, sem).start()

                @pl.when(jnp.logical_not(here))
                def _():
                    sent(block, spot, ss, sem, at(plane, i)).start()

            @pl.when(joined)
            def _():
                hand_to(edge_ret, er)

            @pl.when(jnp.logical_not(joined))
            def _():
                hand_to(ret, rr.at[z])

            return carry

        lax.fori_loop(0, local, hand, 0)

    tile = 256
    inner_tiles = [slice(n, n + tile) for n in range(0, hidden.shape[4], tile)]
    out_width = downv.shape[1] // gates

    def expert(j, c):
        with jax.named_scope("wait_inc"):
            copied(inc.at[j, c], inc.at[j, c], pr.at[j, c]).wait()
        taken_in = inc[j, c].reshape(SIDES * capacity, share)
        for cols in inner_tiles:
            acc = jnp.dot(taken_in, upv[c, :, cols], preferred_element_type=f32)
            acc = acc.reshape(SIDES, PARTS, few, tile)

            @pl.when(c == 0)
            def _():
                hidden[j, :, :, :, cols] = acc

            @pl.when(c != 0)
            def _():
                hidden[j, :, :, :, cols] += acc

    def project(j):
        active = jnp.maximum(hidden[j], 0.0).astype(bf16).reshape(SIDES * capacity, -1)
        for k in range(gates):
            obuf[j, k] = (
                jnp.dot(
                    active,
                    downv[:, k * out_width : (k + 1) * out_width],
                    preferred_element_type=f32,
                )
                .astype(bf16)
                .reshape(SIDES, PARTS, few, out_width)
            )
        with jax.named_scope("back"):
            give_back(j, None)

    def expert_part(j, part):
        c = chunks - 1
        with jax.named_scope("wait_part"):
            arriving = inc.at[j, c, :, part]
            copied(arriving, arriving, raw_r.at[row(j, z), part]).wait()
        taken_in = inc[j, c, :, part].reshape(SIDES * few, share)
        active = []
        for cols in inner_tiles:
            acc = jnp.dot(taken_in, upv[c, :, cols], preferred_element_type=f32)
            acc += hidden[j, :, part, :, cols].reshape(SIDES * few, tile)
            active.append(jnp.maximum(acc, 0.0).astype(bf16))
        active = jnp.concatenate(active, axis=1)
        for k in range(gates):
            obuf[j, k, :, part] = (
                jnp.dot(
                    active,
                    downv[:, k * out_width : (k + 1) * out_width],
                    preferred_element_type=f32,
                )
                .astype(bf16)
                .reshape(SIDES, few, out_width)
            )
        with jax.named_scope("back"):
            give_back(j, part)

    def gate_logits():
        partial = 0.0
        for c in range(chunks):
            partial += lax.dot_general(
                gatev[:, c * width : (c + 1) * width],
                blocks[z, c],
                (((1,), (1,)), ((), ())),
                preferred_element_type=f32,
            )
        logits[g] = partial
        for copy in gate_routes:
            copy.start()

    def gate_factor():
        with jax.named_scope("wait_gate"):
            others = logits.at[pl.ds(0, gates - 1)]
            copied(others, others, gr).wait()
        summed = logits[0]
        for k in range(1, gates):
            summed += logits[k]
        top = jnp.max(summed, axis=0, keepdims=True)
        terms = jnp.exp(summed - top)
        scale = mask[...].astype(f32).reshape(1, rows) / jnp.sum(terms, axis=0, keepdims=True)
        factor[...] = total * terms * scale

        @pl.when(edge)
        def _():
            edge_route.start()

    def join(j, p, weight, returned, index, first):
        ranks = lax.broadcasted_iota(jnp.int32, (capacity, rows), 0).astype(f32)

        def one(i, carry):
            line = places[j, pl.ds(p * local + i, 1), :]
            scale = weight[pl.ds(p * local + i, 1), :]
            select[pl.ds(pl.multiple_of(i * capacity, capacity), capacity), :] = jnp.where(
                line == ranks, scale, 0.0
            ).astype(bf16)
            return carry

        lax.fori_loop(0, local, one, 0)
        if returned is ret:
            with jax.named_scope("wait_ret"):
                copied(ret.at[p], ret.at[p], rr.at[p]).wait()
        found = lax.dot_general(
            select[...],
            returned[p].reshape(slots, out_width),
            (((0,), (0,)), ((), ())),
            preferred_element_type=f32,
        )

        @pl.when(first)
        def _():
            mixed[index] = found

        @pl.when(jnp.logical_not(first))
        def _():
            mixed[index] += found

    def settle():
        others = logits.at[pl.ds(0, gates - 1)]
        copied(others, others, ss).wait()
        ids_on(z).wait_send()
        copied(blocks.at[z], blocks.at[z], ss).wait()
        within = dbuf.at[EDGE, :, :, pl.ds(0, local - 1)]
        copied(within, within, ss).wait()

        @pl.when(middle)
        def _():
            ids_on(near).wait_send()
            copied(blocks.at[near], blocks.at[near], ss).wait()
            more = dbuf.at[pl.ds(0, planes - 1), :, :, pl.ds(0, local - 1)]
            copied(more, more, ss).wait()
            ahead = dbuf.at[pl.ds(planes, planes - 1)]
            copied(ahead, ahead, ss).wait()

    def job(t, carry):
        code = jnp.where(edge, table(EDGE_JOBS, t), table(MIDDLE_JOBS, t))
        kind, rel, c = code // 16, lax.rem(code // 4, 4), lax.rem(code, 4)
        j = plane_of(rel)

        @pl.when(kind == WAIT)
        def _():
            wait(j, rel, c)

        @pl.when((kind == END) | (kind == LOCAL))
        def _():
            dispatch(j, rel, c, kind == END)

        @pl.when(kind == EXPERT)
        def _():
            expert(j, c)

        @pl.when(kind == BACK)
        def _():
            project(j)

        @pl.when(kind == END_PART)
        def _():
            dispatch_part(c)

        @pl.when(kind == EXPERT_PART)
        def _():
            expert_part(j, c)

        @pl.when(kind == WEIGHTS)
        def _():
            with jax.named_scope("wait_w"):
                weights[0].wait()
                copied(upv, upv, own_sem).wait()

        @pl.when(kind == LOGITS)
        def _():
            gate_logits()

        @pl.when(kind == FACTOR)
        def _():
            gate_factor()

        @pl.when(kind == JOIN_EDGE)
        def _():
            @pl.when(rel == OWN)
            def _():
                copied(edge_factor, edge_factor, fr).wait()
                joined = edge_ret.at[pl.ds(0, planes - 1)]
                copied(joined, joined, er).wait()

            join(near, j, edge_factor, edge_ret, 0, rel == OWN)

            @pl.when(rel == FAR)
            def _():
                part[...] = mixed[0].astype(bf16)
                part_route.start()

        @pl.when((kind == OPEN) & late)
        def _():
            copied(named.at[inner], named.at[inner], id_r.at[row(inner, z)]).wait()
            open_inner()

        @pl.when(kind == SETTLE)
        def _():
            settle()

        @pl.when(kind == JOIN)
        def _():
            join(z, j, factor, ret, 1, edge | (rel == OWN))

        return carry

    lax.fori_loop(0, jnp.where(edge, len(EDGE_JOBS), len(MIDDLE_JOBS)), job, 0)

    @pl.when(edge)
    def _():
        with jax.named_scope("wait_taken"):
            copied(taken, taken, fr).wait()
        with jax.named_scope("fin_add"):
            out[...] = (mixed[1] + taken[...].astype(f32)).astype(bf16)

    @pl.when(middle)
    def _():
        with jax.named_scope("fin_add"):
            out[...] = mixed[1].astype(bf16)

    handed = ret.at[pl.ds(0, planes - 1)]
    few_more = ret.at[0, pl.ds(0, local - 2)]
    one_more = ret.at[0, 0]
    copied(handed, handed, ss).wait()
    copied(few_more, few_more, ss).wait()

    @pl.when(edge)
    def _():
        copied(one_more, one_more, ss).wait()
        edge_route.wait_send()

    @pl.when(middle)
    def _():
        part_route.wait_send()


def exchange(samples, ids, pads, gate_weight, up, down, planes, gates, capacity):
    rows, share = samples.shape
    local = SIDES * gates
    total = planes * local
    width = share // CHUNKS
    depth, inner = up.shape[1:]
    outer = down.shape[2]
    out_width = outer // gates
    bf16, f32 = jnp.bfloat16, jnp.float32
    dma = pltpu.SemaphoreType.DMA
    hbm = pl.BlockSpec(memory_space=pl.ANY)
    slots = local * capacity
    few = capacity // PARTS
    kinds = 2 * planes - 1
    return pl.pallas_call(
        functools.partial(exchange_kernel, gates, capacity),
        out_shape=pltpu.VMEM((rows, out_width), bf16),
        in_specs=[hbm] * 6,
        out_specs=pl.BlockSpec(memory_space=pltpu.VMEM),
        scratch_shapes=[
            pltpu.VMEM((planes, CHUNKS, rows, width), bf16),
            pltpu.VMEM((planes,) + ids.shape, jnp.int32),
            pltpu.VMEM(pads.shape, jnp.int32),
            pltpu.VMEM(gate_weight.shape, bf16),
            pltpu.VMEM((planes, total, rows), f32),
            pltpu.VMEM((rows, rows), bf16),
            pltpu.VMEM((kinds, PARTS, local, few, rows), bf16),
            pltpu.VMEM((kinds, CHUNKS, PARTS, local, few, width), bf16),
            pltpu.VMEM((planes, CHUNKS, SIDES, PARTS, few, gates * width), bf16),
            pltpu.VMEM((CHUNKS, depth // CHUNKS, inner), bf16),
            pltpu.VMEM((inner, outer), bf16),
            pltpu.VMEM((planes, SIDES, PARTS, few, inner), f32),
            pltpu.VMEM((planes, gates, SIDES, PARTS, few, out_width), bf16),
            pltpu.VMEM((gates, total, rows), f32),
            pltpu.VMEM((total, rows), f32),
            pltpu.VMEM((total, rows), f32),
            pltpu.VMEM((planes, local, PARTS, few, out_width), bf16),
            pltpu.VMEM((planes, local, PARTS, few, out_width), bf16),
            pltpu.VMEM((slots, rows), bf16),
            pltpu.VMEM((2, rows, out_width), f32),
            pltpu.VMEM((rows, out_width), bf16),
            pltpu.VMEM((rows, out_width), bf16),
            dma,
            dma((3,)),
            dma,
            dma((planes - 1, CHUNKS)),
            dma((planes - 1,)),
            dma((planes, CHUNKS)),
            dma((planes,)),
            dma,
            dma,
            dma,
        ],
        compiler_params=pltpu.CompilerParams(
            collective_id=0, has_side_effects=True, vmem_limit_bytes=58 << 20
        ),
    )(samples, ids, pads, gate_weight, up, down)


def in_one_kernel(samples, gate_weight, expert_ids, pad_mask, up_weight, down_weight):
    group_count = lax.axis_size("expert")
    gate_count = lax.axis_size("gate")
    expert_count = group_count * gate_count
    return exchange(
        samples,
        expert_ids.T,
        pad_mask,
        gate_weight.T,
        up_weight,
        down_weight,
        group_count // SIDES,
        gate_count,
        4 * samples.shape[0] // expert_count,
    )


def fits(samples, up_weight, down_weight):
    group_count = lax.axis_size("expert")
    capacity = 4 * samples.shape[0] // (group_count * lax.axis_size("gate"))
    planes = group_count // SIDES
    held = 2 * (planes * samples.size * 3 + up_weight.size + down_weight.size)
    return planes == 4 and group_count % SIDES == 0 and capacity % (16 * PARTS) == 0 and held < 40 << 20


def per_device(samples, gate_weight, expert_ids, pad_mask, up_weight, down_weight):
    if fits(samples, up_weight, down_weight):
        return in_one_kernel(
            samples, gate_weight, expert_ids, pad_mask, up_weight, down_weight
        )
    row_count, share = samples.shape
    group_count = lax.axis_size("expert")
    gate_count = lax.axis_size("gate")
    expert_count = group_count * gate_count
    capacity = 4 * row_count // expert_count
    partial = jnp.dot(samples, gate_weight, preferred_element_type=jnp.float32)
    logits = jnp.sum(lax.all_gather(partial, "gate"), axis=0)
    first, second, member, before = routing(expert_ids, expert_count)
    place = jnp.where(member, before, -1).T
    ranks = jnp.arange(capacity, dtype=jnp.int32)
    send = (place[:, None, :] == ranks[None, :, None]).astype(jnp.bfloat16)
    outgoing = jnp.dot(
        send.reshape(expert_count * capacity, row_count), samples, preferred_element_type=jnp.float32
    ).astype(jnp.bfloat16)
    incoming = lax.all_to_all(
        outgoing.reshape(expert_count, capacity, share),
        ("expert", "gate"),
        split_axis=0,
        concat_axis=0,
        tiled=True,
    ).reshape(group_count, gate_count, capacity, share)
    hidden = 0.0
    for g in range(gate_count):
        hidden += jnp.dot(
            incoming[:, g].reshape(group_count * capacity, share),
            up_weight[0, g * share : (g + 1) * share],
            preferred_element_type=jnp.float32,
        )
    active = jnp.maximum(hidden, 0.0).astype(jnp.bfloat16)
    expert_out = jnp.dot(active, down_weight[0], preferred_element_type=jnp.float32).astype(
        jnp.bfloat16
    )
    out_share = expert_out.shape[1] // gate_count
    outbound = expert_out.reshape(group_count, capacity, gate_count, out_share)
    outbound = outbound.transpose(0, 2, 1, 3).reshape(expert_count, capacity, out_share)
    returned = lax.all_to_all(
        outbound, ("expert", "gate"), split_axis=0, concat_axis=0, tiled=True
    ).reshape(expert_count * capacity, out_share)
    factor0, factor1 = factors(logits, first, second, pad_mask, expert_count)
    slots = jnp.arange(expert_count * capacity, dtype=jnp.int32)[None, :]
    mixed = 0.0
    for k, (chosen, factor) in enumerate(((first, factor0), (second, factor1))):
        rank = jnp.sum(jnp.where(chosen, before, 0), axis=1, keepdims=True)
        position = expert_ids[:, k : k + 1] * capacity + rank
        pick = (position == slots).astype(jnp.bfloat16)
        mixed += factor * jnp.dot(pick, returned, preferred_element_type=jnp.float32)
    return mixed.astype(jnp.bfloat16)


def solution(mesh):
    placed = (
        P("expert", "gate"),
        P("gate", None),
        P("expert", None),
        P("expert"),
        P(("expert", "gate"), None, None),
        P(("expert", "gate"), None, None),
    )
    return jax.shard_map(
        per_device, mesh=mesh, in_specs=placed, out_specs=P("expert", "gate"), check_vma=False
    )
```
